128 devices in a mesh: facet: 8 (over z, core), chan: 16 (over x, y).
Axes of the slice: x: 4, y: 4, z: 4, core: 2. Of those that a mesh axis runs over, the one named last changes fastest.
Arguments:
- visibilities: bfloat16 [2, 16, 512, 128, 128], P(None, None, None, ('facet', 'chan')), may hold values from -12 to 12
- kernels: bfloat16 [32, 256, 512], replicated, may hold values from -0.25 to 0.25
- delays: float32 [16, 512, 128], P('facet'), may hold values from -4 to 4
- tile_of: int32 [16, 512], P('facet'), may hold values from 0 to 255
- plane_of: int32 [16, 512], P('facet'), may hold values from 0 to 31
- counts: int32 [16], P('facet'), may hold values from 128 to 512
- neighbours: int32 [16, 4], replicated, may hold values from 0 to 15, as said below
Outputs:
- joined_grids: float32 [256, 16, 16, 512], P('chan', 'facet')
The draws below stay inside these ranges and needn't reach their ends.
Inputs may be any that keep to these rules, and one draw needn't show every extreme that they name: `neighbours`: each row names 4 different facets, none of them its own.
All inputs are finite; a program needn't handle non-finite values.
Results may differ from the reference program's by a relative error of at most 0.0043.
Values may be sent and summed in bfloat16 or wider, within the bound.
No kernel may reach another device: no remote copies, remote signals or barrier semaphores. Data moves between devices by JAX's collectives and lax.ppermute only.
A program may use at most 128 MiB of HBM per device.

```python
import math
import jax
import jax.numpy as jnp
from jax import lax

FACETS = 16
BLOCKS = 512
CHANNELS = 128
AVG = 8
OUTCH = 16
BV = 128
TS = 16
TILE = 256
NTILES = 256
WPLANES = 32
EDGE = 4
NNB = 4


def draw_neighbours(key, part):
    facet_keys = jax.random.split(jax.random.fold_in(key, 7), FACETS)

    def draw_row(row_key, facet_id):
        shuffled = jax.random.permutation(row_key, FACETS - 1)[:NNB].astype(jnp.int32)
        return jnp.where(shuffled >= facet_id, shuffled + 1, shuffled).astype(jnp.int32)
    return jax.vmap(draw_row)(facet_keys, jnp.arange(FACETS, dtype=jnp.int32))


def plant(result, stream_key, smallest, largest):
    place = [jax.random.randint(jax.random.fold_in(stream_key, axis), (), 0, length) for axis, length in enumerate(result.shape)]
    widest = result.shape.index(max(result.shape))
    beside = place[:widest] + [(place[widest] + 1) % result.shape[widest]] + place[widest + 1:]
    return result.at[tuple(place)].set(smallest).at[tuple(beside)].set(largest)


def levels(key, dims, pieces, least, top_value):
    gain = 1.0
    for dim, blocks in pieces:
        heights = jax.random.uniform(jax.random.fold_in(jax.random.fold_in(key, 6), dim), (blocks,), jnp.float32, least / len(pieces), top_value / len(pieces))
        gain = gain * jnp.repeat(jnp.exp(heights), dims[dim] // blocks).reshape((-1,) + (1,) * (len(dims) - 1 - dim))
    return gain


def bell_draw(own_key, extent, spread, reach, pieces=(), kind=jnp.bfloat16):
    array = spread * jax.random.normal(own_key, extent, jnp.float32)
    if pieces:
        array = array * levels(own_key, extent, pieces, -0.22, 0.18)
    return jnp.clip(array, -reach, reach).astype(kind)


def setup_inputs(seed: int = 0) -> dict:
    arg_keys = jax.random.split(jax.random.key(seed), 8)
    return {
        "visibilities": bell_draw(arg_keys[0], (2, FACETS, BLOCKS, CHANNELS, BV), 2.0, 12.0, ((3, 128),)),
        "kernels": bell_draw(arg_keys[1], (WPLANES, 2 * BV, 2 * TILE), (2 * BV * BLOCKS // NTILES) ** -0.5, 0.25),
        "delays": jnp.clip(jax.random.uniform(arg_keys[2], (FACETS, BLOCKS, BV), jnp.float32, -4.0, 4.0) * levels(arg_keys[2], (FACETS, BLOCKS, BV), ((0, 8),), -0.4, 0.0), -4.0, 4.0),
        "tile_of": plant(jax.random.randint(arg_keys[3], (FACETS, BLOCKS), 0, NTILES), jax.random.fold_in(arg_keys[3], 1), 0, NTILES - 1).astype(jnp.int32),
        "plane_of": plant(jax.random.randint(arg_keys[4], (FACETS, BLOCKS), 0, WPLANES), jax.random.fold_in(arg_keys[4], 1), 0, WPLANES - 1).astype(jnp.int32),
        "counts": plant(jax.random.randint(arg_keys[5], (FACETS,), BLOCKS // 4, BLOCKS + 1), jax.random.fold_in(arg_keys[5], 1), BLOCKS // 4, BLOCKS).astype(jnp.int32),
        "neighbours": draw_neighbours(jax.random.fold_in(arg_keys[7], 71), 0),
    }


def reference(visibilities, kernels, delays, tile_of, plane_of, counts, neighbours):
    highest = lax.Precision.HIGHEST
    channel = jnp.arange(CHANNELS, dtype=jnp.float32)
    freq_turn = (2.0 * math.pi) * (1.0 + 0.5 * channel / CHANNELS)
    group_rows = math.gcd(BLOCKS, 64)

    def grid_facet(facet_id):
        vis_facet = lax.dynamic_index_in_dim(visibilities, facet_id, 1, keepdims=False)
        delay_facet = lax.dynamic_index_in_dim(delays, facet_id, 0, keepdims=False)
        tiles_facet = lax.dynamic_index_in_dim(tile_of, facet_id, 0, keepdims=False)
        planes_facet = lax.dynamic_index_in_dim(plane_of, facet_id, 0, keepdims=False)
        live_count = lax.dynamic_index_in_dim(counts, facet_id, 0, keepdims=False)

        def one_group(grid_acc, group_index):
            begin_row = (group_index * group_rows).astype(jnp.int32)
            vis_piece = lax.dynamic_slice_in_dim(vis_facet, begin_row, group_rows, 1).astype(jnp.float32)
            delay_piece = lax.dynamic_slice_in_dim(delay_facet, begin_row, group_rows, 0)
            phase_angle = delay_piece[:, None, :] * freq_turn[None, :, None]
            cosine = jnp.cos(phase_angle)
            sine_part = jnp.sin(phase_angle)
            rot_real = vis_piece[0] * cosine - vis_piece[1] * sine_part
            rot_imag = vis_piece[0] * sine_part + vis_piece[1] * cosine
            avg_real = jnp.mean(rot_real.reshape(group_rows, OUTCH, AVG, BV), axis=2)
            avg_imag = jnp.mean(rot_imag.reshape(group_rows, OUTCH, AVG, BV), axis=2)
            avg_rows = jnp.concatenate([avg_real, avg_imag], axis=-1).astype(jnp.bfloat16)
            plane_piece = lax.dynamic_slice_in_dim(planes_facet, begin_row, group_rows, 0).astype(jnp.int32)
            chosen = jnp.take(kernels, plane_piece, axis=0)
            contrib = jnp.einsum("gcv,gvx->gcx", avg_rows.astype(jnp.float32), chosen.astype(jnp.float32), precision=highest)
            block_ids = begin_row + jnp.arange(group_rows, dtype=jnp.int32)
            live_mask = (block_ids < live_count).astype(jnp.float32)
            tile_piece = lax.dynamic_slice_in_dim(tiles_facet, begin_row, group_rows, 0).astype(jnp.int32)
            grid_acc = grid_acc.at[tile_piece].add(contrib * live_mask[:, None, None])
            return grid_acc, None

        start_grid = jnp.zeros((NTILES, OUTCH, 2 * TILE), jnp.float32)
        grid_acc, unused = lax.scan(one_group, start_grid, jnp.arange(BLOCKS // group_rows, dtype=jnp.int32))
        return grid_acc

    facet_grids = lax.map(grid_facet, jnp.arange(FACETS, dtype=jnp.int32))
    facet_grids = jnp.transpose(facet_grids, (1, 0, 2, 3))
    edge_cells = EDGE * TS
    strips = jnp.concatenate([facet_grids[..., :edge_cells], facet_grids[..., TILE:TILE + edge_cells]], axis=-1)
    neighbour_strips = jnp.take(strips, neighbours.astype(jnp.int32), axis=1)
    blended = 0.25 * jnp.sum(neighbour_strips, axis=2)
    joined = facet_grids.at[..., TILE - edge_cells:TILE].add(blended[..., :edge_cells])
    joined = joined.at[..., 2 * TILE - edge_cells:].add(blended[..., edge_cells:])
    return joined
```

```python
import functools
import math

import jax
import jax.numpy as jnp
from jax import lax
from jax.experimental import pallas as pl
from jax.experimental.pallas import tpu as pltpu
from jax.sharding import PartitionSpec as P

AVG = 8
TS = 16
EDGE = 4
STRIP = EDGE * TS
CHUNKS = ((0, 0, 256), (0, 256, 256), (1, 0, 256), (1, 256, 256))

SIN = (-1.0 / 6, 1.0 / 120, -1.0 / 5040, 1.0 / 362880, -1.0 / 39916800)
COS = (-1.0 / 2, 1.0 / 24, -1.0 / 720, 1.0 / 40320, -1.0 / 3628800, 1.0 / 479001600)


def series(turns):
    x = (2.0 * math.pi) * turns
    y = x * x
    s = jnp.full_like(x, SIN[-1])
    for k in SIN[-2::-1]:
        s = s * y + k
    c = jnp.full_like(x, COS[-1])
    for k in COS[-2::-1]:
        c = c * y + k
    return c * y + 1.0, (s * y + 1.0) * x


def turn_by(turns):
    half = jnp.round(2.0 * turns)
    c, s = series(turns - 0.5 * half)
    odd = (half - 2.0 * jnp.floor(0.5 * half)) > 0.5
    sign = jnp.where(odd, -1.0, 1.0)
    return c * sign, s * sign


def times(a, b):
    return a[0] * b[0] - a[1] * b[1], a[0] * b[1] + a[1] * b[0]


def average_kernel(vis_ref, delay_ref, out_ref):
    n_out = out_ref.shape[0]
    rows = out_ref.shape[2]
    for r in range(0, rows, 16):
        d = delay_ref[r : r + 16, :]
        c0, s0 = turn_by(d)
        outer = (c0 * (1.0 / AVG), s0 * (1.0 / AVG))
        step = series(d * (1.0 / 32.0))
        small = series(d * (1.0 / 256.0))
        table = [None, small]
        for j in range(2, AVG):
            table.append(times(table[j // 2], table[j - j // 2]))

        def one(o, turn, r=r, table=table, step=step):
            c = o * AVG
            re = vis_ref[c, 0, r : r + 16, :].astype(jnp.float32)
            im = vis_ref[c, 1, r : r + 16, :].astype(jnp.float32)
            for j in range(1, AVG):
                a = vis_ref[c + j, 0, r : r + 16, :].astype(jnp.float32)
                b = vis_ref[c + j, 1, r : r + 16, :].astype(jnp.float32)
                tc, ts = table[j]
                re += a * tc - b * ts
                im += a * ts + b * tc
            tc, ts = turn
            out_ref[o, 0, r : r + 16, :] = (re * tc - im * ts).astype(jnp.bfloat16)
            out_ref[o, 1, r : r + 16, :] = (re * ts + im * tc).astype(jnp.bfloat16)
            return times(turn, step)

        lax.fori_loop(0, n_out, one, outer)


def average(vis, delay):
    n_ch, halves, rows, bv = vis.shape
    return pl.pallas_call(
        average_kernel,
        out_shape=jax.ShapeDtypeStruct((n_ch // AVG, halves, rows, bv), jnp.bfloat16),
        in_specs=[pl.BlockSpec(memory_space=pltpu.VMEM)] * 2,
        out_specs=pl.BlockSpec(memory_space=pltpu.VMEM),
        name="average",
    )(vis, delay)


def grid_kernel(last, first, *refs):
    if first:
        rows_ref, plane_ref, tile_ref, k_ref, *outs = refs
        before_ref = None
    else:
        rows_ref, plane_ref, tile_ref, k_ref, before_ref, *outs = refs
    acc_ref = outs[-1]
    p = pl.program_id(0)
    n_blocks = acc_ref.shape[0]
    bv = rows_ref.shape[3]

    mine = plane_ref[...] == p.astype(jnp.float32)
    re = rows_ref[:, 0].reshape(n_blocks, bv).astype(jnp.float32)
    im = rows_ref[:, 1].reshape(n_blocks, bv).astype(jnp.float32)
    x = jnp.concatenate([jnp.where(mine, re, 0.0), jnp.where(mine, im, 0.0)], axis=1)
    part = jnp.dot(x.astype(jnp.bfloat16), k_ref[0], preferred_element_type=jnp.float32)

    @pl.when(p == 0)
    def _():
        acc_ref[...] = part

    @pl.when(p > 0)
    def _():
        acc_ref[...] += part

    @pl.when(p == pl.num_programs(0) - 1)
    def _():
        n_tiles = outs[0].shape[0] * outs[0].shape[1] if last else outs[0].shape[0]
        ids = lax.broadcasted_iota(jnp.int32, (n_tiles, n_blocks), 0)
        table = (ids == tile_ref[...]).astype(jnp.float32).astype(jnp.bfloat16)
        contrib = acc_ref[...]
        high = contrib.astype(jnp.bfloat16)
        low = (contrib - high.astype(jnp.float32)).astype(jnp.bfloat16)
        grid = jnp.dot(table, high, preferred_element_type=jnp.float32)
        grid += jnp.dot(table, low, preferred_element_type=jnp.float32)
        if before_ref is not None:
            grid += before_ref[...]
        if last:
            cells = grid.shape[1]
            value = grid.astype(jnp.bfloat16)
            outs[0][...] = value.reshape(outs[0].shape)
            strip = jnp.concatenate([grid[:, :STRIP], grid[:, cells // 2 : cells // 2 + STRIP]], axis=1)
            strip = strip.astype(jnp.bfloat16).reshape(outs[1].shape[1:])
            for k in range(outs[1].shape[0]):
                outs[1][k] = strip
        else:
            outs[0][...] = grid


def grid_piece(rows, planes, tiles, kernels, before, last, n_tiles, n_facet):
    n_src, halves, per, bv = rows.shape
    n_blocks = n_src * per
    planes_n, k_rows, cells = kernels.shape
    whole = lambda *shape: pl.BlockSpec(shape, lambda p: (0,) * len(shape))
    in_specs = [
        whole(*rows.shape),
        whole(n_blocks, bv),
        whole(1, n_blocks),
        pl.BlockSpec((1, k_rows, cells), lambda p: (p, 0, 0)),
    ]
    args = [
        rows,
        jnp.broadcast_to(planes.astype(jnp.float32)[:, None], (n_blocks, bv)),
        tiles[None, :],
        kernels,
    ]
    if before is not None:
        in_specs.append(whole(n_tiles, cells))
        args.append(before)
    if last:
        t_dev = n_tiles // n_src
        shapes = [(n_src, t_dev, cells), (n_facet, n_src, t_dev, 2 * STRIP)]
        out_shape = [jax.ShapeDtypeStruct(s, jnp.bfloat16) for s in shapes]
        out_specs = [whole(*s) for s in shapes]
    else:
        out_shape = [jax.ShapeDtypeStruct((n_tiles, cells), jnp.float32)]
        out_specs = [whole(n_tiles, cells)]
    return pl.pallas_call(
        functools.partial(grid_kernel, last, before is None),
        grid=(planes_n,),
        out_shape=out_shape,
        in_specs=in_specs,
        out_specs=out_specs,
        scratch_shapes=[pltpu.VMEM((n_blocks, cells), jnp.float32)],
        name="grid_last" if last else "grid_part",
    )(*args)


def join_kernel(nb_ref, main0_ref, main1_ref, strip0_ref, strip1_ref, out_ref):
    n_out, t_dev, cells = main0_ref.shape
    half = cells // 2
    n_rows = n_out * t_dev
    to = lax.broadcasted_iota(jnp.int32, (n_rows, n_rows), 0)
    source = lax.broadcasted_iota(jnp.int32, (n_rows, n_rows), 1)
    place = (source == (to % n_out) * t_dev + to // n_out).astype(jnp.float32)
    quarter = (0.25 * place).astype(jnp.bfloat16)
    place = place.astype(jnp.bfloat16)
    upper = lax.broadcasted_iota(jnp.int32, (n_rows, 2 * STRIP), 1) >= STRIP
    for slot, main_ref in enumerate((main0_ref, main1_ref)):
        blend = jnp.zeros((n_rows, 2 * STRIP), jnp.float32)
        for k in range(nb_ref.shape[1]):
            nb = nb_ref[slot, k]
            odd = nb % 2 == 1
            a = strip0_ref[nb // 2].reshape(n_rows, 2 * STRIP)
            b = strip1_ref[nb // 2].reshape(n_rows, 2 * STRIP)
            blend += jnp.dot(quarter, jnp.where(odd, b, a), preferred_element_type=jnp.float32)
        swapped = pltpu.roll(blend, STRIP, 1)
        main = main_ref[...].reshape(n_rows, cells)
        main = jnp.dot(place, main, preferred_element_type=jnp.float32)

        def put(lo, hi, value, slot=slot):
            out_ref[:, slot, :, lo:hi] = value.reshape(t_dev, n_out, hi - lo)

        put(0, half - 128, main[:, 0 : half - 128])
        put(half - 128, half, main[:, half - 128 : half] + jnp.where(upper, swapped, 0.0))
        put(half, cells - 128, main[:, half : cells - 128])
        put(cells - 128, cells, main[:, cells - 128 :] + jnp.where(upper, blend, 0.0))


def join(my_neighbours, mains, strips):
    n_out, t_dev, cells = mains[0].shape
    return pl.pallas_call(
        join_kernel,
        out_shape=jax.ShapeDtypeStruct((t_dev, 2, n_out, cells), jnp.float32),
        in_specs=[pl.BlockSpec(memory_space=pltpu.SMEM)] + [pl.BlockSpec(memory_space=pltpu.VMEM)] * 4,
        out_specs=pl.BlockSpec(memory_space=pltpu.VMEM),
        name="join",
    )(my_neighbours, *mains, *strips)


def exchange(x, axis):
    return lax.all_to_all(x, axis, split_axis=0, concat_axis=0, tiled=True)


def local(visibilities, kernels, delays, tile_of, plane_of, counts, neighbours):
    n_facet = lax.axis_size("facet")
    n_chan = lax.axis_size("chan")
    facet_index = lax.axis_index("facet")
    chan_index = lax.axis_index("chan")
    halves, facets, blocks, _, bv = visibilities.shape
    fac_dev = facets // n_facet
    n_tiles = 16 * n_chan
    cells = kernels.shape[2]
    vis = visibilities.reshape(halves, n_facet, fac_dev, blocks, bv)
    live = jnp.arange(blocks, dtype=jnp.int32)[None, :] < counts[:, None]
    planes = jnp.where(live, plane_of, -1)

    arrived = []
    for slot, begin, length in CHUNKS:
        per = length // n_chan
        piece = lax.slice_in_dim(vis[:, :, slot], begin, begin + length, axis=2)
        piece = piece.reshape(halves, n_facet, n_chan, per, bv)
        piece = jnp.transpose(piece, (1, 2, 0, 3, 4)).reshape(n_facet * n_chan, halves, per, bv)
        arrived.append(exchange(piece, ("facet", "chan")))

    mains, strips = [], []
    part = None
    for index, (slot, begin, length) in enumerate(CHUNKS):
        per = length // n_chan
        delay = lax.dynamic_slice(delays[slot], (begin + chan_index * per, 0), (per, bv))
        rows = exchange(average(arrived[index], delay), "chan")
        last = index + 1 == len(CHUNKS) or CHUNKS[index + 1][0] != slot
        result = grid_piece(
            rows,
            planes[slot, begin : begin + length],
            tile_of[slot, begin : begin + length],
            kernels,
            part,
            last,
            n_tiles,
            n_facet,
        )
        if last:
            part = None
            mains.append(exchange(result[0], "chan"))
            strip = result[1].reshape(n_facet * n_chan, n_tiles // n_chan, 2 * STRIP)
            strip = exchange(strip, ("facet", "chan"))
            strips.append(strip.reshape(n_facet, n_chan, n_tiles // n_chan, 2 * STRIP))
        else:
            part = result[0]
    my_neighbours = lax.dynamic_slice_in_dim(neighbours, facet_index * fac_dev, fac_dev, 0)
    return join(my_neighbours, mains, strips)


def solution(mesh):
    return jax.shard_map(
        local,
        mesh=mesh,
        in_specs=(
            P(None, None, None, ("facet", "chan"), None),
            P(),
            P("facet", None, None),
            P("facet", None),
            P("facet", None),
            P("facet"),
            P(),
        ),
        out_specs=P("chan", "facet", None, None),
        check_vma=False,
    )
```

```python
import functools
import math

import jax
import jax.numpy as jnp
from jax import lax
from jax.experimental import pallas as pl
from jax.experimental.pallas import tpu as pltpu
from jax.sharding import PartitionSpec as P

AVG = 8
TS = 16
EDGE = 4
STRIP = EDGE * TS
GROUP = 16
PIECE = 64
MIB = 1024 * 1024

SIN = (-1.0 / 6, 1.0 / 120, -1.0 / 5040, 1.0 / 362880, -1.0 / 39916800)
COS = (-1.0 / 2, 1.0 / 24, -1.0 / 720, 1.0 / 40320, -1.0 / 3628800, 1.0 / 479001600)


def series(turns):
    x = (2.0 * math.pi) * turns
    y = x * x
    s = jnp.full_like(x, SIN[-1])
    for k in SIN[-2::-1]:
        s = s * y + k
    c = jnp.full_like(x, COS[-1])
    for k in COS[-2::-1]:
        c = c * y + k
    return c * y + 1.0, (s * y + 1.0) * x


def turn_by(turns):
    half = jnp.round(2.0 * turns)
    c, s = series(turns - 0.5 * half)
    odd = (half - 2.0 * jnp.floor(0.5 * half)) > 0.5
    sign = jnp.where(odd, -1.0, 1.0)
    return c * sign, s * sign


def times(a, b):
    return a[0] * b[0] - a[1] * b[1], a[0] * b[1] + a[1] * b[0]


def vmem():
    return pl.BlockSpec(memory_space=pltpu.VMEM)


def send_kernel(vis_ref, out_ref, sem):
    copies = [
        pltpu.make_async_copy(vis_ref.at[h], out_ref.at[:, h], sem.at[h]) for h in range(vis_ref.shape[0])
    ]
    for copy in copies:
        copy.start()
    for copy in copies:
        copy.wait()


def send_order(vis):
    halves, dests, rows, bv = vis.shape
    return pl.pallas_call(
        send_kernel,
        out_shape=jax.ShapeDtypeStruct((dests, halves, rows, bv), vis.dtype),
        in_specs=[pl.BlockSpec(memory_space=pl.ANY)],
        out_specs=pl.BlockSpec(memory_space=pl.ANY),
        scratch_shapes=[pltpu.SemaphoreType.DMA((halves,))],
        compiler_params=pltpu.CompilerParams(vmem_limit_bytes=1 * MIB),
        name="send_order",
    )(vis)


def turns_kernel(delay_ref, inner_ref, outer_ref):
    d = delay_ref[...]
    small = series(d * (1.0 / 256.0))
    table = [None, small]
    for j in range(2, AVG):
        table.append(times(table[j // 2], table[j - j // 2]))
    for j in range(1, AVG):
        inner_ref[j - 1, 0] = table[j][0]
        inner_ref[j - 1, 1] = table[j][1]
    c, s = turn_by(d)
    turn = (c * (1.0 / AVG), s * (1.0 / AVG))
    step = series(d * (1.0 / 32.0))
    for o in range(outer_ref.shape[0]):
        outer_ref[o, 0] = turn[0]
        outer_ref[o, 1] = turn[1]
        turn = times(turn, step)


def turns(delay, n_out):
    rows, bv = delay.shape
    return pl.pallas_call(
        turns_kernel,
        out_shape=[
            jax.ShapeDtypeStruct((AVG - 1, 2, rows, bv), jnp.float32),
            jax.ShapeDtypeStruct((n_out, 2, rows, bv), jnp.float32),
        ],
        in_specs=[vmem()],
        out_specs=[vmem()] * 2,
        compiler_params=pltpu.CompilerParams(vmem_limit_bytes=8 * MIB),
        name="turns",
    )(delay)


def average_kernel(vis_ref, inner_ref, outer_ref, out_ref):
    n_out, _, rows, _ = out_ref.shape
    for r in range(0, rows, 16):
        at = slice(r, r + 16)
        table = [(inner_ref[j, 0, at], inner_ref[j, 1, at]) for j in range(AVG - 1)]

        def one(o, carry, at=at, table=table):
            c = o * AVG
            re = vis_ref[c, 0, at].astype(jnp.float32)
            im = vis_ref[c, 1, at].astype(jnp.float32)
            for j in range(1, AVG):
                a = vis_ref[c + j, 0, at].astype(jnp.float32)
                b = vis_ref[c + j, 1, at].astype(jnp.float32)
                tc, ts = table[j - 1]
                re += a * tc - b * ts
                im += a * ts + b * tc
            tc = outer_ref[o, 0, at]
            ts = outer_ref[o, 1, at]
            out_ref[o, 0, at] = (re * tc - im * ts).astype(jnp.bfloat16)
            out_ref[o, 1, at] = (re * ts + im * tc).astype(jnp.bfloat16)
            return carry

        lax.fori_loop(0, n_out, one, 0, unroll=4)


def average(vis, inner, outer):
    n_ch, halves, rows, bv = vis.shape
    return pl.pallas_call(
        average_kernel,
        out_shape=jax.ShapeDtypeStruct((n_ch // AVG, halves, rows, bv), jnp.bfloat16),
        in_specs=[vmem()] * 3,
        out_specs=vmem(),
        compiler_params=pltpu.CompilerParams(vmem_limit_bytes=12 * MIB),
        name="average",
    )(vis, inner, outer)


def to_bf16(mask):
    return mask.astype(jnp.float32).astype(jnp.bfloat16)


def tables_kernel(n_planes, n_tiles, t_dev, plane_ref, tile_ref, order_ref, tiles_ref, piece_ref):
    n_rows = plane_ref.shape[1]
    f32 = jnp.float32
    iota = lambda shape, dim: lax.broadcasted_iota(jnp.int32, shape, dim)
    plane = plane_ref[...]
    mine = plane == iota((n_planes, n_rows), 0)
    before = to_bf16(iota((n_rows, n_rows), 0) < iota((n_rows, n_rows), 1))
    rank = jnp.dot(to_bf16(mine), before, preferred_element_type=f32)
    count = jnp.sum(mine.astype(f32), axis=1, keepdims=True)
    groups = jnp.floor((count + (GROUP - 1)) * (1.0 / GROUP))
    pieces = jnp.floor((groups + (PIECE // GROUP - 1)) * (GROUP / PIECE))
    earlier = to_bf16(iota((n_planes, n_planes), 1) < iota((n_planes, n_planes), 0))
    both = jnp.concatenate(
        [jnp.broadcast_to(groups, (n_planes, 128)), jnp.broadcast_to(pieces, (n_planes, 128))], axis=1
    )
    both = jnp.dot(earlier, both.astype(jnp.bfloat16), preferred_element_type=f32)
    first_group = both[:, 0:1]
    first_piece = both[:, 128:129]
    place = jnp.sum(jnp.where(mine, rank + GROUP * first_group, 0.0), axis=0, keepdims=True)
    live = jnp.sum(mine.astype(f32), axis=0, keepdims=True)
    place = jnp.where(live > 0.5, place, -1.0).astype(jnp.int32)
    n_order = order_ref.shape[0]
    order = to_bf16(iota((n_order, n_rows), 0) == place)
    order_ref[...] = order

    row = iota((8, n_rows), 0)
    slot = (iota((8, n_rows), 1) >= n_rows // 2).astype(f32)
    values = jnp.where(row == 0, tile_ref[...].astype(f32) + 1.0, jnp.where(row == 1, slot, 0.0))
    n_used = tiles_ref.shape[1]
    ordered = lax.dot_general(
        values.astype(jnp.bfloat16), order[:n_used], (((1,), (1,)), ((), ())), preferred_element_type=f32
    )
    tile = ordered[0:1].astype(jnp.int32) - 1
    slot = ordered[1:2].astype(jnp.int32)
    code = (tile // t_dev) * (2 * t_dev) + slot * t_dev + tile % t_dev
    code = jnp.where(tile < 0, -1, code)
    tiles_ref[...] = to_bf16(iota((2 * n_tiles, n_used), 0) == code)

    total = jnp.sum(pieces)
    which = jnp.minimum(iota((n_planes, 128), 1).astype(f32), total - 1.0)
    taken = (which >= first_piece) & (which < first_piece + pieces)
    group = first_group + (PIECE // GROUP) * (which - first_piece)
    group = jnp.sum(jnp.where(taken, group, 0.0), axis=0, keepdims=True)
    owner = jnp.sum(jnp.where(taken, iota((n_planes, 128), 0).astype(f32), 0.0), axis=0, keepdims=True)
    row = iota((8, 128), 0)
    piece_ref[...] = jnp.where(row == 0, group, jnp.where(row == 1, owner, 0.0)).astype(jnp.int32)


def tables(planes, tiles, n_planes, n_tiles, t_dev):
    n_rows = planes.shape[1]
    used = n_rows + n_planes * (GROUP - 1)
    n_order = -(-(used - GROUP + PIECE) // 32) * 32
    n_used = -(-used // 256) * 256
    assert n_used <= n_order
    return pl.pallas_call(
        functools.partial(tables_kernel, n_planes, n_tiles, t_dev),
        out_shape=[
            jax.ShapeDtypeStruct((n_order, n_rows), jnp.bfloat16),
            jax.ShapeDtypeStruct((2 * n_tiles, n_used), jnp.bfloat16),
            jax.ShapeDtypeStruct((8, 128), jnp.int32),
        ],
        in_specs=[vmem()] * 2,
        out_specs=[vmem()] * 3,
        compiler_params=pltpu.CompilerParams(vmem_limit_bytes=40 * MIB),
        name="tables",
    )(planes, tiles)


def grid_kernel(n_pieces, piece_ref, rows_ref, order_ref, tiles_ref, k_ref, out_ref, x_ref, c_ref):
    n_src, _, per, bv = rows_ref.shape
    re = rows_ref[:, 0].reshape(n_src * per, bv)
    im = rows_ref[:, 1].reshape(n_src * per, bv)
    x = jnp.concatenate([re, im], axis=1)
    x_ref[...] = jnp.dot(order_ref[...], x, preferred_element_type=jnp.float32).astype(jnp.bfloat16)
    n_used = tiles_ref.shape[1]
    c_ref[...] = jnp.zeros_like(c_ref)
    for i in range(n_pieces):
        at = pl.ds(pl.multiple_of(piece_ref[0, i] * GROUP, GROUP), PIECE)
        product = jnp.dot(x_ref[at, :], k_ref[piece_ref[1, i]], preferred_element_type=jnp.float32)
        c_ref[at, :] = product.astype(jnp.bfloat16)
    grid = jnp.dot(tiles_ref[...], c_ref[:n_used, :], preferred_element_type=jnp.float32)
    out_ref[...] = grid.astype(jnp.bfloat16).reshape(out_ref.shape)


def grid_rows(piece, rows, order, tiles, kernels, n_chan):
    n_planes, k_rows, cells = kernels.shape
    n_order, n_rows = order.shape
    return pl.pallas_call(
        functools.partial(grid_kernel, n_rows // PIECE + n_planes),
        out_shape=jax.ShapeDtypeStruct((n_chan, tiles.shape[0] // n_chan, cells), jnp.bfloat16),
        in_specs=[pl.BlockSpec(memory_space=pltpu.SMEM)] + [vmem()] * 4,
        out_specs=vmem(),
        scratch_shapes=[
            pltpu.VMEM((n_order, k_rows), jnp.bfloat16),
            pltpu.VMEM((n_order, cells), jnp.bfloat16),
        ],
        compiler_params=pltpu.CompilerParams(vmem_limit_bytes=40 * MIB),
        name="grid_rows",
    )(piece, rows, order, tiles, kernels)


def strip_kernel(main_ref, out_ref):
    n_out, per, cells = main_ref.shape
    half = cells // 2
    low = main_ref[:, :, 0:128].reshape(n_out * per, 128).astype(jnp.float32)
    high = main_ref[:, :, half : half + 128].reshape(n_out * per, 128).astype(jnp.float32)
    lane = lax.broadcasted_iota(jnp.int32, low.shape, 1)
    strip = jnp.where(lane < STRIP, low, pltpu.roll(high, STRIP, 1)).astype(jnp.bfloat16)
    for k in range(out_ref.shape[0]):
        out_ref[k] = strip.reshape(out_ref.shape[1:])


def strips_for_each(main, n_facet):
    n_out, per, _ = main.shape
    return pl.pallas_call(
        strip_kernel,
        out_shape=jax.ShapeDtypeStruct((n_facet, n_out, per, 2 * STRIP), jnp.bfloat16),
        in_specs=[vmem()],
        out_specs=vmem(),
        compiler_params=pltpu.CompilerParams(vmem_limit_bytes=12 * MIB),
        name="strips",
    )(main)


def join_kernel(nb_ref, main_ref, strip_ref, out_ref):
    n_out, per, cells = main_ref.shape
    t_dev = per // 2
    half = cells // 2
    n_rows = n_out * t_dev
    iota = lambda shape, dim: lax.broadcasted_iota(jnp.int32, shape, dim)
    upper = iota((n_rows, 2 * STRIP), 1) >= STRIP
    to = iota((n_rows, n_rows), 0)
    place = (iota((n_rows, n_rows), 1) == (to % n_out) * t_dev + to // n_out).astype(jnp.float32)
    quarter = (0.25 * place).astype(jnp.bfloat16)
    place = place.astype(jnp.bfloat16)
    for slot in range(2):
        blend = jnp.zeros((n_rows, 2 * STRIP), jnp.float32)
        for k in range(nb_ref.shape[1]):
            nb = nb_ref[slot, k]
            strip = strip_ref[nb // 2, :, nb % 2].reshape(n_rows, 2 * STRIP)
            blend += jnp.dot(quarter, strip, preferred_element_type=jnp.float32)
        swapped = pltpu.roll(blend, STRIP, 1)
        main = main_ref[:, slot * t_dev : (slot + 1) * t_dev, :].reshape(n_rows, cells)
        main = jnp.dot(place, main, preferred_element_type=jnp.float32)

        def put(lo, hi, value, slot=slot):
            out_ref[:, slot, :, lo:hi] = value.reshape(t_dev, n_out, hi - lo)

        put(0, half - 128, main[:, 0 : half - 128])
        put(half - 128, half, main[:, half - 128 : half] + jnp.where(upper, swapped, 0.0))
        put(half, cells - 128, main[:, half : cells - 128])
        put(cells - 128, cells, main[:, cells - 128 :] + jnp.where(upper, blend, 0.0))


def join(my_neighbours, main, strips):
    n_out, per, cells = main.shape
    n_facet = strips.shape[0]
    strips = strips.reshape(n_facet, n_out, 2, per // 2, 2 * STRIP)
    return pl.pallas_call(
        join_kernel,
        out_shape=jax.ShapeDtypeStruct((per // 2, 2, n_out, cells), jnp.float32),
        in_specs=[pl.BlockSpec(memory_space=pltpu.SMEM)] + [vmem()] * 2,
        out_specs=vmem(),
        compiler_params=pltpu.CompilerParams(vmem_limit_bytes=16 * MIB),
        name="join",
    )(my_neighbours, main, strips)


def exchange(x, axis):
    return lax.all_to_all(x, axis, split_axis=0, concat_axis=0, tiled=True)


def local(visibilities, kernels, delays, tile_of, plane_of, counts, neighbours):
    n_facet = lax.axis_size("facet")
    n_chan = lax.axis_size("chan")
    facet_index = lax.axis_index("facet")
    chan_index = lax.axis_index("chan")
    halves, facets, blocks, _, bv = visibilities.shape
    fac_dev = facets // n_facet
    n_out = n_chan
    n_tiles = 16 * n_chan
    t_dev = n_tiles // n_chan
    n_rows = fac_dev * blocks
    per = n_rows // n_chan

    vis = send_order(visibilities.reshape(halves, n_facet * n_chan, per, bv))
    vis = exchange(vis, ("facet", "chan"))
    delay = lax.dynamic_index_in_dim(delays.reshape(n_chan, per, bv), chan_index, 0, keepdims=False)
    inner, outer = turns(delay, n_out)
    live = jnp.arange(blocks, dtype=jnp.int32)[None, :] < counts[:, None]
    planes = jnp.where(live, plane_of, -1).reshape(1, n_rows)
    order, tiles, piece = tables(planes, tile_of.reshape(1, n_rows), kernels.shape[0], n_tiles, t_dev)

    rows = exchange(average(vis, inner, outer), "chan")
    grids = grid_rows(piece, rows, order, tiles, kernels, n_chan)
    main = exchange(grids, "chan")
    strips = exchange(strips_for_each(main, n_facet), "facet")
    my_neighbours = lax.dynamic_slice_in_dim(neighbours, facet_index * fac_dev, fac_dev, 0)
    return join(my_neighbours, main, strips)


def solution(mesh):
    return jax.shard_map(
        local,
        mesh=mesh,
        in_specs=(
            P(None, None, None, ("facet", "chan"), None),
            P(),
            P("facet", None, None),
            P("facet", None),
            P("facet", None),
            P("facet"),
            P(),
        ),
        out_specs=P("chan", "facet", None, None),
        check_vma=False,
    )
```

```python
import functools
import math

import jax
import jax.numpy as jnp
from jax import lax
from jax.experimental import pallas as pl
from jax.experimental.pallas import tpu as pltpu
from jax.sharding import PartitionSpec as P

AVG = 8
TS = 16
EDGE = 4
STRIP = EDGE * TS
GROUP = 16
PIECE = 64
MIB = 1024 * 1024

SIN = (-1.0 / 6, 1.0 / 120, -1.0 / 5040, 1.0 / 362880, -1.0 / 39916800)
COS = (-1.0 / 2, 1.0 / 24, -1.0 / 720, 1.0 / 40320, -1.0 / 3628800, 1.0 / 479001600)


def series(turns):
    x = (2.0 * math.pi) * turns
    y = x * x
    s = jnp.full_like(x, SIN[-1])
    for k in SIN[-2::-1]:
        s = s * y + k
    c = jnp.full_like(x, COS[-1])
    for k in COS[-2::-1]:
        c = c * y + k
    return c * y + 1.0, (s * y + 1.0) * x


def turn_by(turns):
    half = jnp.round(2.0 * turns)
    c, s = series(turns - 0.5 * half)
    odd = (half - 2.0 * jnp.floor(0.5 * half)) > 0.5
    sign = jnp.where(odd, -1.0, 1.0)
    return c * sign, s * sign


def times(a, b):
    return a[0] * b[0] - a[1] * b[1], a[0] * b[1] + a[1] * b[0]


def vmem():
    return pl.BlockSpec(memory_space=pltpu.VMEM)


def send_kernel(vis_ref, out_ref, sem):
    halves, dests = vis_ref.shape[:2]
    n = sem.shape[1]
    copies = []
    for h in range(halves):
        for i in range(n):
            at = pl.ds(i * (dests // n), dests // n)
            copies.append(pltpu.make_async_copy(vis_ref.at[h, at], out_ref.at[at, h], sem.at[h, i]))
    for copy in copies:
        copy.start()
    for copy in copies:
        copy.wait()


def send_order(vis):
    halves, dests, rows, bv = vis.shape
    return pl.pallas_call(
        send_kernel,
        out_shape=pltpu.HBM((dests, halves, rows, bv), vis.dtype),
        in_specs=[pl.BlockSpec(memory_space=pltpu.HBM)],
        out_specs=pl.BlockSpec(memory_space=pltpu.HBM),
        scratch_shapes=[pltpu.SemaphoreType.DMA((halves, 4))],
        compiler_params=pltpu.CompilerParams(vmem_limit_bytes=1 * MIB),
        name="send_order",
    )(pltpu.with_memory_space_constraint(vis, pltpu.HBM))


def fill_turns(d, inner_ref, outer_ref):
    small = series(d * (1.0 / 256.0))
    table = [None, small]
    for j in range(2, AVG):
        table.append(times(table[j // 2], table[j - j // 2]))
    for j in range(1, AVG):
        inner_ref[j - 1, 0] = table[j][0]
        inner_ref[j - 1, 1] = table[j][1]
    c, s = turn_by(d)
    turn = (c * (1.0 / AVG), s * (1.0 / AVG))
    step = series(d * (1.0 / 32.0))
    for o in range(outer_ref.shape[0]):
        outer_ref[o, 0] = turn[0]
        outer_ref[o, 1] = turn[1]
        turn = times(turn, step)


def average_kernel(piece_ref, delay_ref, vis_hbm, out_ref, vis_ref, inner_ref, outer_ref, sem):
    n_out, _, rows, _ = out_ref.shape
    steps = sem.shape[0]
    size = vis_ref.shape[0] // steps
    copies = []
    for i in range(steps):
        at = pl.ds(i * size, size)
        copies.append(pltpu.make_async_copy(vis_hbm.at[at], vis_ref.at[at], sem.at[i]))
        copies[-1].start()
    fill_turns(delay_ref[...], inner_ref, outer_ref)
    for i in range(steps):
        copies[i].wait()
        for r in range(0, rows, 16):
            at = slice(r, r + 16)
            table = [(inner_ref[j, 0, at], inner_ref[j, 1, at]) for j in range(AVG - 1)]

            def one(o, carry, at=at, table=table):
                c = o * AVG
                re = vis_ref[c, 0, at].astype(jnp.float32)
                im = vis_ref[c, 1, at].astype(jnp.float32)
                for j in range(1, AVG):
                    a = vis_ref[c + j, 0, at].astype(jnp.float32)
                    b = vis_ref[c + j, 1, at].astype(jnp.float32)
                    tc, ts = table[j - 1]
                    re += a * tc - b * ts
                    im += a * ts + b * tc
                tc = outer_ref[o, 0, at]
                ts = outer_ref[o, 1, at]
                out_ref[o, 0, at] = (re * tc - im * ts).astype(jnp.bfloat16)
                out_ref[o, 1, at] = (re * ts + im * tc).astype(jnp.bfloat16)
                return carry

            n = n_out // steps
            lax.fori_loop(i * n, (i + 1) * n, one, 0, unroll=n)


def average(piece, vis, delay):
    n_ch, halves, rows, bv = vis.shape
    n_out = n_ch // AVG
    return pl.pallas_call(
        average_kernel,
        out_shape=jax.ShapeDtypeStruct((n_out, halves, rows, bv), jnp.bfloat16),
        in_specs=[vmem(), vmem(), pl.BlockSpec(memory_space=pltpu.HBM)],
        out_specs=vmem(),
        scratch_shapes=[
            pltpu.VMEM(vis.shape, vis.dtype),
            pltpu.VMEM((AVG - 1, 2, rows, bv), jnp.float32),
            pltpu.VMEM((n_out, 2, rows, bv), jnp.float32),
            pltpu.SemaphoreType.DMA((4,)),
        ],
        compiler_params=pltpu.CompilerParams(vmem_limit_bytes=12 * MIB),
        name="average",
    )(piece, delay, pltpu.with_memory_space_constraint(vis, pltpu.HBM))


def to_bf16(mask):
    return mask.astype(jnp.float32).astype(jnp.bfloat16)


def iota(shape, dim):
    return lax.broadcasted_iota(jnp.int32, shape, dim)


def tables_kernel(n_planes, n_order, t_dev, plane_ref, tile_ref, place_ref, code_ref, piece_ref):
    n_rows = plane_ref.shape[1]
    f32 = jnp.float32
    plane = plane_ref[...]
    mine = plane == iota((n_planes, n_rows), 0)
    before = to_bf16(iota((n_rows, n_rows), 0) < iota((n_rows, n_rows), 1))
    rank = jnp.dot(to_bf16(mine), before, preferred_element_type=f32)
    count = jnp.sum(mine.astype(f32), axis=1, keepdims=True)
    groups = jnp.floor((count + (GROUP - 1)) * (1.0 / GROUP))
    pieces = jnp.floor((groups + (PIECE // GROUP - 1)) * (GROUP / PIECE))
    earlier = to_bf16(iota((n_planes, n_planes), 1) < iota((n_planes, n_planes), 0))
    both = jnp.concatenate(
        [jnp.broadcast_to(groups, (n_planes, 128)), jnp.broadcast_to(pieces, (n_planes, 128))], axis=1
    )
    both = jnp.dot(earlier, both.astype(jnp.bfloat16), preferred_element_type=f32)
    first_group = both[:, 0:1]
    first_piece = both[:, 128:129]
    place = jnp.sum(jnp.where(mine, rank + GROUP * first_group, 0.0), axis=0, keepdims=True)
    live = jnp.sum(mine.astype(f32), axis=0, keepdims=True)
    place = jnp.where(live > 0.5, place, -1.0).astype(jnp.int32)
    place_ref[...] = place
    order = to_bf16(iota((n_order, n_rows), 0) == place)

    row = iota((8, n_rows), 0)
    slot = (iota((8, n_rows), 1) >= n_rows // 2).astype(f32)
    values = jnp.where(row == 0, tile_ref[...].astype(f32) + 1.0, jnp.where(row == 1, slot, 0.0))
    n_used = code_ref.shape[1]
    ordered = lax.dot_general(
        values.astype(jnp.bfloat16), order[:n_used], (((1,), (1,)), ((), ())), preferred_element_type=f32
    )
    tile = ordered[0:1].astype(jnp.int32) - 1
    slot = ordered[1:2].astype(jnp.int32)
    code = (tile // t_dev) * (2 * t_dev) + slot * t_dev + tile % t_dev
    code_ref[...] = jnp.where(tile < 0, -1, code)

    total = jnp.sum(pieces)
    which = jnp.minimum(iota((n_planes, 128), 1).astype(f32), total - 1.0)
    taken = (which >= first_piece) & (which < first_piece + pieces)
    group = first_group + (PIECE // GROUP) * (which - first_piece)
    group = jnp.sum(jnp.where(taken, group, 0.0), axis=0, keepdims=True)
    owner = jnp.sum(jnp.where(taken, iota((n_planes, 128), 0).astype(f32), 0.0), axis=0, keepdims=True)
    row = iota((8, 128), 0)
    piece_ref[...] = jnp.where(row == 0, group, jnp.where(row == 1, owner, 0.0)).astype(jnp.int32)


def sizes(n_rows, n_planes):
    used = n_rows + n_planes * (GROUP - 1)
    n_order = -(-(used - GROUP + PIECE) // 32) * 32
    n_used = -(-used // 256) * 256
    assert n_used <= n_order
    return n_order, n_used


def tables(planes, tiles, n_planes, t_dev):
    n_rows = planes.shape[1]
    n_order, n_used = sizes(n_rows, n_planes)
    return pl.pallas_call(
        functools.partial(tables_kernel, n_planes, n_order, t_dev),
        out_shape=[
            jax.ShapeDtypeStruct((1, n_rows), jnp.int32),
            jax.ShapeDtypeStruct((1, n_used), jnp.int32),
            jax.ShapeDtypeStruct((8, 128), jnp.int32),
        ],
        in_specs=[vmem()] * 2,
        out_specs=[vmem()] * 3,
        compiler_params=pltpu.CompilerParams(vmem_limit_bytes=40 * MIB),
        name="tables",
    )(planes, tiles)


def grid_kernel(n_pieces, piece_ref, place_ref, code_ref, rows_ref, k_hbm, out_ref, k_ref, x_ref, c_ref, sem):
    n_fetch = sem.shape[0]
    part = k_ref.shape[0] // n_fetch
    fetches = []
    for i in range(n_fetch):
        at = pl.ds(i * part, part)
        fetches.append(pltpu.make_async_copy(k_hbm.at[at], k_ref.at[at], sem.at[i]))
        fetches[-1].start()
    n_src, _, per, bv = rows_ref.shape
    n_order = x_ref.shape[0]
    re = rows_ref[:, 0].reshape(n_src * per, bv)
    im = rows_ref[:, 1].reshape(n_src * per, bv)
    x = jnp.concatenate([re, im], axis=1)
    order = to_bf16(iota((n_order, n_src * per), 0) == place_ref[...])
    x_ref[...] = jnp.dot(order, x, preferred_element_type=jnp.float32).astype(jnp.bfloat16)
    n_used = code_ref.shape[1]
    n_codes = out_ref.shape[0] * out_ref.shape[1]
    tiles = to_bf16(iota((n_codes, n_used), 0) == code_ref[...])
    c_ref[...] = jnp.zeros_like(c_ref)
    for fetch in fetches:
        fetch.wait()
    for i in range(n_pieces):
        at = pl.ds(pl.multiple_of(piece_ref[0, i] * GROUP, GROUP), PIECE)
        product = jnp.dot(x_ref[at, :], k_ref[piece_ref[1, i]], preferred_element_type=jnp.float32)
        c_ref[at, :] = product.astype(jnp.bfloat16)
    grid = jnp.dot(tiles, c_ref[:n_used, :], preferred_element_type=jnp.float32)
    out_ref[...] = grid.astype(jnp.bfloat16).reshape(out_ref.shape)


def grid_rows(piece, place, code, rows, kernels, n_codes):
    n_planes, k_rows, cells = kernels.shape
    n_rows = place.shape[1]
    n_chan = rows.shape[0]
    n_order, n_used = sizes(n_rows, n_planes)
    return pl.pallas_call(
        functools.partial(grid_kernel, n_rows // PIECE + n_planes),
        out_shape=jax.ShapeDtypeStruct((n_chan, n_codes // n_chan, cells), jnp.bfloat16),
        in_specs=[pl.BlockSpec(memory_space=pltpu.SMEM)] + [vmem()] * 3 + [pl.BlockSpec(memory_space=pltpu.HBM)],
        out_specs=vmem(),
        scratch_shapes=[
            pltpu.VMEM(kernels.shape, kernels.dtype),
            pltpu.VMEM((n_order, k_rows), jnp.bfloat16),
            pltpu.VMEM((n_order, cells), jnp.bfloat16),
            pltpu.SemaphoreType.DMA((8,)),
        ],
        compiler_params=pltpu.CompilerParams(vmem_limit_bytes=40 * MIB),
        name="grid_rows",
    )(piece, place, code, rows, pltpu.with_memory_space_constraint(kernels, pltpu.HBM))


def strip_kernel(main_ref, out_ref):
    n_out, per, cells = main_ref.shape
    half = cells // 2
    low = main_ref[:, :, 0:128].reshape(n_out * per, 128).astype(jnp.float32)
    high = main_ref[:, :, half : half + 128].reshape(n_out * per, 128).astype(jnp.float32)
    lane = lax.broadcasted_iota(jnp.int32, low.shape, 1)
    strip = jnp.where(lane < STRIP, low, pltpu.roll(high, STRIP, 1)).astype(jnp.bfloat16)
    out_ref[...] = strip.reshape(out_ref.shape)


def strips_of(main):
    n_out, per, _ = main.shape
    return pl.pallas_call(
        strip_kernel,
        out_shape=jax.ShapeDtypeStruct((n_out, per, 2 * STRIP), jnp.bfloat16),
        in_specs=[vmem()],
        out_specs=vmem(),
        compiler_params=pltpu.CompilerParams(vmem_limit_bytes=8 * MIB),
        name="strips",
    )(main)


def join_kernel(nb_ref, main_ref, *refs):
    strips, out_ref, strip_ref = refs[:-2], refs[-2], refs[-1]
    n_out, per, cells = main_ref.shape
    t_dev = per // 2
    half = cells // 2
    n_rows = n_out * t_dev
    for i, ref in enumerate(strips):
        strip_ref[i] = ref[...].reshape(strip_ref.shape[1:])
    upper = iota((n_rows, 2 * STRIP), 1) >= STRIP
    to = iota((n_rows, n_rows), 0)
    place = (iota((n_rows, n_rows), 1) == (to % n_out) * t_dev + to // n_out).astype(jnp.float32)
    quarter = (0.25 * place).astype(jnp.bfloat16)
    place = place.astype(jnp.bfloat16)
    n_nb = nb_ref.shape[1] // 2
    for slot in range(2):
        blend = jnp.zeros((n_rows, 2 * STRIP), jnp.float32)
        for k in range(n_nb):
            strip = strip_ref[nb_ref[slot, k], :, nb_ref[slot, n_nb + k]].reshape(n_rows, 2 * STRIP)
            blend += jnp.dot(quarter, strip, preferred_element_type=jnp.float32)
        swapped = pltpu.roll(blend, STRIP, 1)
        main = main_ref[:, slot * t_dev : (slot + 1) * t_dev, :].reshape(n_rows, cells)
        main = jnp.dot(place, main, preferred_element_type=jnp.float32)

        def put(lo, hi, value, slot=slot):
            out_ref[:, slot, :, lo:hi] = value.reshape(t_dev, n_out, hi - lo)

        put(0, half - 128, main[:, 0 : half - 128])
        put(half - 128, half, main[:, half - 128 : half] + jnp.where(upper, swapped, 0.0))
        put(half, cells - 128, main[:, half : cells - 128])
        put(cells - 128, cells, main[:, cells - 128 :] + jnp.where(upper, blend, 0.0))


def join(sources, main, strips):
    n_out, per, cells = main.shape
    return pl.pallas_call(
        join_kernel,
        out_shape=jax.ShapeDtypeStruct((per // 2, 2, n_out, cells), jnp.float32),
        in_specs=[pl.BlockSpec(memory_space=pltpu.SMEM)] + [vmem()] * (1 + len(strips)),
        out_specs=vmem(),
        scratch_shapes=[pltpu.VMEM((len(strips), n_out, 2, per // 2, 2 * STRIP), jnp.bfloat16)],
        compiler_params=pltpu.CompilerParams(vmem_limit_bytes=16 * MIB),
        name="join",
    )(sources, main, *strips)


def exchange(x, axis):
    return lax.all_to_all(x, axis, split_axis=0, concat_axis=0, tiled=True)


def local(visibilities, kernels, delays, tile_of, plane_of, counts, neighbours):
    n_facet = lax.axis_size("facet")
    n_chan = lax.axis_size("chan")
    facet_index = lax.axis_index("facet")
    chan_index = lax.axis_index("chan")
    halves, facets, blocks, _, bv = visibilities.shape
    fac_dev = facets // n_facet
    n_tiles = 16 * n_chan
    t_dev = n_tiles // n_chan
    n_rows = fac_dev * blocks
    per = n_rows // n_chan

    vis = send_order(visibilities.reshape(halves, n_facet * n_chan, per, bv))
    vis = exchange(vis, ("facet", "chan"))
    delay = lax.dynamic_index_in_dim(delays.reshape(n_chan, per, bv), chan_index, 0, keepdims=False)
    live = jnp.arange(blocks, dtype=jnp.int32)[None, :] < counts[:, None]
    planes = jnp.where(live, plane_of, -1).reshape(1, n_rows)
    place, code, piece = tables(planes, tile_of.reshape(1, n_rows), kernels.shape[0], t_dev)

    rows = exchange(average(piece, vis, delay), "chan")
    grids = grid_rows(piece, place, code, rows, kernels, fac_dev * n_tiles)
    main = exchange(grids, "chan")

    own = strips_of(main)
    chips = n_facet // 2
    strips = [own]
    for dz in range(1, chips):
        strips.append(lax.ppermute(own, "facet", [(f, (f + 2 * dz) % n_facet) for f in range(n_facet)]))
    strips += [lax.ppermute(s, "facet", [(f, f ^ 1) for f in range(n_facet)]) for s in strips]
    mine = lax.dynamic_slice_in_dim(neighbours, facet_index * fac_dev, fac_dev, 0)
    group = mine // fac_dev
    source = (facet_index // 2 - group // 2) % chips + chips * ((group + facet_index) % 2)
    sources = jnp.concatenate([source, mine % fac_dev], axis=1).astype(jnp.int32)
    return join(sources, main, strips)


def solution(mesh):
    return jax.shard_map(
        local,
        mesh=mesh,
        in_specs=(
            P(None, None, None, ("facet", "chan"), None),
            P(),
            P("facet", None, None),
            P("facet", None),
            P("facet", None),
            P("facet"),
            P(),
        ),
        out_specs=P("chan", "facet", None, None),
        check_vma=False,
    )
```

```python
import functools
import math

import jax
import jax.numpy as jnp
from jax import lax
from jax.experimental import pallas as pl
from jax.experimental.pallas import tpu as pltpu
from jax.sharding import PartitionSpec as P

AVG = 8
TS = 16
EDGE = 4
STRIP = EDGE * TS
GROUP = 16
PIECE = 64
MIB = 1024 * 1024

SIN = (-1.0 / 6, 1.0 / 120, -1.0 / 5040, 1.0 / 362880, -1.0 / 39916800)
COS = (-1.0 / 2, 1.0 / 24, -1.0 / 720, 1.0 / 40320, -1.0 / 3628800, 1.0 / 479001600)


def series(turns):
    x = (2.0 * math.pi) * turns
    y = x * x
    s = jnp.full_like(x, SIN[-1])
    for k in SIN[-2::-1]:
        s = s * y + k
    c = jnp.full_like(x, COS[-1])
    for k in COS[-2::-1]:
        c = c * y + k
    return c * y + 1.0, (s * y + 1.0) * x


def turn_by(turns):
    half = jnp.round(2.0 * turns)
    c, s = series(turns - 0.5 * half)
    odd = (half - 2.0 * jnp.floor(0.5 * half)) > 0.5
    sign = jnp.where(odd, -1.0, 1.0)
    return c * sign, s * sign


def times(a, b):
    return a[0] * b[0] - a[1] * b[1], a[0] * b[1] + a[1] * b[0]


def vmem():
    return pl.BlockSpec(memory_space=pltpu.VMEM)


def send_kernel(vis_ref, out_ref, held_ref, in_sem, out_sem):
    halves, dests = vis_ref.shape[:2]
    n = in_sem.shape[1]
    loads, stores = [], []
    for i in range(n):
        at = pl.ds(i * (dests // n), dests // n)
        for h in range(halves):
            loads.append(pltpu.make_async_copy(vis_ref.at[h, at], held_ref.at[h, at], in_sem.at[h, i]))
            stores.append(pltpu.make_async_copy(held_ref.at[h, at], out_ref.at[at, h], out_sem.at[h, i]))
            loads[-1].start()
    for load, store in zip(loads, stores):
        load.wait()
        store.start()
    for store in stores:
        store.wait()


def send_order(vis):
    halves, dests, rows, bv = vis.shape
    return pl.pallas_call(
        send_kernel,
        out_shape=pltpu.HBM((dests, halves, rows, bv), vis.dtype),
        in_specs=[pl.BlockSpec(memory_space=pltpu.HBM)],
        out_specs=pl.BlockSpec(memory_space=pltpu.HBM),
        scratch_shapes=[
            pltpu.VMEM(vis.shape, vis.dtype),
            pltpu.SemaphoreType.DMA((halves, 8)),
            pltpu.SemaphoreType.DMA((halves, 8)),
        ],
        compiler_params=pltpu.CompilerParams(vmem_limit_bytes=8 * MIB),
        name="send_order",
    )(pltpu.with_memory_space_constraint(vis, pltpu.HBM))


def fill_turns(d, inner_ref, outer_ref):
    small = series(d * (1.0 / 256.0))
    table = [None, small]
    for j in range(2, AVG):
        table.append(times(table[j // 2], table[j - j // 2]))
    for j in range(1, AVG):
        inner_ref[j - 1, 0] = table[j][0]
        inner_ref[j - 1, 1] = table[j][1]
    c, s = turn_by(d)
    turn = (c * (1.0 / AVG), s * (1.0 / AVG))
    step = series(d * (1.0 / 32.0))
    for o in range(outer_ref.shape[0]):
        outer_ref[o, 0] = turn[0]
        outer_ref[o, 1] = turn[1]
        turn = times(turn, step)


def average_kernel(piece_ref, delay_ref, vis_hbm, out_ref, vis_ref, inner_ref, outer_ref, sem):
    n_out, _, rows, _ = out_ref.shape
    steps = sem.shape[0]
    size = vis_ref.shape[0] // steps
    copies = []
    for i in range(steps):
        at = pl.ds(i * size, size)
        copies.append(pltpu.make_async_copy(vis_hbm.at[at], vis_ref.at[at], sem.at[i]))
        copies[-1].start()
    fill_turns(delay_ref[...], inner_ref, outer_ref)
    for i in range(steps):
        copies[i].wait()
        for r in range(0, rows, 16):
            at = slice(r, r + 16)
            table = [(inner_ref[j, 0, at], inner_ref[j, 1, at]) for j in range(AVG - 1)]

            def one(o, carry, at=at, table=table):
                c = o * AVG
                re = vis_ref[c, 0, at].astype(jnp.float32)
                im = vis_ref[c, 1, at].astype(jnp.float32)
                for j in range(1, AVG):
                    a = vis_ref[c + j, 0, at].astype(jnp.float32)
                    b = vis_ref[c + j, 1, at].astype(jnp.float32)
                    tc, ts = table[j - 1]
                    re += a * tc - b * ts
                    im += a * ts + b * tc
                tc = outer_ref[o, 0, at]
                ts = outer_ref[o, 1, at]
                out_ref[o, 0, at] = (re * tc - im * ts).astype(jnp.bfloat16)
                out_ref[o, 1, at] = (re * ts + im * tc).astype(jnp.bfloat16)
                return carry

            n = n_out // steps
            lax.fori_loop(i * n, (i + 1) * n, one, 0, unroll=n)


def average(piece, vis, delay):
    n_ch, halves, rows, bv = vis.shape
    n_out = n_ch // AVG
    return pl.pallas_call(
        average_kernel,
        out_shape=jax.ShapeDtypeStruct((n_out, halves, rows, bv), jnp.bfloat16),
        in_specs=[vmem(), vmem(), pl.BlockSpec(memory_space=pltpu.HBM)],
        out_specs=vmem(),
        scratch_shapes=[
            pltpu.VMEM(vis.shape, vis.dtype),
            pltpu.VMEM((AVG - 1, 2, rows, bv), jnp.float32),
            pltpu.VMEM((n_out, 2, rows, bv), jnp.float32),
            pltpu.SemaphoreType.DMA((4,)),
        ],
        compiler_params=pltpu.CompilerParams(vmem_limit_bytes=12 * MIB),
        name="average",
    )(piece, delay, pltpu.with_memory_space_constraint(vis, pltpu.HBM))


def to_bf16(mask):
    return mask.astype(jnp.float32).astype(jnp.bfloat16)


def iota(shape, dim):
    return lax.broadcasted_iota(jnp.int32, shape, dim)


def tables_kernel(n_planes, n_order, t_dev, plane_ref, tile_ref, place_ref, code_ref, piece_ref):
    n_rows = plane_ref.shape[1]
    f32 = jnp.float32
    plane = plane_ref[...]
    mine = plane == iota((n_planes, n_rows), 0)
    before = to_bf16(iota((n_rows, n_rows), 0) < iota((n_rows, n_rows), 1))
    rank = jnp.dot(to_bf16(mine), before, preferred_element_type=f32)
    count = jnp.sum(mine.astype(f32), axis=1, keepdims=True)
    groups = jnp.floor((count + (GROUP - 1)) * (1.0 / GROUP))
    pieces = jnp.floor((groups + (PIECE // GROUP - 1)) * (GROUP / PIECE))
    earlier = to_bf16(iota((n_planes, n_planes), 1) < iota((n_planes, n_planes), 0))
    both = jnp.concatenate(
        [jnp.broadcast_to(groups, (n_planes, 128)), jnp.broadcast_to(pieces, (n_planes, 128))], axis=1
    )
    both = jnp.dot(earlier, both.astype(jnp.bfloat16), preferred_element_type=f32)
    first_group = both[:, 0:1]
    first_piece = both[:, 128:129]
    place = jnp.sum(jnp.where(mine, rank + GROUP * first_group, 0.0), axis=0, keepdims=True)
    live = jnp.sum(mine.astype(f32), axis=0, keepdims=True)
    place = jnp.where(live > 0.5, place, -1.0).astype(jnp.int32)
    place_ref[...] = place
    order = to_bf16(iota((n_order, n_rows), 0) == place)

    row = iota((8, n_rows), 0)
    slot = (iota((8, n_rows), 1) >= n_rows // 2).astype(f32)
    values = jnp.where(row == 0, tile_ref[...].astype(f32) + 1.0, jnp.where(row == 1, slot, 0.0))
    n_used = code_ref.shape[1]
    ordered = lax.dot_general(
        values.astype(jnp.bfloat16), order[:n_used], (((1,), (1,)), ((), ())), preferred_element_type=f32
    )
    tile = ordered[0:1].astype(jnp.int32) - 1
    slot = ordered[1:2].astype(jnp.int32)
    code = (tile // t_dev) * (2 * t_dev) + slot * t_dev + tile % t_dev
    code_ref[...] = jnp.where(tile < 0, -1, code)

    total = jnp.sum(pieces)
    which = jnp.minimum(iota((n_planes, 128), 1).astype(f32), total - 1.0)
    taken = (which >= first_piece) & (which < first_piece + pieces)
    group = first_group + (PIECE // GROUP) * (which - first_piece)
    group = jnp.sum(jnp.where(taken, group, 0.0), axis=0, keepdims=True)
    owner = jnp.sum(jnp.where(taken, iota((n_planes, 128), 0).astype(f32), 0.0), axis=0, keepdims=True)
    row = iota((8, 128), 0)
    piece_ref[...] = jnp.where(row == 0, group, jnp.where(row == 1, owner, 0.0)).astype(jnp.int32)


def sizes(n_rows, n_planes):
    used = n_rows + n_planes * (GROUP - 1)
    n_order = -(-(used - GROUP + PIECE) // 32) * 32
    n_used = -(-used // 256) * 256
    assert n_used <= n_order
    return n_order, n_used


def tables(planes, tiles, n_planes, t_dev):
    n_rows = planes.shape[1]
    n_order, n_used = sizes(n_rows, n_planes)
    return pl.pallas_call(
        functools.partial(tables_kernel, n_planes, n_order, t_dev),
        out_shape=[
            jax.ShapeDtypeStruct((1, n_rows), jnp.int32),
            jax.ShapeDtypeStruct((1, n_used), jnp.int32),
            jax.ShapeDtypeStruct((8, 128), jnp.int32),
        ],
        in_specs=[vmem()] * 2,
        out_specs=[vmem()] * 3,
        compiler_params=pltpu.CompilerParams(vmem_limit_bytes=40 * MIB),
        name="tables",
    )(planes, tiles)


def grid_kernel(n_pieces, piece_ref, place_ref, code_ref, rows_ref, k_hbm, out_ref, k_ref, x_ref, c_ref, sem):
    n_fetch = sem.shape[0]
    part = k_ref.shape[0] // n_fetch
    fetches = []
    for i in range(n_fetch):
        at = pl.ds(i * part, part)
        fetches.append(pltpu.make_async_copy(k_hbm.at[at], k_ref.at[at], sem.at[i]))
        fetches[-1].start()
    n_src, _, per, bv = rows_ref.shape
    n_order = x_ref.shape[0]
    re = rows_ref[:, 0].reshape(n_src * per, bv)
    im = rows_ref[:, 1].reshape(n_src * per, bv)
    x = jnp.concatenate([re, im], axis=1)
    order = to_bf16(iota((n_order, n_src * per), 0) == place_ref[...])
    x_ref[...] = jnp.dot(order, x, preferred_element_type=jnp.float32).astype(jnp.bfloat16)
    n_used = code_ref.shape[1]
    n_codes = out_ref.shape[0] * out_ref.shape[1]
    tiles = to_bf16(iota((n_codes, n_used), 0) == code_ref[...])
    c_ref[...] = jnp.zeros_like(c_ref)
    for fetch in fetches:
        fetch.wait()
    for i in range(n_pieces):
        at = pl.ds(pl.multiple_of(piece_ref[0, i] * GROUP, GROUP), PIECE)
        product = jnp.dot(x_ref[at, :], k_ref[piece_ref[1, i]], preferred_element_type=jnp.float32)
        c_ref[at, :] = product.astype(jnp.bfloat16)
    grid = jnp.dot(tiles, c_ref[:n_used, :], preferred_element_type=jnp.float32)
    out_ref[...] = grid.astype(jnp.bfloat16).reshape(out_ref.shape)


def grid_rows(piece, place, code, rows, kernels, n_codes):
    n_planes, k_rows, cells = kernels.shape
    n_rows = place.shape[1]
    n_chan = rows.shape[0]
    n_order, n_used = sizes(n_rows, n_planes)
    return pl.pallas_call(
        functools.partial(grid_kernel, n_rows // PIECE + n_planes),
        out_shape=jax.ShapeDtypeStruct((n_chan, n_codes // n_chan, cells), jnp.bfloat16),
        in_specs=[pl.BlockSpec(memory_space=pltpu.SMEM)] + [vmem()] * 3 + [pl.BlockSpec(memory_space=pltpu.HBM)],
        out_specs=vmem(),
        scratch_shapes=[
            pltpu.VMEM(kernels.shape, kernels.dtype),
            pltpu.VMEM((n_order, k_rows), jnp.bfloat16),
            pltpu.VMEM((n_order, cells), jnp.bfloat16),
            pltpu.SemaphoreType.DMA((8,)),
        ],
        compiler_params=pltpu.CompilerParams(vmem_limit_bytes=40 * MIB),
        name="grid_rows",
    )(piece, place, code, rows, pltpu.with_memory_space_constraint(kernels, pltpu.HBM))


def strip_kernel(main_ref, out_ref):
    n_out, per, cells = main_ref.shape
    half = cells // 2
    low = main_ref[:, :, 0:128].reshape(n_out * per, 128).astype(jnp.float32)
    high = main_ref[:, :, half : half + 128].reshape(n_out * per, 128).astype(jnp.float32)
    lane = lax.broadcasted_iota(jnp.int32, low.shape, 1)
    strip = jnp.where(lane < STRIP, low, pltpu.roll(high, STRIP, 1)).astype(jnp.bfloat16)
    out_ref[...] = strip.reshape(out_ref.shape)


def strips_of(main):
    n_out, per, _ = main.shape
    return pl.pallas_call(
        strip_kernel,
        out_shape=jax.ShapeDtypeStruct((n_out, per, 2 * STRIP), jnp.bfloat16),
        in_specs=[vmem()],
        out_specs=vmem(),
        compiler_params=pltpu.CompilerParams(vmem_limit_bytes=8 * MIB),
        name="strips",
    )(main)


def join_kernel(nb_ref, main_ref, *refs):
    strips, out_ref, strip_ref = refs[:-2], refs[-2], refs[-1]
    n_out, per, cells = main_ref.shape
    t_dev = per // 2
    half = cells // 2
    n_rows = n_out * t_dev
    for i, ref in enumerate(strips):
        strip_ref[i] = ref[...].reshape(strip_ref.shape[1:])
    upper = iota((n_rows, 2 * STRIP), 1) >= STRIP
    to = iota((n_rows, n_rows), 0)
    place = (iota((n_rows, n_rows), 1) == (to % n_out) * t_dev + to // n_out).astype(jnp.float32)
    quarter = (0.25 * place).astype(jnp.bfloat16)
    place = place.astype(jnp.bfloat16)
    n_nb = nb_ref.shape[1] // 2
    for slot in range(2):
        blend = jnp.zeros((n_rows, 2 * STRIP), jnp.float32)
        for k in range(n_nb):
            strip = strip_ref[nb_ref[slot, k], :, nb_ref[slot, n_nb + k]].reshape(n_rows, 2 * STRIP)
            blend += jnp.dot(quarter, strip, preferred_element_type=jnp.float32)
        swapped = pltpu.roll(blend, STRIP, 1)
        main = main_ref[:, slot * t_dev : (slot + 1) * t_dev, :].reshape(n_rows, cells)
        main = jnp.dot(place, main, preferred_element_type=jnp.float32)

        def put(lo, hi, value, slot=slot):
            out_ref[:, slot, :, lo:hi] = value.reshape(t_dev, n_out, hi - lo)

        put(0, half - 128, main[:, 0 : half - 128])
        put(half - 128, half, main[:, half - 128 : half] + jnp.where(upper, swapped, 0.0))
        put(half, cells - 128, main[:, half : cells - 128])
        put(cells - 128, cells, main[:, cells - 128 :] + jnp.where(upper, blend, 0.0))


def join(sources, main, strips):
    n_out, per, cells = main.shape
    return pl.pallas_call(
        join_kernel,
        out_shape=jax.ShapeDtypeStruct((per // 2, 2, n_out, cells), jnp.float32),
        in_specs=[pl.BlockSpec(memory_space=pltpu.SMEM)] + [vmem()] * (1 + len(strips)),
        out_specs=vmem(),
        scratch_shapes=[pltpu.VMEM((len(strips), n_out, 2, per // 2, 2 * STRIP), jnp.bfloat16)],
        compiler_params=pltpu.CompilerParams(vmem_limit_bytes=16 * MIB),
        name="join",
    )(sources, main, *strips)


def exchange(x, axis):
    return lax.all_to_all(x, axis, split_axis=0, concat_axis=0, tiled=True)


def local(visibilities, kernels, delays, tile_of, plane_of, counts, neighbours):
    n_facet = lax.axis_size("facet")
    n_chan = lax.axis_size("chan")
    facet_index = lax.axis_index("facet")
    chan_index = lax.axis_index("chan")
    halves, facets, blocks, _, bv = visibilities.shape
    fac_dev = facets // n_facet
    n_tiles = 16 * n_chan
    t_dev = n_tiles // n_chan
    n_rows = fac_dev * blocks
    per = n_rows // n_chan

    vis = send_order(visibilities.reshape(halves, n_facet * n_chan, per, bv))
    vis = exchange(vis, ("facet", "chan"))
    delay = lax.dynamic_index_in_dim(delays.reshape(n_chan, per, bv), chan_index, 0, keepdims=False)
    live = jnp.arange(blocks, dtype=jnp.int32)[None, :] < counts[:, None]
    planes = jnp.where(live, plane_of, -1).reshape(1, n_rows)
    place, code, piece = tables(planes, tile_of.reshape(1, n_rows), kernels.shape[0], t_dev)

    rows = exchange(average(piece, vis, delay), "chan")
    grids = grid_rows(piece, place, code, rows, kernels, fac_dev * n_tiles)
    main = exchange(grids, "chan")

    own = strips_of(main)
    chips = n_facet // 2
    strips = [own]
    for dz in range(1, chips):
        strips.append(lax.ppermute(own, "facet", [(f, (f + 2 * dz) % n_facet) for f in range(n_facet)]))
    strips += [lax.ppermute(s, "facet", [(f, f ^ 1) for f in range(n_facet)]) for s in strips]
    mine = lax.dynamic_slice_in_dim(neighbours, facet_index * fac_dev, fac_dev, 0)
    group = mine // fac_dev
    source = (facet_index // 2 - group // 2) % chips + chips * ((group + facet_index) % 2)
    sources = jnp.concatenate([source, mine % fac_dev], axis=1).astype(jnp.int32)
    return join(sources, main, strips)


def solution(mesh):
    return jax.shard_map(
        local,
        mesh=mesh,
        in_specs=(
            P(None, None, None, ("facet", "chan"), None),
            P(),
            P("facet", None, None),
            P("facet", None),
            P("facet", None),
            P("facet"),
            P(),
        ),
        out_specs=P("chan", "facet", None, None),
        check_vma=False,
    )
```

```python
import functools
import math

import jax
import jax.numpy as jnp
from jax import lax
from jax.experimental import pallas as pl
from jax.experimental.pallas import tpu as pltpu
from jax.sharding import PartitionSpec as P

AVG = 8
TS = 16
EDGE = 4
STRIP = EDGE * TS
GROUP = 16
PIECE = 64
STRETCH = 12
MIB = 1024 * 1024

SIN = (-1.0 / 6, 1.0 / 120, -1.0 / 5040, 1.0 / 362880, -1.0 / 39916800)
COS = (-1.0 / 2, 1.0 / 24, -1.0 / 720, 1.0 / 40320, -1.0 / 3628800, 1.0 / 479001600)


def series(turns):
    x = (2.0 * math.pi) * turns
    y = x * x
    s = jnp.full_like(x, SIN[-1])
    for k in SIN[-2::-1]:
        s = s * y + k
    c = jnp.full_like(x, COS[-1])
    for k in COS[-2::-1]:
        c = c * y + k
    return c * y + 1.0, (s * y + 1.0) * x


def turn_by(turns):
    half = jnp.round(2.0 * turns)
    c, s = series(turns - 0.5 * half)
    odd = (half - 2.0 * jnp.floor(0.5 * half)) > 0.5
    sign = jnp.where(odd, -1.0, 1.0)
    return c * sign, s * sign


def times(a, b):
    return a[0] * b[0] - a[1] * b[1], a[0] * b[1] + a[1] * b[0]


def vmem():
    return pl.BlockSpec(memory_space=pltpu.VMEM)


def to_bf16(mask):
    return mask.astype(jnp.float32).astype(jnp.bfloat16)


def iota(shape, dim):
    return lax.broadcasted_iota(jnp.int32, shape, dim)


def fill_tables(n_planes, n_order, t_dev, count_ref, plane_ref, tile_ref, place_ref, code_ref, piece_ref):
    f32 = jnp.float32
    slots, blocks = plane_ref.shape
    n_rows = slots * blocks
    planes, tiles = [], []
    for slot in range(slots):
        alive = iota((1, blocks), 1) < count_ref[slot]
        planes.append(jnp.where(alive, plane_ref[slot : slot + 1, :], -1))
        tiles.append(tile_ref[slot : slot + 1, :])
    plane = jnp.concatenate(planes, axis=1)
    tile = jnp.concatenate(tiles, axis=1)
    mine = plane == iota((n_planes, n_rows), 0)
    before = to_bf16(iota((n_rows, n_rows), 0) < iota((n_rows, n_rows), 1))
    rank = jnp.dot(to_bf16(mine), before, preferred_element_type=f32)
    count = jnp.sum(mine.astype(f32), axis=1, keepdims=True)
    groups = jnp.floor((count + (GROUP - 1)) * (1.0 / GROUP))
    pieces = jnp.floor((groups + (PIECE // GROUP - 1)) * (GROUP / PIECE))
    earlier = to_bf16(iota((n_planes, n_planes), 1) < iota((n_planes, n_planes), 0))
    both = jnp.concatenate(
        [jnp.broadcast_to(groups, (n_planes, 128)), jnp.broadcast_to(pieces, (n_planes, 128))], axis=1
    )
    both = jnp.dot(earlier, both.astype(jnp.bfloat16), preferred_element_type=f32)
    first_group = both[:, 0:1]
    first_piece = both[:, 128:129]
    place = jnp.sum(jnp.where(mine, rank + GROUP * first_group, 0.0), axis=0, keepdims=True)
    live = jnp.sum(mine.astype(f32), axis=0, keepdims=True)
    place = jnp.where(live > 0.5, place, -1.0).astype(jnp.int32)
    place_ref[...] = place
    order = to_bf16(iota((n_order, n_rows), 0) == place)

    row = iota((8, n_rows), 0)
    slot = (iota((8, n_rows), 1) >= n_rows // 2).astype(f32)
    values = jnp.where(row == 0, tile.astype(f32) + 1.0, jnp.where(row == 1, slot, 0.0))
    n_used = code_ref.shape[1]
    ordered = lax.dot_general(
        values.astype(jnp.bfloat16), order[:n_used], (((1,), (1,)), ((), ())), preferred_element_type=f32
    )
    tile = ordered[0:1].astype(jnp.int32) - 1
    slot = ordered[1:2].astype(jnp.int32)
    code = (tile // t_dev) * (2 * t_dev) + slot * t_dev + tile % t_dev
    code_ref[...] = jnp.where(tile < 0, -1, code)

    total = jnp.sum(pieces)
    which = jnp.minimum(iota((n_planes, 128), 1).astype(f32), total - 1.0)
    taken = (which >= first_piece) & (which < first_piece + pieces)
    group = first_group + (PIECE // GROUP) * (which - first_piece)
    group = jnp.sum(jnp.where(taken, group, 0.0), axis=0, keepdims=True)
    owner = jnp.sum(jnp.where(taken, iota((n_planes, 128), 0).astype(f32), 0.0), axis=0, keepdims=True)
    row = iota((8, 128), 0)
    piece_ref[...] = jnp.where(row == 0, group, jnp.where(row == 1, owner, 0.0)).astype(jnp.int32)


def sizes(n_rows, n_planes):
    used = n_rows + n_planes * (GROUP - 1)
    n_order = -(-(used - GROUP + PIECE) // 32) * 32
    n_used = -(-used // 256) * 256
    assert n_used <= n_order
    return n_order, n_used


def send_kernel(n_planes, n_order, t_dev, count_ref, plane_ref, tile_ref, vis_ref, out_ref, *rest):
    tables, sem = rest[:-1], rest[-1]
    halves, dests = vis_ref.shape[:2]
    n = sem.shape[1]
    copies = []
    for i in range(n):
        at = pl.ds(i * (dests // n), dests // n)
        for h in range(halves):
            copies.append(pltpu.make_async_copy(vis_ref.at[h, at], out_ref.at[at, h], sem.at[h, i]))
            copies[-1].start()
    fill_tables(n_planes, n_order, t_dev, count_ref, plane_ref, tile_ref, *tables)
    for copy in copies:
        copy.wait()


def send_order(counts, planes, tiles, vis, n_planes, t_dev):
    halves, dests, rows, bv = vis.shape
    n_rows = planes.shape[0] * planes.shape[1]
    n_order, n_used = sizes(n_rows, n_planes)
    return pl.pallas_call(
        functools.partial(send_kernel, n_planes, n_order, t_dev),
        out_shape=[
            jax.ShapeDtypeStruct((dests, halves, rows, bv), vis.dtype),
            jax.ShapeDtypeStruct((1, n_rows), jnp.int32),
            jax.ShapeDtypeStruct((1, n_used), jnp.int32),
            jax.ShapeDtypeStruct((8, 128), jnp.int32),
        ],
        in_specs=[
            pl.BlockSpec(memory_space=pltpu.SMEM),
            vmem(),
            vmem(),
            pl.BlockSpec(memory_space=pltpu.HBM),
        ],
        out_specs=[vmem()] * 4,
        scratch_shapes=[pltpu.SemaphoreType.DMA((halves, 4))],
        compiler_params=pltpu.CompilerParams(vmem_limit_bytes=32 * MIB),
        name="send_order",
    )(counts, planes, tiles, pltpu.with_memory_space_constraint(vis, pltpu.HBM))


def fill_turns(d, inner_ref, outer_ref):
    small = series(d * (1.0 / 256.0))
    table = [None, small]
    for j in range(2, AVG):
        table.append(times(table[j // 2], table[j - j // 2]))
    for j in range(1, AVG):
        inner_ref[j - 1, 0] = table[j][0]
        inner_ref[j - 1, 1] = table[j][1]
    c, s = turn_by(d)
    turn = (c * (1.0 / AVG), s * (1.0 / AVG))
    step = series(d * (1.0 / 32.0))
    for o in range(outer_ref.shape[0]):
        outer_ref[o, 0] = turn[0]
        outer_ref[o, 1] = turn[1]
        turn = times(turn, step)


def average_kernel(delay_hbm, vis_ref, out_ref, delay_ref, inner_ref, outer_ref, sem):
    fetch = pltpu.make_async_copy(delay_hbm.at[lax.axis_index("chan")], delay_ref, sem.at[0])
    fetch.start()
    fetch.wait()
    fill_turns(delay_ref[...], inner_ref, outer_ref)
    n_out, _, rows, _ = out_ref.shape
    for r in range(0, rows, 16):
        at = slice(r, r + 16)
        table = [(inner_ref[j, 0, at], inner_ref[j, 1, at]) for j in range(AVG - 1)]

        def one(o, carry, at=at, table=table):
            c = o * AVG
            re = vis_ref[c, 0, at].astype(jnp.float32)
            im = vis_ref[c, 1, at].astype(jnp.float32)
            for j in range(1, AVG):
                a = vis_ref[c + j, 0, at].astype(jnp.float32)
                b = vis_ref[c + j, 1, at].astype(jnp.float32)
                tc, ts = table[j - 1]
                re += a * tc - b * ts
                im += a * ts + b * tc
            tc = outer_ref[o, 0, at]
            ts = outer_ref[o, 1, at]
            out_ref[o, 0, at] = (re * tc - im * ts).astype(jnp.bfloat16)
            out_ref[o, 1, at] = (re * ts + im * tc).astype(jnp.bfloat16)
            return carry

        lax.fori_loop(0, n_out, one, 0, unroll=4)


def average(delays, vis):
    n_ch, halves, rows, bv = vis.shape
    n_out = n_ch // AVG
    return pl.pallas_call(
        average_kernel,
        out_shape=jax.ShapeDtypeStruct((n_out, halves, rows, bv), jnp.bfloat16),
        in_specs=[pl.BlockSpec(memory_space=pltpu.HBM), vmem()],
        out_specs=vmem(),
        scratch_shapes=[
            pltpu.VMEM((rows, bv), jnp.float32),
            pltpu.VMEM((AVG - 1, 2, rows, bv), jnp.float32),
            pltpu.VMEM((n_out, 2, rows, bv), jnp.float32),
            pltpu.SemaphoreType.DMA((1,)),
        ],
        compiler_params=pltpu.CompilerParams(vmem_limit_bytes=12 * MIB),
        name="average",
    )(pltpu.with_memory_space_constraint(delays, pltpu.HBM), vis)


def grid_kernel(n_pieces, piece_ref, place_ref, code_ref, rows_ref, k_hbm, out_ref, k_ref, x_ref, c_ref, sem):
    n_fetch = sem.shape[0]
    part = k_ref.shape[0] // n_fetch
    fetches = []
    for i in range(n_fetch):
        at = pl.ds(i * part, part)
        fetches.append(pltpu.make_async_copy(k_hbm.at[at], k_ref.at[at], sem.at[i]))
        fetches[-1].start()
    n_src, _, per, bv = rows_ref.shape
    n_order = x_ref.shape[0]
    re = rows_ref[:, 0].reshape(n_src * per, bv)
    im = rows_ref[:, 1].reshape(n_src * per, bv)
    x = jnp.concatenate([re, im], axis=1)
    order = to_bf16(iota((n_order, n_src * per), 0) == place_ref[...])
    x_ref[...] = jnp.dot(order, x, preferred_element_type=jnp.float32).astype(jnp.bfloat16)
    n_used = code_ref.shape[1]
    n_codes = out_ref.shape[0] * out_ref.shape[1]
    tiles = to_bf16(iota((n_codes, n_used), 0) == code_ref[...])
    c_ref[...] = jnp.zeros_like(c_ref)
    had = jnp.int32(0)
    for i in range(n_pieces):
        if i % STRETCH == 0:
            need = n_fetch if i + STRETCH >= n_pieces else piece_ref[1, i + STRETCH - 1] // part + 1
            for k, fetch in enumerate(fetches):

                @pl.when((k >= had) & (k < need))
                def _(fetch=fetch):
                    fetch.wait()

            had = jnp.maximum(had, need)
        at = pl.ds(pl.multiple_of(piece_ref[0, i] * GROUP, GROUP), PIECE)
        product = jnp.dot(x_ref[at, :], k_ref[piece_ref[1, i]], preferred_element_type=jnp.float32)
        c_ref[at, :] = product.astype(jnp.bfloat16)
    grid = jnp.dot(tiles, c_ref[:n_used, :], preferred_element_type=jnp.float32)
    out_ref[...] = grid.astype(jnp.bfloat16).reshape(out_ref.shape)


def grid_rows(piece, place, code, rows, kernels, n_codes):
    n_planes, k_rows, cells = kernels.shape
    n_rows = place.shape[1]
    n_chan = rows.shape[0]
    n_order, n_used = sizes(n_rows, n_planes)
    return pl.pallas_call(
        functools.partial(grid_kernel, n_rows // PIECE + n_planes),
        out_shape=jax.ShapeDtypeStruct((n_chan, n_codes // n_chan, cells), jnp.bfloat16),
        in_specs=[pl.BlockSpec(memory_space=pltpu.SMEM)] + [vmem()] * 3 + [pl.BlockSpec(memory_space=pltpu.HBM)],
        out_specs=vmem(),
        scratch_shapes=[
            pltpu.VMEM(kernels.shape, kernels.dtype),
            pltpu.VMEM((n_order, k_rows), jnp.bfloat16),
            pltpu.VMEM((n_order, cells), jnp.bfloat16),
            pltpu.SemaphoreType.DMA((8,)),
        ],
        compiler_params=pltpu.CompilerParams(vmem_limit_bytes=40 * MIB),
        name="grid_rows",
    )(piece, place, code, rows, pltpu.with_memory_space_constraint(kernels, pltpu.HBM))


def strip_kernel(main_ref, out_ref):
    n_out, per, cells = main_ref.shape
    half = cells // 2
    low = main_ref[:, :, 0:128].reshape(n_out * per, 128).astype(jnp.float32)
    high = main_ref[:, :, half : half + 128].reshape(n_out * per, 128).astype(jnp.float32)
    lane = lax.broadcasted_iota(jnp.int32, low.shape, 1)
    strip = jnp.where(lane < STRIP, low, pltpu.roll(high, STRIP, 1)).astype(jnp.bfloat16)
    out_ref[...] = strip.reshape(out_ref.shape)


def strips_of(main):
    n_out, per, _ = main.shape
    return pl.pallas_call(
        strip_kernel,
        out_shape=jax.ShapeDtypeStruct((n_out, per, 2 * STRIP), jnp.bfloat16),
        in_specs=[vmem()],
        out_specs=vmem(),
        compiler_params=pltpu.CompilerParams(vmem_limit_bytes=8 * MIB),
        name="strips",
    )(main)


def join_kernel(nb_ref, main_ref, *refs):
    strips, out_ref, strip_ref = refs[:-2], refs[-2], refs[-1]
    n_out, per, cells = main_ref.shape
    t_dev = per // 2
    half = cells // 2
    n_rows = n_out * t_dev
    for i, ref in enumerate(strips):
        strip_ref[i] = ref[...].reshape(strip_ref.shape[1:])
    upper = iota((n_rows, 2 * STRIP), 1) >= STRIP
    to = iota((n_rows, n_rows), 0)
    place = (iota((n_rows, n_rows), 1) == (to % n_out) * t_dev + to // n_out).astype(jnp.float32)
    quarter = (0.25 * place).astype(jnp.bfloat16)
    place = place.astype(jnp.bfloat16)
    n_nb = nb_ref.shape[1] // 2
    for slot in range(2):
        blend = jnp.zeros((n_rows, 2 * STRIP), jnp.float32)
        for k in range(n_nb):
            strip = strip_ref[nb_ref[slot, k], :, nb_ref[slot, n_nb + k]].reshape(n_rows, 2 * STRIP)
            blend += jnp.dot(quarter, strip, preferred_element_type=jnp.float32)
        swapped = pltpu.roll(blend, STRIP, 1)
        main = main_ref[:, slot * t_dev : (slot + 1) * t_dev, :].reshape(n_rows, cells)
        main = jnp.dot(place, main, preferred_element_type=jnp.float32)

        def put(lo, hi, value, slot=slot):
            out_ref[:, slot, :, lo:hi] = value.reshape(t_dev, n_out, hi - lo)

        put(0, half - 128, main[:, 0 : half - 128])
        put(half - 128, half, main[:, half - 128 : half] + jnp.where(upper, swapped, 0.0))
        put(half, cells - 128, main[:, half : cells - 128])
        put(cells - 128, cells, main[:, cells - 128 :] + jnp.where(upper, blend, 0.0))


def join(sources, main, strips):
    n_out, per, cells = main.shape
    return pl.pallas_call(
        join_kernel,
        out_shape=jax.ShapeDtypeStruct((per // 2, 2, n_out, cells), jnp.float32),
        in_specs=[pl.BlockSpec(memory_space=pltpu.SMEM)] + [vmem()] * (1 + len(strips)),
        out_specs=vmem(),
        scratch_shapes=[pltpu.VMEM((len(strips), n_out, 2, per // 2, 2 * STRIP), jnp.bfloat16)],
        compiler_params=pltpu.CompilerParams(vmem_limit_bytes=16 * MIB),
        name="join",
    )(sources, main, *strips)


def exchange(x, axis):
    return lax.all_to_all(x, axis, split_axis=0, concat_axis=0, tiled=True)


def local(visibilities, kernels, delays, tile_of, plane_of, counts, neighbours):
    n_facet = lax.axis_size("facet")
    n_chan = lax.axis_size("chan")
    facet_index = lax.axis_index("facet")
    halves, facets, blocks, _, bv = visibilities.shape
    fac_dev = facets // n_facet
    n_tiles = 16 * n_chan
    t_dev = n_tiles // n_chan
    n_rows = fac_dev * blocks
    per = n_rows // n_chan

    vis = visibilities.reshape(halves, n_facet * n_chan, per, bv)
    vis, place, code, piece = send_order(counts, plane_of, tile_of, vis, kernels.shape[0], t_dev)
    vis = exchange(vis, ("facet", "chan"))

    rows = exchange(average(delays.reshape(n_chan, per, bv), vis), "chan")
    grids = grid_rows(piece, place, code, rows, kernels, fac_dev * n_tiles)
    main = exchange(grids, "chan")

    own = strips_of(main)
    chips = n_facet // 2
    strips = [own]
    for dz in range(1, chips):
        strips.append(lax.ppermute(own, "facet", [(f, (f + 2 * dz) % n_facet) for f in range(n_facet)]))
    strips += [lax.ppermute(s, "facet", [(f, f ^ 1) for f in range(n_facet)]) for s in strips]
    mine = lax.dynamic_slice_in_dim(neighbours, facet_index * fac_dev, fac_dev, 0)
    group = mine // fac_dev
    source = (facet_index // 2 - group // 2) % chips + chips * ((group + facet_index) % 2)
    sources = jnp.concatenate([source, mine % fac_dev], axis=1).astype(jnp.int32)
    return join(sources, main, strips)


def solution(mesh):
    return jax.shard_map(
        local,
        mesh=mesh,
        in_specs=(
            P(None, None, None, ("facet", "chan"), None),
            P(),
            P("facet", None, None),
            P("facet", None),
            P("facet", None),
            P("facet"),
            P(),
        ),
        out_specs=P("chan", "facet", None, None),
        check_vma=False,
    )
```

```python
import functools
import math

import jax
import jax.numpy as jnp
from jax import lax
from jax.experimental import pallas as pl
from jax.experimental.pallas import tpu as pltpu
from jax.sharding import PartitionSpec as P

AVG = 8
TS = 16
EDGE = 4
STRIP = EDGE * TS
GROUP = 16
PIECE = 64
STRETCH = 12
MIB = 1024 * 1024

SIN = (-1.0 / 6, 1.0 / 120, -1.0 / 5040, 1.0 / 362880, -1.0 / 39916800)
COS = (-1.0 / 2, 1.0 / 24, -1.0 / 720, 1.0 / 40320, -1.0 / 3628800, 1.0 / 479001600)


def series(turns):
    x = (2.0 * math.pi) * turns
    y = x * x
    s = jnp.full_like(x, SIN[-1])
    for k in SIN[-2::-1]:
        s = s * y + k
    c = jnp.full_like(x, COS[-1])
    for k in COS[-2::-1]:
        c = c * y + k
    return c * y + 1.0, (s * y + 1.0) * x


def turn_by(turns):
    half = jnp.round(2.0 * turns)
    c, s = series(turns - 0.5 * half)
    odd = (half - 2.0 * jnp.floor(0.5 * half)) > 0.5
    sign = jnp.where(odd, -1.0, 1.0)
    return c * sign, s * sign


def times(a, b):
    return a[0] * b[0] - a[1] * b[1], a[0] * b[1] + a[1] * b[0]


def vmem():
    return pl.BlockSpec(memory_space=pltpu.VMEM)


def to_bf16(mask):
    return mask.astype(jnp.float32).astype(jnp.bfloat16)


def iota(shape, dim):
    return lax.broadcasted_iota(jnp.int32, shape, dim)


def fill_tables(n_planes, n_order, t_dev, count_ref, plane_ref, tile_ref, place_ref, code_ref, piece_ref):
    f32 = jnp.float32
    slots, blocks = plane_ref.shape
    n_rows = slots * blocks
    planes, tiles = [], []
    for slot in range(slots):
        alive = iota((1, blocks), 1) < count_ref[slot]
        planes.append(jnp.where(alive, plane_ref[slot : slot + 1, :], -1))
        tiles.append(tile_ref[slot : slot + 1, :])
    plane = jnp.concatenate(planes, axis=1)
    tile = jnp.concatenate(tiles, axis=1)
    mine = plane == iota((n_planes, n_rows), 0)
    before = to_bf16(iota((n_rows, n_rows), 0) < iota((n_rows, n_rows), 1))
    rank = jnp.dot(to_bf16(mine), before, preferred_element_type=f32)
    count = jnp.sum(mine.astype(f32), axis=1, keepdims=True)
    groups = jnp.floor((count + (GROUP - 1)) * (1.0 / GROUP))
    pieces = jnp.floor((groups + (PIECE // GROUP - 1)) * (GROUP / PIECE))
    earlier = to_bf16(iota((n_planes, n_planes), 1) < iota((n_planes, n_planes), 0))
    both = jnp.concatenate(
        [jnp.broadcast_to(groups, (n_planes, 128)), jnp.broadcast_to(pieces, (n_planes, 128))], axis=1
    )
    both = jnp.dot(earlier, both.astype(jnp.bfloat16), preferred_element_type=f32)
    first_group = both[:, 0:1]
    first_piece = both[:, 128:129]
    place = jnp.sum(jnp.where(mine, rank + GROUP * first_group, 0.0), axis=0, keepdims=True)
    live = jnp.sum(mine.astype(f32), axis=0, keepdims=True)
    place = jnp.where(live > 0.5, place, -1.0).astype(jnp.int32)
    place_ref[...] = place
    order = to_bf16(iota((n_order, n_rows), 0) == place)

    row = iota((8, n_rows), 0)
    slot = (iota((8, n_rows), 1) >= n_rows // 2).astype(f32)
    values = jnp.where(row == 0, tile.astype(f32) + 1.0, jnp.where(row == 1, slot, 0.0))
    n_used = code_ref.shape[1]
    ordered = lax.dot_general(
        values.astype(jnp.bfloat16), order[:n_used], (((1,), (1,)), ((), ())), preferred_element_type=f32
    )
    tile = ordered[0:1].astype(jnp.int32) - 1
    slot = ordered[1:2].astype(jnp.int32)
    code = (tile // t_dev) * (2 * t_dev) + slot * t_dev + tile % t_dev
    code_ref[...] = jnp.where(tile < 0, -1, code)

    total = jnp.sum(pieces)
    which = jnp.minimum(iota((n_planes, 128), 1).astype(f32), total - 1.0)
    taken = (which >= first_piece) & (which < first_piece + pieces)
    group = first_group + (PIECE // GROUP) * (which - first_piece)
    group = jnp.sum(jnp.where(taken, group, 0.0), axis=0, keepdims=True)
    owner = jnp.sum(jnp.where(taken, iota((n_planes, 128), 0).astype(f32), 0.0), axis=0, keepdims=True)
    row = iota((8, 128), 0)
    piece_ref[...] = jnp.where(row == 0, group, jnp.where(row == 1, owner, 0.0)).astype(jnp.int32)


def sizes(n_rows, n_planes):
    used = n_rows + n_planes * (GROUP - 1)
    n_order = -(-(used - GROUP + PIECE) // 32) * 32
    n_used = -(-used // 256) * 256
    assert n_used <= n_order
    return n_order, n_used


def send_kernel(n_planes, n_order, t_dev, *refs):
    (count_hbm, plane_hbm, tile_hbm, delay_hbm, vis_hbm), refs = refs[:5], refs[5:]
    (out_ref, delay_ref, *tables), (count_ref, plane_ref, tile_ref, small_sem, sem) = refs[:-5], refs[-5:]
    smalls = [
        pltpu.make_async_copy(count_hbm, count_ref, small_sem.at[0]),
        pltpu.make_async_copy(plane_hbm, plane_ref, small_sem.at[1]),
        pltpu.make_async_copy(tile_hbm, tile_ref, small_sem.at[2]),
        pltpu.make_async_copy(delay_hbm.at[lax.axis_index("chan")], delay_ref, small_sem.at[3]),
    ]
    for copy in smalls:
        copy.start()
    halves, dests = vis_hbm.shape[:2]
    n = sem.shape[1]
    copies = []
    for i in range(n):
        at = pl.ds(i * (dests // n), dests // n)
        for h in range(halves):
            copies.append(pltpu.make_async_copy(vis_hbm.at[h, at], out_ref.at[at, h], sem.at[h, i]))
            copies[-1].start()
    for copy in smalls:
        copy.wait()
    fill_tables(n_planes, n_order, t_dev, count_ref, plane_ref, tile_ref, *tables)
    for copy in copies:
        copy.wait()


def send_order(counts, planes, tiles, delays, vis, n_planes, t_dev):
    halves, dests, rows, bv = vis.shape
    n_rows = planes.shape[0] * planes.shape[1]
    n_order, n_used = sizes(n_rows, n_planes)
    args = [pltpu.with_memory_space_constraint(x, pltpu.HBM) for x in (counts, planes, tiles, delays, vis)]
    return pl.pallas_call(
        functools.partial(send_kernel, n_planes, n_order, t_dev),
        out_shape=[
            jax.ShapeDtypeStruct((dests, halves, rows, bv), vis.dtype),
            jax.ShapeDtypeStruct(delays.shape[1:], delays.dtype),
            jax.ShapeDtypeStruct((1, n_rows), jnp.int32),
            jax.ShapeDtypeStruct((1, n_used), jnp.int32),
            jax.ShapeDtypeStruct((8, 128), jnp.int32),
        ],
        in_specs=[pl.BlockSpec(memory_space=pltpu.HBM)] * len(args),
        out_specs=[vmem()] * 5,
        scratch_shapes=[
            pltpu.SMEM(counts.shape, jnp.int32),
            pltpu.VMEM(planes.shape, jnp.int32),
            pltpu.VMEM(tiles.shape, jnp.int32),
            pltpu.SemaphoreType.DMA((4,)),
            pltpu.SemaphoreType.DMA((halves, 8)),
        ],
        compiler_params=pltpu.CompilerParams(vmem_limit_bytes=32 * MIB),
        name="send_order",
    )(*args)


def fill_turns(d, inner_ref, outer_ref):
    small = series(d * (1.0 / 256.0))
    table = [None, small]
    for j in range(2, AVG):
        table.append(times(table[j // 2], table[j - j // 2]))
    for j in range(1, AVG):
        inner_ref[j - 1, 0] = table[j][0]
        inner_ref[j - 1, 1] = table[j][1]
    c, s = turn_by(d)
    turn = (c * (1.0 / AVG), s * (1.0 / AVG))
    step = series(d * (1.0 / 32.0))
    for o in range(outer_ref.shape[0]):
        outer_ref[o, 0] = turn[0]
        outer_ref[o, 1] = turn[1]
        turn = times(turn, step)


def average_kernel(delay_ref, vis_ref, out_ref, inner_ref, outer_ref):
    fill_turns(delay_ref[...], inner_ref, outer_ref)
    n_out, _, rows, _ = out_ref.shape
    for r in range(0, rows, 16):
        at = slice(r, r + 16)
        table = [(inner_ref[j, 0, at], inner_ref[j, 1, at]) for j in range(AVG - 1)]

        def one(o, carry, at=at, table=table):
            c = o * AVG
            re = vis_ref[c, 0, at].astype(jnp.float32)
            im = vis_ref[c, 1, at].astype(jnp.float32)
            for j in range(1, AVG):
                a = vis_ref[c + j, 0, at].astype(jnp.float32)
                b = vis_ref[c + j, 1, at].astype(jnp.float32)
                tc, ts = table[j - 1]
                re += a * tc - b * ts
                im += a * ts + b * tc
            tc = outer_ref[o, 0, at]
            ts = outer_ref[o, 1, at]
            out_ref[o, 0, at] = (re * tc - im * ts).astype(jnp.bfloat16)
            out_ref[o, 1, at] = (re * ts + im * tc).astype(jnp.bfloat16)
            return carry

        lax.fori_loop(0, n_out, one, 0, unroll=4)


def average(delay, vis):
    n_ch, halves, rows, bv = vis.shape
    n_out = n_ch // AVG
    return pl.pallas_call(
        average_kernel,
        out_shape=jax.ShapeDtypeStruct((n_out, halves, rows, bv), jnp.bfloat16),
        in_specs=[vmem()] * 2,
        out_specs=vmem(),
        scratch_shapes=[
            pltpu.VMEM((AVG - 1, 2, rows, bv), jnp.float32),
            pltpu.VMEM((n_out, 2, rows, bv), jnp.float32),
        ],
        compiler_params=pltpu.CompilerParams(vmem_limit_bytes=12 * MIB),
        name="average",
    )(delay, vis)


def products(n_pieces, column, piece_ref, k_hbm, k_ref, x_ref, c_ref, sem, before):
    n_fetch = sem.shape[1]
    planes, _, width = k_ref.shape
    part = planes // n_fetch
    run = width // 2
    half = k_hbm.shape[2] // 2
    fetches = []
    for i in range(n_fetch):
        at = pl.ds(i * part, part)
        for j in range(2):
            source = k_hbm.at[at, :, pl.ds(j * half + column * run, run)]
            fetches.append(pltpu.make_async_copy(source, k_ref.at[at, :, pl.ds(j * run, run)], sem.at[j, i]))
            fetches[-1].start()
    before()
    c_ref[...] = jnp.zeros_like(c_ref)
    had = jnp.int32(0)
    for i in range(n_pieces):
        if i % STRETCH == 0:
            need = n_fetch if i + STRETCH >= n_pieces else piece_ref[1, i + STRETCH - 1] // part + 1
            for k in range(n_fetch):

                @pl.when((k >= had) & (k < need))
                def _(k=k):
                    fetches[2 * k].wait()
                    fetches[2 * k + 1].wait()

            had = jnp.maximum(had, need)
        at = pl.ds(pl.multiple_of(piece_ref[0, i] * GROUP, GROUP), PIECE)
        product = jnp.dot(x_ref[at, :], k_ref[piece_ref[1, i]], preferred_element_type=jnp.float32)
        c_ref[at, :] = product.astype(jnp.bfloat16)


def sum_tiles(code_ref, c_ref, out_ref):
    n_used = code_ref.shape[1]
    n_codes = out_ref.shape[0] * out_ref.shape[1]
    tiles = to_bf16(iota((n_codes, n_used), 0) == code_ref[...])
    grid = jnp.dot(tiles, c_ref[:n_used, :], preferred_element_type=jnp.float32)
    out_ref[...] = grid.astype(jnp.bfloat16).reshape(out_ref.shape)


def grid_first_kernel(n_pieces, *refs):
    piece_vmem, place_ref, code_ref, rows_ref, k_hbm, out_ref, x_ref, piece_ref, k_ref, c_ref, sem, piece_sem = refs
    fetch = pltpu.make_async_copy(piece_vmem, piece_ref, piece_sem.at[0])
    fetch.start()

    def before():
        n_src, _, per, bv = rows_ref.shape
        re = rows_ref[:, 0].reshape(n_src * per, bv)
        im = rows_ref[:, 1].reshape(n_src * per, bv)
        x = jnp.concatenate([re, im], axis=1)
        order = to_bf16(iota((x_ref.shape[0], n_src * per), 0) == place_ref[...])
        x_ref[...] = jnp.dot(order, x, preferred_element_type=jnp.float32).astype(jnp.bfloat16)
        fetch.wait()

    products(n_pieces, 0, piece_ref, k_hbm, k_ref, x_ref, c_ref, sem, before)
    sum_tiles(code_ref, c_ref, out_ref)


def grid_second_kernel(n_pieces, *refs):
    piece_vmem, code_ref, x_ref, k_hbm, out_ref, piece_ref, k_ref, c_ref, sem, piece_sem = refs
    fetch = pltpu.make_async_copy(piece_vmem, piece_ref, piece_sem.at[0])
    fetch.start()
    products(n_pieces, 1, piece_ref, k_hbm, k_ref, x_ref, c_ref, sem, fetch.wait)
    sum_tiles(code_ref, c_ref, out_ref)


def grid_scratch(piece, n_order, kernels):
    n_planes, k_rows, cells = kernels.shape
    return [
        pltpu.SMEM(piece.shape, jnp.int32),
        pltpu.VMEM((n_planes, k_rows, cells // 2), jnp.bfloat16),
        pltpu.VMEM((n_order, cells // 2), jnp.bfloat16),
        pltpu.SemaphoreType.DMA((2, 4)),
        pltpu.SemaphoreType.DMA((1,)),
    ]


def grid_first(piece, place, code, rows, kernels, n_codes):
    n_planes, k_rows, cells = kernels.shape
    n_rows = place.shape[1]
    n_chan = rows.shape[0]
    n_order, n_used = sizes(n_rows, n_planes)
    return pl.pallas_call(
        functools.partial(grid_first_kernel, n_rows // PIECE + n_planes),
        out_shape=[
            jax.ShapeDtypeStruct((n_chan, n_codes // n_chan, cells // 2), jnp.bfloat16),
            jax.ShapeDtypeStruct((n_order, k_rows), jnp.bfloat16),
        ],
        in_specs=[vmem()] * 4 + [pl.BlockSpec(memory_space=pltpu.HBM)],
        out_specs=[vmem()] * 2,
        scratch_shapes=grid_scratch(piece, n_order, kernels),
        compiler_params=pltpu.CompilerParams(vmem_limit_bytes=32 * MIB),
        name="grid_first",
    )(piece, place, code, rows, pltpu.with_memory_space_constraint(kernels, pltpu.HBM))


def grid_second(piece, code, ordered, kernels, n_rows, n_chan, n_codes):
    n_planes, k_rows, cells = kernels.shape
    n_order, n_used = sizes(n_rows, n_planes)
    return pl.pallas_call(
        functools.partial(grid_second_kernel, n_rows // PIECE + n_planes),
        out_shape=jax.ShapeDtypeStruct((n_chan, n_codes // n_chan, cells // 2), jnp.bfloat16),
        in_specs=[vmem()] * 3 + [pl.BlockSpec(memory_space=pltpu.HBM)],
        out_specs=vmem(),
        scratch_shapes=grid_scratch(piece, n_order, kernels),
        compiler_params=pltpu.CompilerParams(vmem_limit_bytes=32 * MIB),
        name="grid_second",
    )(piece, code, ordered, pltpu.with_memory_space_constraint(kernels, pltpu.HBM))


def strip_kernel(main_ref, out_ref):
    n_out, per, width = main_ref.shape
    low = main_ref[:, :, :128].reshape(n_out * per, 128).astype(jnp.float32)
    high = main_ref[:, :, 128:].reshape(n_out * per, 128).astype(jnp.float32)
    lane = lax.broadcasted_iota(jnp.int32, low.shape, 1)
    strip = jnp.where(lane < STRIP, low, pltpu.roll(high, STRIP, 1)).astype(jnp.bfloat16)
    out_ref[...] = strip.reshape(out_ref.shape)


def strips_of(main):
    n_out, per, _ = main.shape
    return pl.pallas_call(
        strip_kernel,
        out_shape=jax.ShapeDtypeStruct((n_out, per, 2 * STRIP), jnp.bfloat16),
        in_specs=[vmem()],
        out_specs=vmem(),
        compiler_params=pltpu.CompilerParams(vmem_limit_bytes=8 * MIB),
        name="strips",
    )(main)


def join_kernel(nb_ref, first_ref, second_ref, *refs):
    strips, out_ref, strip_ref = refs[:-2], refs[-2], refs[-1]
    n_out, per, width = first_ref.shape
    t_dev = per // 2
    run = width // 2
    n_rows = n_out * t_dev
    for i, ref in enumerate(strips):
        strip_ref[i] = ref[...].reshape(strip_ref.shape[1:])
    upper = iota((n_rows, 2 * STRIP), 1) >= STRIP
    to = iota((n_rows, n_rows), 0)
    place = (iota((n_rows, n_rows), 1) == (to % n_out) * t_dev + to // n_out).astype(jnp.float32)
    quarter = (0.25 * place).astype(jnp.bfloat16)
    place = place.astype(jnp.bfloat16)
    n_nb = nb_ref.shape[1] // 2
    for slot in range(2):
        blend = jnp.zeros((n_rows, 2 * STRIP), jnp.float32)
        for k in range(n_nb):
            strip = strip_ref[nb_ref[slot, k], :, nb_ref[slot, n_nb + k]].reshape(n_rows, 2 * STRIP)
            blend += jnp.dot(quarter, strip, preferred_element_type=jnp.float32)
        swapped = pltpu.roll(blend, STRIP, 1)
        rows = slice(slot * t_dev, (slot + 1) * t_dev)
        first = first_ref[:, rows, :].reshape(n_rows, width)
        first = jnp.dot(place, first, preferred_element_type=jnp.float32)
        second = second_ref[:, rows, :].reshape(n_rows, width)
        second = jnp.dot(place, second, preferred_element_type=jnp.float32)
        parts = [
            first[:, :run],
            second[:, :run] + jnp.where(upper, swapped, 0.0),
            first[:, run:],
            second[:, run:] + jnp.where(upper, blend, 0.0),
        ]
        for i, part in enumerate(parts):
            out_ref[:, slot, :, i * run : (i + 1) * run] = part.reshape(t_dev, n_out, run)


def join(sources, first, second, strips):
    n_out, per, width = first.shape
    assert width == 4 * STRIP
    return pl.pallas_call(
        join_kernel,
        out_shape=jax.ShapeDtypeStruct((per // 2, 2, n_out, 2 * width), jnp.float32),
        in_specs=[pl.BlockSpec(memory_space=pltpu.SMEM)] + [vmem()] * (2 + len(strips)),
        out_specs=vmem(),
        scratch_shapes=[pltpu.VMEM((len(strips), n_out, 2, per // 2, 2 * STRIP), jnp.bfloat16)],
        compiler_params=pltpu.CompilerParams(vmem_limit_bytes=16 * MIB),
        name="join",
    )(sources, first, second, *strips)


def exchange(x, axis):
    return lax.all_to_all(x, axis, split_axis=0, concat_axis=0, tiled=True)


def local(visibilities, kernels, delays, tile_of, plane_of, counts, neighbours):
    n_facet = lax.axis_size("facet")
    n_chan = lax.axis_size("chan")
    facet_index = lax.axis_index("facet")
    halves, facets, blocks, _, bv = visibilities.shape
    fac_dev = facets // n_facet
    n_tiles = 16 * n_chan
    t_dev = n_tiles // n_chan
    n_rows = fac_dev * blocks
    per = n_rows // n_chan

    vis = visibilities.reshape(halves, n_facet * n_chan, per, bv)
    vis, delay, place, code, piece = send_order(
        counts, plane_of, tile_of, delays.reshape(n_chan, per, bv), vis, kernels.shape[0], t_dev
    )
    vis = exchange(vis, ("facet", "chan"))

    rows = exchange(average(delay, vis), "chan")
    n_codes = fac_dev * n_tiles
    grids, ordered = grid_first(piece, place, code, rows, kernels, n_codes)
    first = exchange(grids, "chan")
    grids = grid_second(piece, code, ordered, kernels, n_rows, n_chan, n_codes)

    own = strips_of(first)
    own, grids = lax.optimization_barrier((own, grids))
    second = exchange(grids, "chan")
    chips = n_facet // 2
    strips = [own]
    for dz in range(1, chips):
        strips.append(lax.ppermute(own, "facet", [(f, (f + 2 * dz) % n_facet) for f in range(n_facet)]))
    strips += [lax.ppermute(s, "facet", [(f, f ^ 1) for f in range(n_facet)]) for s in strips]
    mine = lax.dynamic_slice_in_dim(neighbours, facet_index * fac_dev, fac_dev, 0)
    group = mine // fac_dev
    source = (facet_index // 2 - group // 2) % chips + chips * ((group + facet_index) % 2)
    sources = jnp.concatenate([source, mine % fac_dev], axis=1).astype(jnp.int32)
    return join(sources, first, second, strips)


def solution(mesh):
    return jax.shard_map(
        local,
        mesh=mesh,
        in_specs=(
            P(None, None, None, ("facet", "chan"), None),
            P(),
            P("facet", None, None),
            P("facet", None),
            P("facet", None),
            P("facet"),
            P(),
        ),
        out_specs=P("chan", "facet", None, None),
        check_vma=False,
    )
```

```python
import functools
import math

import jax
import jax.numpy as jnp
from jax import lax
from jax.experimental import pallas as pl
from jax.experimental.pallas import tpu as pltpu
from jax.sharding import PartitionSpec as P

AVG = 8
TS = 16
EDGE = 4
STRIP = EDGE * TS
GROUP = 16
PIECE = 64
STRETCH = 8
MIB = 1024 * 1024

SIN = (-1.0 / 6, 1.0 / 120, -1.0 / 5040, 1.0 / 362880, -1.0 / 39916800)
COS = (-1.0 / 2, 1.0 / 24, -1.0 / 720, 1.0 / 40320, -1.0 / 3628800, 1.0 / 479001600)


def series(turns):
    x = (2.0 * math.pi) * turns
    y = x * x
    s = jnp.full_like(x, SIN[-1])
    for k in SIN[-2::-1]:
        s = s * y + k
    c = jnp.full_like(x, COS[-1])
    for k in COS[-2::-1]:
        c = c * y + k
    return c * y + 1.0, (s * y + 1.0) * x


def turn_by(turns):
    half = jnp.round(2.0 * turns)
    c, s = series(turns - 0.5 * half)
    odd = (half - 2.0 * jnp.floor(0.5 * half)) > 0.5
    sign = jnp.where(odd, -1.0, 1.0)
    return c * sign, s * sign


def times(a, b):
    return a[0] * b[0] - a[1] * b[1], a[0] * b[1] + a[1] * b[0]


def vmem():
    return pl.BlockSpec(memory_space=pltpu.VMEM)


def to_bf16(mask):
    return mask.astype(jnp.float32).astype(jnp.bfloat16)


def iota(shape, dim):
    return lax.broadcasted_iota(jnp.int32, shape, dim)


def fill_tables(n_planes, n_order, t_dev, count_ref, plane_ref, tile_ref, order_ref, tiles_ref, piece_ref):
    f32 = jnp.float32
    slots, blocks = plane_ref.shape
    n_rows = slots * blocks
    planes, tiles = [], []
    for slot in range(slots):
        alive = iota((1, blocks), 1) < count_ref[slot]
        planes.append(jnp.where(alive, plane_ref[slot : slot + 1, :], -1))
        tiles.append(tile_ref[slot : slot + 1, :])
    plane = jnp.concatenate(planes, axis=1)
    tile = jnp.concatenate(tiles, axis=1)
    mine = plane == iota((n_planes, n_rows), 0)
    before = to_bf16(iota((n_rows, n_rows), 0) < iota((n_rows, n_rows), 1))
    rank = jnp.dot(to_bf16(mine), before, preferred_element_type=f32)
    count = jnp.sum(mine.astype(f32), axis=1, keepdims=True)
    groups = jnp.floor((count + (GROUP - 1)) * (1.0 / GROUP))
    pieces = jnp.floor((groups + (PIECE // GROUP - 1)) * (GROUP / PIECE))
    earlier = to_bf16(iota((n_planes, n_planes), 1) < iota((n_planes, n_planes), 0))
    both = jnp.concatenate(
        [jnp.broadcast_to(groups, (n_planes, 128)), jnp.broadcast_to(pieces, (n_planes, 128))], axis=1
    )
    both = jnp.dot(earlier, both.astype(jnp.bfloat16), preferred_element_type=f32)
    first_group = both[:, 0:1]
    first_piece = both[:, 128:129]
    place = jnp.sum(jnp.where(mine, rank + GROUP * first_group, 0.0), axis=0, keepdims=True)
    live = jnp.sum(mine.astype(f32), axis=0, keepdims=True)
    place = jnp.where(live > 0.5, place, -1.0).astype(jnp.int32)
    order = to_bf16(iota((n_order, n_rows), 0) == place)
    order_ref[...] = order

    row = iota((8, n_rows), 0)
    slot = (iota((8, n_rows), 1) >= n_rows // 2).astype(f32)
    values = jnp.where(row == 0, tile.astype(f32) + 1.0, jnp.where(row == 1, slot, 0.0))
    n_codes, n_used = tiles_ref.shape
    ordered = lax.dot_general(
        values.astype(jnp.bfloat16), order[:n_used], (((1,), (1,)), ((), ())), preferred_element_type=f32
    )
    tile = ordered[0:1].astype(jnp.int32) - 1
    slot = ordered[1:2].astype(jnp.int32)
    code = (tile // t_dev) * (2 * t_dev) + slot * t_dev + tile % t_dev
    code = jnp.where(tile < 0, -1, code)
    tiles_ref[...] = to_bf16(iota((n_codes, n_used), 0) == code)

    lower = jnp.sum(jnp.where(iota((n_planes, 1), 0) < n_planes // 2, pieces, 0.0))
    upper = jnp.sum(pieces) - lower
    lane = iota((n_planes, 128), 1)
    at = (lane % 64).astype(f32)
    is_upper = lane >= 64
    which = jnp.minimum(at, jnp.where(is_upper, upper, lower) - 1.0) + jnp.where(is_upper, lower, 0.0)
    taken = (which >= first_piece) & (which < first_piece + pieces)
    group = first_group + (PIECE // GROUP) * (which - first_piece)
    group = jnp.sum(jnp.where(taken, group, 0.0), axis=0, keepdims=True)
    owner = jnp.sum(jnp.where(taken, iota((n_planes, 128), 0).astype(f32), 0.0), axis=0, keepdims=True)
    owner = owner - jnp.where(iota((1, 128), 1) >= 64, float(n_planes // 2), 0.0)
    row = iota((8, 128), 0)
    totals = jnp.where(iota((8, 128), 1) >= 64, upper, lower)
    value = jnp.where(row == 0, group, jnp.where(row == 1, jnp.maximum(owner, 0.0), jnp.where(row == 2, totals, 0.0)))
    piece_ref[...] = value.astype(jnp.int32)


def sizes(n_rows, n_planes):
    used = n_rows + n_planes * (GROUP - 1)
    n_order = -(-(used - GROUP + PIECE) // 32) * 32
    n_used = -(-used // 256) * 256
    assert n_used <= n_order
    return n_order, n_used


def send_kernel(n_planes, n_order, t_dev, *refs):
    (count_hbm, plane_hbm, tile_hbm, delay_hbm, vis_hbm), refs = refs[:5], refs[5:]
    (out_ref, delay_ref, *tables), (count_ref, plane_ref, tile_ref, small_sem, sem) = refs[:-5], refs[-5:]
    smalls = [
        pltpu.make_async_copy(count_hbm, count_ref, small_sem.at[0]),
        pltpu.make_async_copy(plane_hbm, plane_ref, small_sem.at[1]),
        pltpu.make_async_copy(tile_hbm, tile_ref, small_sem.at[2]),
        pltpu.make_async_copy(delay_hbm.at[lax.axis_index("chan")], delay_ref, small_sem.at[3]),
    ]
    for copy in smalls:
        copy.start()
    halves, dests = vis_hbm.shape[:2]
    n = sem.shape[1]
    copies = []
    for i in range(n):
        at = pl.ds(i * (dests // n), dests // n)
        for h in range(halves):
            copies.append(pltpu.make_async_copy(vis_hbm.at[h, at], out_ref.at[at, h], sem.at[h, i]))
            copies[-1].start()
    for copy in smalls:
        copy.wait()
    fill_tables(n_planes, n_order, t_dev, count_ref, plane_ref, tile_ref, *tables)
    for copy in copies:
        copy.wait()


def send_order(counts, planes, tiles, delays, vis, n_planes, n_codes, t_dev):
    halves, dests, rows, bv = vis.shape
    n_rows = planes.shape[0] * planes.shape[1]
    n_order, n_used = sizes(n_rows, n_planes)
    args = [pltpu.with_memory_space_constraint(x, pltpu.HBM) for x in (counts, planes, tiles, delays, vis)]
    return pl.pallas_call(
        functools.partial(send_kernel, n_planes, n_order, t_dev),
        out_shape=[
            jax.ShapeDtypeStruct((dests, halves, rows, bv), vis.dtype),
            jax.ShapeDtypeStruct(delays.shape[1:], delays.dtype),
            jax.ShapeDtypeStruct((n_order, n_rows), jnp.bfloat16),
            jax.ShapeDtypeStruct((n_codes, n_used), jnp.bfloat16),
            jax.ShapeDtypeStruct((8, 128), jnp.int32),
        ],
        in_specs=[pl.BlockSpec(memory_space=pltpu.HBM)] * len(args),
        out_specs=[vmem()] * 5,
        scratch_shapes=[
            pltpu.SMEM(counts.shape, jnp.int32),
            pltpu.VMEM(planes.shape, jnp.int32),
            pltpu.VMEM(tiles.shape, jnp.int32),
            pltpu.SemaphoreType.DMA((4,)),
            pltpu.SemaphoreType.DMA((halves, 8)),
        ],
        compiler_params=pltpu.CompilerParams(vmem_limit_bytes=32 * MIB),
        name="send_order",
    )(*args)


def fill_turns(d, inner_ref, outer_ref):
    small = series(d * (1.0 / 256.0))
    table = [None, small]
    for j in range(2, AVG):
        table.append(times(table[j // 2], table[j - j // 2]))
    for j in range(1, AVG):
        inner_ref[j - 1, 0] = table[j][0]
        inner_ref[j - 1, 1] = table[j][1]
    c, s = turn_by(d)
    turn = (c * (1.0 / AVG), s * (1.0 / AVG))
    step = series(d * (1.0 / 32.0))
    for o in range(outer_ref.shape[0]):
        outer_ref[o, 0] = turn[0]
        outer_ref[o, 1] = turn[1]
        turn = times(turn, step)


def fetch_matrices(k_hbm, first, k_ref, sem):
    n_fetch = sem.shape[0]
    part = k_ref.shape[0] // n_fetch
    fetches = []
    for i in range(n_fetch):
        source = k_hbm.at[pl.ds(first + i * part, part)]
        fetches.append(pltpu.make_async_copy(source, k_ref.at[pl.ds(i * part, part)], sem.at[i]))
        fetches[-1].start()
    return fetches


def average_kernel(delay_ref, vis_ref, k_hbm, out_ref, k_ref, inner_ref, outer_ref, sem):
    fetches = fetch_matrices(k_hbm, 0, k_ref, sem)
    fill_turns(delay_ref[...], inner_ref, outer_ref)
    n_out, _, rows, _ = out_ref.shape
    for r in range(0, rows, 16):
        at = slice(r, r + 16)
        table = [(inner_ref[j, 0, at], inner_ref[j, 1, at]) for j in range(AVG - 1)]

        def one(o, carry, at=at, table=table):
            c = o * AVG
            re = vis_ref[c, 0, at].astype(jnp.float32)
            im = vis_ref[c, 1, at].astype(jnp.float32)
            for j in range(1, AVG):
                a = vis_ref[c + j, 0, at].astype(jnp.float32)
                b = vis_ref[c + j, 1, at].astype(jnp.float32)
                tc, ts = table[j - 1]
                re += a * tc - b * ts
                im += a * ts + b * tc
            tc = outer_ref[o, 0, at]
            ts = outer_ref[o, 1, at]
            out_ref[o, 0, at] = (re * tc - im * ts).astype(jnp.bfloat16)
            out_ref[o, 1, at] = (re * ts + im * tc).astype(jnp.bfloat16)
            return carry

        lax.fori_loop(0, n_out, one, 0, unroll=4)
    for fetch in fetches:
        fetch.wait()


def average(delay, vis, kernels):
    n_ch, halves, rows, bv = vis.shape
    n_out = n_ch // AVG
    n_planes, k_rows, cells = kernels.shape
    return pl.pallas_call(
        average_kernel,
        out_shape=[
            jax.ShapeDtypeStruct((n_out, halves, rows, bv), jnp.bfloat16),
            jax.ShapeDtypeStruct((n_planes // 2, k_rows, cells), kernels.dtype),
        ],
        in_specs=[vmem()] * 2 + [pl.BlockSpec(memory_space=pltpu.HBM)],
        out_specs=[vmem()] * 2,
        scratch_shapes=[
            pltpu.VMEM((AVG - 1, 2, rows, bv), jnp.float32),
            pltpu.VMEM((n_out, 2, rows, bv), jnp.float32),
            pltpu.SemaphoreType.DMA((4,)),
        ],
        compiler_params=pltpu.CompilerParams(vmem_limit_bytes=16 * MIB),
        name="average",
    )(delay, vis, pltpu.with_memory_space_constraint(kernels, pltpu.HBM))


def grid_kernel(n_pieces, *refs):
    piece_vmem, rows_ref, order_ref, tiles_ref, low_ref, k_hbm, out_ref, piece_ref, high_ref, x_ref, c_ref, sem, piece_sem = refs
    piece_copy = pltpu.make_async_copy(piece_vmem, piece_ref, piece_sem.at[0])
    piece_copy.start()
    fetches = fetch_matrices(k_hbm, low_ref.shape[0], high_ref, sem)
    n_src, _, per, bv = rows_ref.shape
    re = rows_ref[:, 0].reshape(n_src * per, bv)
    im = rows_ref[:, 1].reshape(n_src * per, bv)
    x = jnp.concatenate([re, im], axis=1)
    x_ref[...] = jnp.dot(order_ref[...], x, preferred_element_type=jnp.float32).astype(jnp.bfloat16)
    c_ref[...] = jnp.zeros_like(c_ref)
    piece_copy.wait()
    for lane, k_ref in ((0, low_ref), (64, high_ref)):
        if lane:
            for fetch in fetches:
                fetch.wait()
        for begin in range(0, n_pieces, STRETCH):

            @pl.when(begin < piece_ref[2, lane])
            def _(begin=begin, lane=lane, k_ref=k_ref):
                for i in range(lane + begin, lane + min(begin + STRETCH, n_pieces)):
                    at = pl.ds(pl.multiple_of(piece_ref[0, i] * GROUP, GROUP), PIECE)
                    product = jnp.dot(x_ref[at, :], k_ref[piece_ref[1, i]], preferred_element_type=jnp.float32)
                    c_ref[at, :] = product.astype(jnp.bfloat16)

    grid = jnp.dot(tiles_ref[...], c_ref[: tiles_ref.shape[1], :], preferred_element_type=jnp.float32)
    out_ref[...] = grid.astype(jnp.bfloat16).reshape(out_ref.shape)


def grid_rows(piece, rows, order, tiles, low, kernels):
    n_planes, k_rows, cells = kernels.shape
    n_order, n_rows = order.shape
    n_chan = rows.shape[0]
    n_pieces = n_rows // PIECE + n_planes // 2
    assert n_pieces <= 64
    return pl.pallas_call(
        functools.partial(grid_kernel, n_pieces),
        out_shape=jax.ShapeDtypeStruct((n_chan, tiles.shape[0] // n_chan, cells), jnp.bfloat16),
        in_specs=[vmem()] * 5 + [pl.BlockSpec(memory_space=pltpu.HBM)],
        out_specs=vmem(),
        scratch_shapes=[
            pltpu.SMEM(piece.shape, jnp.int32),
            pltpu.VMEM(low.shape, low.dtype),
            pltpu.VMEM((n_order, k_rows), jnp.bfloat16),
            pltpu.VMEM((n_order, cells), jnp.bfloat16),
            pltpu.SemaphoreType.DMA((4,)),
            pltpu.SemaphoreType.DMA((1,)),
        ],
        compiler_params=pltpu.CompilerParams(vmem_limit_bytes=24 * MIB),
        name="grid_rows",
    )(piece, rows, order, tiles, low, pltpu.with_memory_space_constraint(kernels, pltpu.HBM))


def strip_kernel(main_ref, out_ref):
    n_out, per, cells = main_ref.shape
    half = cells // 2
    low = main_ref[:, :, :128].reshape(n_out * per, 128).astype(jnp.float32)
    high = main_ref[:, :, half : half + 128].reshape(n_out * per, 128).astype(jnp.float32)
    lane = lax.broadcasted_iota(jnp.int32, low.shape, 1)
    strip = jnp.where(lane < STRIP, low, pltpu.roll(high, STRIP, 1)).astype(jnp.bfloat16)
    out_ref[...] = strip.reshape(out_ref.shape)


def strips_of(main):
    n_out, per, _ = main.shape
    return pl.pallas_call(
        strip_kernel,
        out_shape=jax.ShapeDtypeStruct((n_out, per, 2 * STRIP), jnp.bfloat16),
        in_specs=[vmem()],
        out_specs=vmem(),
        compiler_params=pltpu.CompilerParams(vmem_limit_bytes=8 * MIB),
        name="strips",
    )(main)


def placing(n_out, t_dev):
    n_rows = n_out * t_dev
    to = iota((n_rows, n_rows), 0)
    return (iota((n_rows, n_rows), 1) == (to % n_out) * t_dev + to // n_out).astype(jnp.float32)


def place_kernel(main_ref, out_hbm, rest_ref, done_ref, sem):
    n_out, per, cells = main_ref.shape
    t_dev = per // 2
    run = cells // 4
    place = placing(n_out, t_dev).astype(jnp.bfloat16)
    copies = []
    for slot in range(2):
        main = main_ref[:, slot * t_dev : (slot + 1) * t_dev, :].reshape(n_out * t_dev, cells)
        main = jnp.dot(place, main, preferred_element_type=jnp.float32)
        for i in range(2):
            at = slice(2 * i * run, (2 * i + 1) * run)
            done_ref[i, :, slot] = main[:, at].reshape(t_dev, n_out, run)
            rest_ref[i, :, slot] = main[:, at.stop : at.stop + run].reshape(t_dev, n_out, run)
    for i in range(2):
        copies.append(pltpu.make_async_copy(done_ref.at[i], out_hbm.at[:, :, :, pl.ds(2 * i * run, run)], sem.at[i]))
        copies[-1].start()
    for copy in copies:
        copy.wait()


def place_main(main):
    n_out, per, cells = main.shape
    part = (2, per // 2, 2, n_out, cells // 4)
    return pl.pallas_call(
        place_kernel,
        out_shape=[
            pltpu.HBM((per // 2, 2, n_out, cells), jnp.float32),
            jax.ShapeDtypeStruct(part, jnp.float32),
        ],
        in_specs=[vmem()],
        out_specs=[pl.BlockSpec(memory_space=pltpu.HBM), vmem()],
        scratch_shapes=[pltpu.VMEM(part, jnp.float32), pltpu.SemaphoreType.DMA((2,))],
        compiler_params=pltpu.CompilerParams(vmem_limit_bytes=8 * MIB),
        name="place",
    )(main)


def join_kernel(nb_ref, placed_hbm, rest_ref, *refs):
    strips, (out_hbm, strip_ref, done_ref, sem) = refs[:-4], refs[-4:]
    _, t_dev, _, n_out, run = rest_ref.shape
    n_rows = n_out * t_dev
    for i, ref in enumerate(strips):
        strip_ref[i] = ref[...].reshape(strip_ref.shape[1:])
    upper = iota((n_rows, 2 * STRIP), 1) >= STRIP
    quarter = (0.25 * placing(n_out, t_dev)).astype(jnp.bfloat16)
    n_nb = nb_ref.shape[1] // 2
    copies = []
    for slot in range(2):
        blend = jnp.zeros((n_rows, 2 * STRIP), jnp.float32)
        for k in range(n_nb):
            strip = strip_ref[nb_ref[slot, k], :, nb_ref[slot, n_nb + k]].reshape(n_rows, 2 * STRIP)
            blend += jnp.dot(quarter, strip, preferred_element_type=jnp.float32)
        for i, part in enumerate((pltpu.roll(blend, STRIP, 1), blend)):
            part = jnp.where(upper, part, 0.0).reshape(t_dev, n_out, run)
            done_ref[i, :, slot] = rest_ref[i, :, slot] + part
            target = out_hbm.at[:, slot, :, pl.ds((2 * i + 1) * run, run)]
            copies.append(pltpu.make_async_copy(done_ref.at[i, :, slot], target, sem.at[slot, i]))
            copies[-1].start()
    for copy in copies:
        copy.wait()


def join(sources, placed, rest, strips):
    _, t_dev, _, n_out, run = rest.shape
    assert run == 2 * STRIP
    return pl.pallas_call(
        join_kernel,
        out_shape=pltpu.HBM(placed.shape, placed.dtype),
        in_specs=[pl.BlockSpec(memory_space=pltpu.SMEM), pl.BlockSpec(memory_space=pltpu.HBM)]
        + [vmem()] * (1 + len(strips)),
        out_specs=pl.BlockSpec(memory_space=pltpu.HBM),
        scratch_shapes=[
            pltpu.VMEM((len(strips), n_out, 2, t_dev, 2 * STRIP), jnp.bfloat16),
            pltpu.VMEM(rest.shape, jnp.float32),
            pltpu.SemaphoreType.DMA((2, 2)),
        ],
        input_output_aliases={1: 0},
        compiler_params=pltpu.CompilerParams(vmem_limit_bytes=16 * MIB),
        name="join",
    )(sources, placed, rest, *strips)


def exchange(x, axis):
    return lax.all_to_all(x, axis, split_axis=0, concat_axis=0, tiled=True)


def local(visibilities, kernels, delays, tile_of, plane_of, counts, neighbours):
    n_facet = lax.axis_size("facet")
    n_chan = lax.axis_size("chan")
    facet_index = lax.axis_index("facet")
    halves, facets, blocks, _, bv = visibilities.shape
    fac_dev = facets // n_facet
    n_tiles = 16 * n_chan
    t_dev = n_tiles // n_chan
    n_rows = fac_dev * blocks
    per = n_rows // n_chan

    vis = visibilities.reshape(halves, n_facet * n_chan, per, bv)
    vis, delay, order, tiles, piece = send_order(
        counts,
        plane_of,
        tile_of,
        delays.reshape(n_chan, per, bv),
        vis,
        kernels.shape[0],
        fac_dev * n_tiles,
        t_dev,
    )
    vis = exchange(vis, ("facet", "chan"))

    rows, low = average(delay, vis, kernels)
    rows = exchange(rows, "chan")
    main = exchange(grid_rows(piece, rows, order, tiles, low, kernels), "chan")

    own = strips_of(main)
    chips = n_facet // 2
    strips = [own]
    for dz in range(1, chips):
        strips.append(lax.ppermute(own, "facet", [(f, (f + 2 * dz) % n_facet) for f in range(n_facet)]))
    strips += [lax.ppermute(s, "facet", [(f, f ^ 1) for f in range(n_facet)]) for s in strips]
    mine = lax.dynamic_slice_in_dim(neighbours, facet_index * fac_dev, fac_dev, 0)
    group = mine // fac_dev
    source = (facet_index // 2 - group // 2) % chips + chips * ((group + facet_index) % 2)
    sources = jnp.concatenate([source, mine % fac_dev], axis=1).astype(jnp.int32)
    placed, rest = place_main(main)
    return join(sources, placed, rest, strips)


def solution(mesh):
    return jax.shard_map(
        local,
        mesh=mesh,
        in_specs=(
            P(None, None, None, ("facet", "chan"), None),
            P(),
            P("facet", None, None),
            P("facet", None),
            P("facet", None),
            P("facet"),
            P(),
        ),
        out_specs=P("chan", "facet", None, None),
        check_vma=False,
    )
```

```python
import functools
import math

import jax
import jax.numpy as jnp
from jax import lax
from jax.experimental import pallas as pl
from jax.experimental.pallas import tpu as pltpu
from jax.sharding import PartitionSpec as P

AVG = 8
TS = 16
EDGE = 4
STRIP = EDGE * TS
GROUP = 16
PIECE = 64
STRETCH = 8
MIB = 1024 * 1024

SIN = (-1.0 / 6, 1.0 / 120, -1.0 / 5040, 1.0 / 362880, -1.0 / 39916800)
COS = (-1.0 / 2, 1.0 / 24, -1.0 / 720, 1.0 / 40320, -1.0 / 3628800, 1.0 / 479001600)


def series(turns):
    x = (2.0 * math.pi) * turns
    y = x * x
    s = jnp.full_like(x, SIN[-1])
    for k in SIN[-2::-1]:
        s = s * y + k
    c = jnp.full_like(x, COS[-1])
    for k in COS[-2::-1]:
        c = c * y + k
    return c * y + 1.0, (s * y + 1.0) * x


def turn_by(turns):
    half = jnp.round(2.0 * turns)
    c, s = series(turns - 0.5 * half)
    odd = (half - 2.0 * jnp.floor(0.5 * half)) > 0.5
    sign = jnp.where(odd, -1.0, 1.0)
    return c * sign, s * sign


def times(a, b):
    return a[0] * b[0] - a[1] * b[1], a[0] * b[1] + a[1] * b[0]


def vmem():
    return pl.BlockSpec(memory_space=pltpu.VMEM)


def to_bf16(mask):
    return mask.astype(jnp.float32).astype(jnp.bfloat16)


def iota(shape, dim):
    return lax.broadcasted_iota(jnp.int32, shape, dim)


def fill_tables(n_planes, t_dev, count_ref, plane_ref, tile_ref, place_ref, code_ref, piece_ref):
    f32 = jnp.float32
    slots, blocks = plane_ref.shape
    n_rows = slots * blocks
    planes, tiles = [], []
    for slot in range(slots):
        alive = iota((1, blocks), 1) < count_ref[slot]
        planes.append(jnp.where(alive, plane_ref[slot : slot + 1, :], -1))
        tiles.append(tile_ref[slot : slot + 1, :])
    plane = jnp.concatenate(planes, axis=1)
    tile = jnp.concatenate(tiles, axis=1)
    mine = plane == iota((n_planes, n_rows), 0)
    before = to_bf16(iota((n_rows, n_rows), 0) < iota((n_rows, n_rows), 1))
    rank = jnp.dot(to_bf16(mine), before, preferred_element_type=f32)
    count = jnp.sum(mine.astype(f32), axis=1, keepdims=True)
    groups = jnp.floor((count + (GROUP - 1)) * (1.0 / GROUP))
    pieces = jnp.floor((groups + (PIECE // GROUP - 1)) * (GROUP / PIECE))
    earlier = to_bf16(iota((n_planes, n_planes), 1) < iota((n_planes, n_planes), 0))
    both = jnp.concatenate(
        [jnp.broadcast_to(groups, (n_planes, 128)), jnp.broadcast_to(pieces, (n_planes, 128))], axis=1
    )
    both = jnp.dot(earlier, both.astype(jnp.bfloat16), preferred_element_type=f32)
    first_group = both[:, 0:1]
    first_piece = both[:, 128:129]
    place = jnp.sum(jnp.where(mine, rank + GROUP * first_group, 0.0), axis=0, keepdims=True)
    live = jnp.sum(mine.astype(f32), axis=0, keepdims=True)
    place = jnp.where(live > 0.5, place, -1.0).astype(jnp.int32)
    place_ref[...] = place
    n_used = code_ref.shape[1]
    order = to_bf16(iota((n_used, n_rows), 0) == place)

    row = iota((8, n_rows), 0)
    slot = (iota((8, n_rows), 1) >= n_rows // 2).astype(f32)
    values = jnp.where(row == 0, tile.astype(f32) + 1.0, jnp.where(row == 1, slot, 0.0))
    ordered = lax.dot_general(
        values.astype(jnp.bfloat16), order, (((1,), (1,)), ((), ())), preferred_element_type=f32
    )
    tile = ordered[0:1].astype(jnp.int32) - 1
    slot = ordered[1:2].astype(jnp.int32)
    code = (tile // t_dev) * (2 * t_dev) + slot * t_dev + tile % t_dev
    code_ref[...] = jnp.where(tile < 0, -1, code)

    lower = jnp.sum(jnp.where(iota((n_planes, 1), 0) < n_planes // 2, pieces, 0.0))
    upper = jnp.sum(pieces) - lower
    lane = iota((n_planes, 128), 1)
    at = (lane % 64).astype(f32)
    is_upper = lane >= 64
    which = jnp.minimum(at, jnp.where(is_upper, upper, lower) - 1.0) + jnp.where(is_upper, lower, 0.0)
    taken = (which >= first_piece) & (which < first_piece + pieces)
    group = first_group + (PIECE // GROUP) * (which - first_piece)
    group = jnp.sum(jnp.where(taken, group, 0.0), axis=0, keepdims=True)
    owner = jnp.sum(jnp.where(taken, iota((n_planes, 128), 0).astype(f32), 0.0), axis=0, keepdims=True)
    owner = owner - jnp.where(iota((1, 128), 1) >= 64, float(n_planes // 2), 0.0)
    row = iota((8, 128), 0)
    totals = jnp.where(iota((8, 128), 1) >= 64, upper, lower)
    value = jnp.where(row == 0, group, jnp.where(row == 1, jnp.maximum(owner, 0.0), jnp.where(row == 2, totals, 0.0)))
    piece_ref[...] = value.astype(jnp.int32)


def sizes(n_rows, n_planes):
    used = n_rows + n_planes * (GROUP - 1)
    n_order = -(-(used - GROUP + PIECE) // 32) * 32
    n_used = -(-used // 256) * 256
    assert n_used <= n_order
    return n_order, n_used


def send_kernel(n_planes, t_dev, *refs):
    (count_hbm, plane_hbm, tile_hbm, delay_hbm, vis_hbm), refs = refs[:5], refs[5:]
    (out_ref, delay_ref, *tables), (count_ref, plane_ref, tile_ref, small_sem, sem) = refs[:-5], refs[-5:]
    smalls = [
        pltpu.make_async_copy(count_hbm, count_ref, small_sem.at[0]),
        pltpu.make_async_copy(plane_hbm, plane_ref, small_sem.at[1]),
        pltpu.make_async_copy(tile_hbm, tile_ref, small_sem.at[2]),
        pltpu.make_async_copy(delay_hbm.at[lax.axis_index("chan")], delay_ref, small_sem.at[3]),
    ]
    for copy in smalls:
        copy.start()
    halves, dests = vis_hbm.shape[:2]
    n = sem.shape[1]
    copies = []
    for i in range(n):
        at = pl.ds(i * (dests // n), dests // n)
        for h in range(halves):
            copies.append(pltpu.make_async_copy(vis_hbm.at[h, at], out_ref.at[at, h], sem.at[h, i]))
            copies[-1].start()
    for copy in smalls:
        copy.wait()
    fill_tables(n_planes, t_dev, count_ref, plane_ref, tile_ref, *tables)
    for copy in copies:
        copy.wait()


def send_order(counts, planes, tiles, delays, vis, n_planes, t_dev):
    halves, dests, rows, bv = vis.shape
    n_rows = planes.shape[0] * planes.shape[1]
    n_order, n_used = sizes(n_rows, n_planes)
    args = [pltpu.with_memory_space_constraint(x, pltpu.HBM) for x in (counts, planes, tiles, delays, vis)]
    return pl.pallas_call(
        functools.partial(send_kernel, n_planes, t_dev),
        out_shape=[
            jax.ShapeDtypeStruct((dests, halves, rows, bv), vis.dtype),
            jax.ShapeDtypeStruct(delays.shape[1:], delays.dtype),
            jax.ShapeDtypeStruct((1, n_rows), jnp.int32),
            jax.ShapeDtypeStruct((1, n_used), jnp.int32),
            jax.ShapeDtypeStruct((8, 128), jnp.int32),
        ],
        in_specs=[pl.BlockSpec(memory_space=pltpu.HBM)] * len(args),
        out_specs=[vmem()] * 5,
        scratch_shapes=[
            pltpu.SMEM(counts.shape, jnp.int32),
            pltpu.VMEM(planes.shape, jnp.int32),
            pltpu.VMEM(tiles.shape, jnp.int32),
            pltpu.SemaphoreType.DMA((4,)),
            pltpu.SemaphoreType.DMA((halves, 8)),
        ],
        compiler_params=pltpu.CompilerParams(vmem_limit_bytes=32 * MIB),
        name="send_order",
    )(*args)


def fill_turns(d, inner_ref, outer_ref):
    small = series(d * (1.0 / 256.0))
    table = [None, small]
    for j in range(2, AVG):
        table.append(times(table[j // 2], table[j - j // 2]))
    for j in range(1, AVG):
        inner_ref[j - 1, 0] = table[j][0]
        inner_ref[j - 1, 1] = table[j][1]
    c, s = turn_by(d)
    turn = (c * (1.0 / AVG), s * (1.0 / AVG))
    step = series(d * (1.0 / 32.0))
    for o in range(outer_ref.shape[0]):
        outer_ref[o, 0] = turn[0]
        outer_ref[o, 1] = turn[1]
        turn = times(turn, step)


def fetch_matrices(k_hbm, first, k_ref, sem):
    n_fetch = sem.shape[0]
    part = k_ref.shape[0] // n_fetch
    fetches = []
    for i in range(n_fetch):
        source = k_hbm.at[pl.ds(first + i * part, part)]
        fetches.append(pltpu.make_async_copy(source, k_ref.at[pl.ds(i * part, part)], sem.at[i]))
        fetches[-1].start()
    return fetches


def average_kernel(delay_ref, vis_ref, k_hbm, out_ref, k_ref, inner_ref, outer_ref, sem):
    fetches = fetch_matrices(k_hbm, 0, k_ref, sem)
    fill_turns(delay_ref[...], inner_ref, outer_ref)
    n_out, _, rows, _ = out_ref.shape
    for r in range(0, rows, 16):
        at = slice(r, r + 16)
        table = [(inner_ref[j, 0, at], inner_ref[j, 1, at]) for j in range(AVG - 1)]

        def one(o, carry, at=at, table=table):
            c = o * AVG
            re = vis_ref[c, 0, at].astype(jnp.float32)
            im = vis_ref[c, 1, at].astype(jnp.float32)
            for j in range(1, AVG):
                a = vis_ref[c + j, 0, at].astype(jnp.float32)
                b = vis_ref[c + j, 1, at].astype(jnp.float32)
                tc, ts = table[j - 1]
                re += a * tc - b * ts
                im += a * ts + b * tc
            tc = outer_ref[o, 0, at]
            ts = outer_ref[o, 1, at]
            out_ref[o, 0, at] = (re * tc - im * ts).astype(jnp.bfloat16)
            out_ref[o, 1, at] = (re * ts + im * tc).astype(jnp.bfloat16)
            return carry

        lax.fori_loop(0, n_out, one, 0, unroll=4)
    for fetch in fetches:
        fetch.wait()


def average(delay, vis, kernels):
    n_ch, halves, rows, bv = vis.shape
    n_out = n_ch // AVG
    n_planes, k_rows, cells = kernels.shape
    return pl.pallas_call(
        average_kernel,
        out_shape=[
            jax.ShapeDtypeStruct((n_out, halves, rows, bv), jnp.bfloat16),
            jax.ShapeDtypeStruct((n_planes // 2, k_rows, cells), kernels.dtype),
        ],
        in_specs=[vmem()] * 2 + [pl.BlockSpec(memory_space=pltpu.HBM)],
        out_specs=[vmem()] * 2,
        scratch_shapes=[
            pltpu.VMEM((AVG - 1, 2, rows, bv), jnp.float32),
            pltpu.VMEM((n_out, 2, rows, bv), jnp.float32),
            pltpu.SemaphoreType.DMA((4,)),
        ],
        compiler_params=pltpu.CompilerParams(vmem_limit_bytes=16 * MIB),
        name="average",
    )(delay, vis, pltpu.with_memory_space_constraint(kernels, pltpu.HBM))


def grid_kernel(n_pieces, *refs):
    piece_vmem, rows_ref, place_ref, code_ref, low_ref, k_hbm, out_ref, piece_ref, high_ref, x_ref, c_ref, sem, piece_sem = refs
    piece_copy = pltpu.make_async_copy(piece_vmem, piece_ref, piece_sem.at[0])
    piece_copy.start()
    fetches = fetch_matrices(k_hbm, low_ref.shape[0], high_ref, sem)
    n_src, _, per, bv = rows_ref.shape
    re = rows_ref[:, 0].reshape(n_src * per, bv)
    im = rows_ref[:, 1].reshape(n_src * per, bv)
    x = jnp.concatenate([re, im], axis=1)
    order = to_bf16(iota((x_ref.shape[0], n_src * per), 0) == place_ref[...])
    x_ref[...] = jnp.dot(order, x, preferred_element_type=jnp.float32).astype(jnp.bfloat16)
    c_ref[...] = jnp.zeros_like(c_ref)
    piece_copy.wait()
    for lane, k_ref in ((0, low_ref), (64, high_ref)):
        if lane:
            for fetch in fetches:
                fetch.wait()
        for begin in range(0, n_pieces, STRETCH):

            @pl.when(begin < piece_ref[2, lane])
            def _(begin=begin, lane=lane, k_ref=k_ref):
                for i in range(lane + begin, lane + min(begin + STRETCH, n_pieces)):
                    at = pl.ds(pl.multiple_of(piece_ref[0, i] * GROUP, GROUP), PIECE)
                    product = jnp.dot(x_ref[at, :], k_ref[piece_ref[1, i]], preferred_element_type=jnp.float32)
                    c_ref[at, :] = product.astype(jnp.bfloat16)

    n_used = code_ref.shape[1]
    tiles = to_bf16(iota((out_ref.shape[0] * out_ref.shape[1], n_used), 0) == code_ref[...])
    grid = jnp.dot(tiles, c_ref[:n_used, :], preferred_element_type=jnp.float32)
    out_ref[...] = grid.astype(jnp.bfloat16).reshape(out_ref.shape)


def grid_rows(piece, rows, place, code, low, kernels, n_codes):
    n_planes, k_rows, cells = kernels.shape
    n_rows = place.shape[1]
    n_order, _ = sizes(n_rows, n_planes)
    n_chan = rows.shape[0]
    n_pieces = n_rows // PIECE + n_planes // 2
    assert n_pieces <= 64
    return pl.pallas_call(
        functools.partial(grid_kernel, n_pieces),
        out_shape=jax.ShapeDtypeStruct((n_chan, n_codes // n_chan, cells), jnp.bfloat16),
        in_specs=[vmem()] * 5 + [pl.BlockSpec(memory_space=pltpu.HBM)],
        out_specs=vmem(),
        scratch_shapes=[
            pltpu.SMEM(piece.shape, jnp.int32),
            pltpu.VMEM(low.shape, low.dtype),
            pltpu.VMEM((n_order, k_rows), jnp.bfloat16),
            pltpu.VMEM((n_order, cells), jnp.bfloat16),
            pltpu.SemaphoreType.DMA((4,)),
            pltpu.SemaphoreType.DMA((1,)),
        ],
        compiler_params=pltpu.CompilerParams(vmem_limit_bytes=24 * MIB),
        name="grid_rows",
    )(piece, rows, place, code, low, pltpu.with_memory_space_constraint(kernels, pltpu.HBM))


def strip_kernel(main_ref, out_ref):
    n_out, per, cells = main_ref.shape
    half = cells // 2
    low = main_ref[:, :, :128].reshape(n_out * per, 128).astype(jnp.float32)
    high = main_ref[:, :, half : half + 128].reshape(n_out * per, 128).astype(jnp.float32)
    lane = lax.broadcasted_iota(jnp.int32, low.shape, 1)
    strip = jnp.where(lane < STRIP, low, pltpu.roll(high, STRIP, 1)).astype(jnp.bfloat16)
    out_ref[...] = strip.reshape(out_ref.shape)


def strips_of(main):
    n_out, per, _ = main.shape
    return pl.pallas_call(
        strip_kernel,
        out_shape=jax.ShapeDtypeStruct((n_out, per, 2 * STRIP), jnp.bfloat16),
        in_specs=[vmem()],
        out_specs=vmem(),
        compiler_params=pltpu.CompilerParams(vmem_limit_bytes=8 * MIB),
        name="strips",
    )(main)


def placing(n_out, t_dev):
    n_rows = n_out * t_dev
    to = iota((n_rows, n_rows), 0)
    return (iota((n_rows, n_rows), 1) == (to % n_out) * t_dev + to // n_out).astype(jnp.float32)


def place_kernel(main_ref, out_hbm, rest_ref, done_ref, sem):
    n_out, per, cells = main_ref.shape
    t_dev = per // 2
    run = cells // 4
    place = placing(n_out, t_dev).astype(jnp.bfloat16)
    copies = []
    for slot in range(2):
        main = main_ref[:, slot * t_dev : (slot + 1) * t_dev, :].reshape(n_out * t_dev, cells)
        main = jnp.dot(place, main, preferred_element_type=jnp.float32)
        for i in range(2):
            at = slice(2 * i * run, (2 * i + 1) * run)
            done_ref[i, :, slot] = main[:, at].reshape(t_dev, n_out, run)
            rest_ref[i, :, slot] = main[:, at.stop : at.stop + run].reshape(t_dev, n_out, run)
    for i in range(2):
        copies.append(pltpu.make_async_copy(done_ref.at[i], out_hbm.at[:, :, :, pl.ds(2 * i * run, run)], sem.at[i]))
        copies[-1].start()
    for copy in copies:
        copy.wait()


def place_main(main):
    n_out, per, cells = main.shape
    part = (2, per // 2, 2, n_out, cells // 4)
    return pl.pallas_call(
        place_kernel,
        out_shape=[
            pltpu.HBM((per // 2, 2, n_out, cells), jnp.float32),
            jax.ShapeDtypeStruct(part, jnp.float32),
        ],
        in_specs=[vmem()],
        out_specs=[pl.BlockSpec(memory_space=pltpu.HBM), vmem()],
        scratch_shapes=[pltpu.VMEM(part, jnp.float32), pltpu.SemaphoreType.DMA((2,))],
        compiler_params=pltpu.CompilerParams(vmem_limit_bytes=8 * MIB),
        cost_estimate=pl.CostEstimate(flops=2 * n_out * per * n_out * per // 2 * cells, transcendentals=0, bytes_accessed=3 * MIB // 2),
        name="place",
    )(main)


def join_kernel(nb_vmem, placed_hbm, rest_ref, *refs):
    strips, (out_hbm, nb_ref, strip_ref, done_ref, sem, nb_sem) = refs[:-6], refs[-6:]
    nb_copy = pltpu.make_async_copy(nb_vmem, nb_ref, nb_sem.at[0])
    nb_copy.start()
    _, t_dev, _, n_out, run = rest_ref.shape
    n_rows = n_out * t_dev
    for i, ref in enumerate(strips):
        strip_ref[i] = ref[...].reshape(strip_ref.shape[1:])
    upper = iota((n_rows, 2 * STRIP), 1) >= STRIP
    quarter = (0.25 * placing(n_out, t_dev)).astype(jnp.bfloat16)
    n_nb = nb_ref.shape[1] // 2
    nb_copy.wait()
    copies = []
    for slot in range(2):
        blend = jnp.zeros((n_rows, 2 * STRIP), jnp.float32)
        for k in range(n_nb):
            strip = strip_ref[nb_ref[slot, k], :, nb_ref[slot, n_nb + k]].reshape(n_rows, 2 * STRIP)
            blend += jnp.dot(quarter, strip, preferred_element_type=jnp.float32)
        for i, part in enumerate((pltpu.roll(blend, STRIP, 1), blend)):
            part = jnp.where(upper, part, 0.0).reshape(t_dev, n_out, run)
            done_ref[i, :, slot] = rest_ref[i, :, slot] + part
            target = out_hbm.at[:, slot, :, pl.ds((2 * i + 1) * run, run)]
            copies.append(pltpu.make_async_copy(done_ref.at[i, :, slot], target, sem.at[slot, i]))
            copies[-1].start()
    for copy in copies:
        copy.wait()


def join(sources, placed, rest, strips):
    _, t_dev, _, n_out, run = rest.shape
    assert run == 2 * STRIP
    return pl.pallas_call(
        join_kernel,
        out_shape=pltpu.HBM(placed.shape, placed.dtype),
        in_specs=[vmem(), pl.BlockSpec(memory_space=pltpu.HBM)] + [vmem()] * (1 + len(strips)),
        out_specs=pl.BlockSpec(memory_space=pltpu.HBM),
        scratch_shapes=[
            pltpu.SMEM(sources.shape, jnp.int32),
            pltpu.VMEM((len(strips), n_out, 2, t_dev, 2 * STRIP), jnp.bfloat16),
            pltpu.VMEM(rest.shape, jnp.float32),
            pltpu.SemaphoreType.DMA((2, 2)),
            pltpu.SemaphoreType.DMA((1,)),
        ],
        input_output_aliases={1: 0},
        compiler_params=pltpu.CompilerParams(vmem_limit_bytes=16 * MIB),
        name="join",
    )(sources, placed, rest, *strips)


def exchange(x, axis):
    return lax.all_to_all(x, axis, split_axis=0, concat_axis=0, tiled=True)


def local(visibilities, kernels, delays, tile_of, plane_of, counts, neighbours):
    n_facet = lax.axis_size("facet")
    n_chan = lax.axis_size("chan")
    facet_index = lax.axis_index("facet")
    halves, facets, blocks, _, bv = visibilities.shape
    fac_dev = facets // n_facet
    n_tiles = 16 * n_chan
    t_dev = n_tiles // n_chan
    n_rows = fac_dev * blocks
    per = n_rows // n_chan

    vis = visibilities.reshape(halves, n_facet * n_chan, per, bv)
    vis, delay, place, code, piece = send_order(
        counts, plane_of, tile_of, delays.reshape(n_chan, per, bv), vis, kernels.shape[0], t_dev
    )
    vis = exchange(vis, ("facet", "chan"))

    rows, low = average(delay, vis, kernels)
    rows = exchange(rows, "chan")
    main = exchange(grid_rows(piece, rows, place, code, low, kernels, fac_dev * n_tiles), "chan")

    own = strips_of(main)
    chips = n_facet // 2
    along = lambda x, dz: lax.ppermute(x, "facet", [(f, (f + 2 * dz) % n_facet) for f in range(n_facet)])
    across = lambda x: lax.ppermute(x, "facet", [(f, f ^ 1) for f in range(n_facet)])
    arrived = {dz: along(own, dz) for dz in range(1, chips - 1)}
    placed, rest = place_main(main)
    own, rest = lax.optimization_barrier((own, rest))
    arrived[chips - 1] = along(own, chips - 1)
    strips = [own] + [arrived[dz] for dz in range(1, chips)]
    strips += [across(s) for s in strips]
    mine = lax.dynamic_slice_in_dim(neighbours, facet_index * fac_dev, fac_dev, 0)
    group = mine // fac_dev
    source = (facet_index // 2 - group // 2) % chips + chips * ((group + facet_index) % 2)
    sources = jnp.concatenate([source, mine % fac_dev], axis=1).astype(jnp.int32)
    return join(sources, placed, rest, strips)


def solution(mesh):
    return jax.shard_map(
        local,
        mesh=mesh,
        in_specs=(
            P(None, None, None, ("facet", "chan"), None),
            P(),
            P("facet", None, None),
            P("facet", None),
            P("facet", None),
            P("facet"),
            P(),
        ),
        out_specs=P("chan", "facet", None, None),
        check_vma=False,
    )
```

```python
import functools
import math

import jax
import jax.numpy as jnp
from jax import lax
from jax.experimental import pallas as pl
from jax.experimental.pallas import tpu as pltpu
from jax.sharding import PartitionSpec as P

AVG = 8
TS = 16
EDGE = 4
STRIP = EDGE * TS
GROUP = 16
PIECE = 64
STRETCH = 8
MIB = 1024 * 1024

SIN = (-1.0 / 6, 1.0 / 120, -1.0 / 5040, 1.0 / 362880, -1.0 / 39916800)
COS = (-1.0 / 2, 1.0 / 24, -1.0 / 720, 1.0 / 40320, -1.0 / 3628800, 1.0 / 479001600)


def series(turns):
    x = (2.0 * math.pi) * turns
    y = x * x
    s = jnp.full_like(x, SIN[-1])
    for k in SIN[-2::-1]:
        s = s * y + k
    c = jnp.full_like(x, COS[-1])
    for k in COS[-2::-1]:
        c = c * y + k
    return c * y + 1.0, (s * y + 1.0) * x


def turn_by(turns):
    half = jnp.round(2.0 * turns)
    c, s = series(turns - 0.5 * half)
    odd = (half - 2.0 * jnp.floor(0.5 * half)) > 0.5
    sign = jnp.where(odd, -1.0, 1.0)
    return c * sign, s * sign


def times(a, b):
    return a[0] * b[0] - a[1] * b[1], a[0] * b[1] + a[1] * b[0]


def vmem():
    return pl.BlockSpec(memory_space=pltpu.VMEM)


def to_bf16(mask):
    return mask.astype(jnp.float32).astype(jnp.bfloat16)


def iota(shape, dim):
    return lax.broadcasted_iota(jnp.int32, shape, dim)


def fill_tables(n_planes, t_dev, count_ref, plane_ref, tile_ref, place_ref, code_ref, piece_ref):
    f32 = jnp.float32
    slots, blocks = plane_ref.shape
    n_rows = slots * blocks
    planes, tiles = [], []
    for slot in range(slots):
        alive = iota((1, blocks), 1) < count_ref[slot]
        planes.append(jnp.where(alive, plane_ref[slot : slot + 1, :], -1))
        tiles.append(tile_ref[slot : slot + 1, :])
    plane = jnp.concatenate(planes, axis=1)
    tile = jnp.concatenate(tiles, axis=1)
    mine = plane == iota((n_planes, n_rows), 0)
    before = to_bf16(iota((n_rows, n_rows), 0) < iota((n_rows, n_rows), 1))
    rank = jnp.dot(to_bf16(mine), before, preferred_element_type=f32)
    count = jnp.sum(mine.astype(f32), axis=1, keepdims=True)
    groups = jnp.floor((count + (GROUP - 1)) * (1.0 / GROUP))
    pieces = jnp.floor((groups + (PIECE // GROUP - 1)) * (GROUP / PIECE))
    earlier = to_bf16(iota((n_planes, n_planes), 1) < iota((n_planes, n_planes), 0))
    both = jnp.concatenate(
        [jnp.broadcast_to(groups, (n_planes, 128)), jnp.broadcast_to(pieces, (n_planes, 128))], axis=1
    )
    both = jnp.dot(earlier, both.astype(jnp.bfloat16), preferred_element_type=f32)
    first_group = both[:, 0:1]
    first_piece = both[:, 128:129]
    place = jnp.sum(jnp.where(mine, rank + GROUP * first_group, 0.0), axis=0, keepdims=True)
    live = jnp.sum(mine.astype(f32), axis=0, keepdims=True)
    place = jnp.where(live > 0.5, place, -1.0).astype(jnp.int32)
    place_ref[...] = place
    n_used = code_ref.shape[1]
    order = to_bf16(iota((n_used, n_rows), 0) == place)

    row = iota((8, n_rows), 0)
    slot = (iota((8, n_rows), 1) >= n_rows // 2).astype(f32)
    values = jnp.where(row == 0, tile.astype(f32) + 1.0, jnp.where(row == 1, slot, 0.0))
    ordered = lax.dot_general(
        values.astype(jnp.bfloat16), order, (((1,), (1,)), ((), ())), preferred_element_type=f32
    )
    tile = ordered[0:1].astype(jnp.int32) - 1
    slot = ordered[1:2].astype(jnp.int32)
    code = (tile // t_dev) * (2 * t_dev) + slot * t_dev + tile % t_dev
    code_ref[...] = jnp.where(tile < 0, -1, code)

    lower = jnp.sum(jnp.where(iota((n_planes, 1), 0) < n_planes // 2, pieces, 0.0))
    upper = jnp.sum(pieces) - lower
    lane = iota((n_planes, 128), 1)
    at = (lane % 64).astype(f32)
    is_upper = lane >= 64
    which = jnp.minimum(at, jnp.where(is_upper, upper, lower) - 1.0) + jnp.where(is_upper, lower, 0.0)
    taken = (which >= first_piece) & (which < first_piece + pieces)
    group = first_group + (PIECE // GROUP) * (which - first_piece)
    group = jnp.sum(jnp.where(taken, group, 0.0), axis=0, keepdims=True)
    owner = jnp.sum(jnp.where(taken, iota((n_planes, 128), 0).astype(f32), 0.0), axis=0, keepdims=True)
    owner = owner - jnp.where(iota((1, 128), 1) >= 64, float(n_planes // 2), 0.0)
    row = iota((8, 128), 0)
    totals = jnp.where(iota((8, 128), 1) >= 64, upper, lower)
    value = jnp.where(row == 0, group, jnp.where(row == 1, jnp.maximum(owner, 0.0), jnp.where(row == 2, totals, 0.0)))
    piece_ref[...] = value.astype(jnp.int32)


def sizes(n_rows, n_planes):
    used = n_rows + n_planes * (GROUP - 1)
    n_order = -(-(used - GROUP + PIECE) // 32) * 32
    n_used = -(-used // 256) * 256
    assert n_used <= n_order
    return n_order, n_used


def send_kernel(n_planes, t_dev, *refs):
    (count_hbm, plane_hbm, tile_hbm, delay_hbm, vis_hbm), refs = refs[:5], refs[5:]
    (out_ref, delay_ref, *tables), (count_ref, plane_ref, tile_ref, small_sem, sem) = refs[:-5], refs[-5:]
    smalls = [
        pltpu.make_async_copy(count_hbm, count_ref, small_sem.at[0]),
        pltpu.make_async_copy(plane_hbm, plane_ref, small_sem.at[1]),
        pltpu.make_async_copy(tile_hbm, tile_ref, small_sem.at[2]),
        pltpu.make_async_copy(delay_hbm.at[lax.axis_index("chan")], delay_ref, small_sem.at[3]),
    ]
    for copy in smalls:
        copy.start()
    for copy in smalls:
        copy.wait()
    halves, dests = vis_hbm.shape[:2]
    n = sem.shape[1]
    copies = []
    for i in range(n):
        at = pl.ds(i * (dests // n), dests // n)
        for h in range(halves):
            copies.append(pltpu.make_async_copy(vis_hbm.at[h, at], out_ref.at[at, h], sem.at[h, i]))
            copies[-1].start()
    fill_tables(n_planes, t_dev, count_ref, plane_ref, tile_ref, *tables)
    for copy in copies:
        copy.wait()


def send_order(counts, planes, tiles, delays, vis, n_planes, t_dev):
    halves, dests, rows, bv = vis.shape
    n_rows = planes.shape[0] * planes.shape[1]
    n_order, n_used = sizes(n_rows, n_planes)
    args = [pltpu.with_memory_space_constraint(x, pltpu.HBM) for x in (counts, planes, tiles, delays, vis)]
    return pl.pallas_call(
        functools.partial(send_kernel, n_planes, t_dev),
        out_shape=[
            jax.ShapeDtypeStruct((dests, halves, rows, bv), vis.dtype),
            jax.ShapeDtypeStruct(delays.shape[1:], delays.dtype),
            jax.ShapeDtypeStruct((1, n_rows), jnp.int32),
            jax.ShapeDtypeStruct((1, n_used), jnp.int32),
            jax.ShapeDtypeStruct((8, 128), jnp.int32),
        ],
        in_specs=[pl.BlockSpec(memory_space=pltpu.HBM)] * len(args),
        out_specs=[vmem()] * 5,
        scratch_shapes=[
            pltpu.SMEM(counts.shape, jnp.int32),
            pltpu.VMEM(planes.shape, jnp.int32),
            pltpu.VMEM(tiles.shape, jnp.int32),
            pltpu.SemaphoreType.DMA((4,)),
            pltpu.SemaphoreType.DMA((halves, 8)),
        ],
        compiler_params=pltpu.CompilerParams(vmem_limit_bytes=32 * MIB),
        name="send_order",
    )(*args)


def fill_turns(d, inner_ref, outer_ref):
    small = series(d * (1.0 / 256.0))
    table = [None, small]
    for j in range(2, AVG):
        table.append(times(table[j // 2], table[j - j // 2]))
    for j in range(1, AVG):
        inner_ref[j - 1, 0] = table[j][0]
        inner_ref[j - 1, 1] = table[j][1]
    c, s = turn_by(d)
    turn = (c * (1.0 / AVG), s * (1.0 / AVG))
    step = series(d * (1.0 / 32.0))
    for o in range(outer_ref.shape[0]):
        outer_ref[o, 0] = turn[0]
        outer_ref[o, 1] = turn[1]
        turn = times(turn, step)


def average_kernel(delay_ref, vis_ref, out_ref, inner_ref, outer_ref):
    fill_turns(delay_ref[...], inner_ref, outer_ref)
    n_out, _, rows, _ = out_ref.shape
    for r in range(0, rows, 16):
        at = slice(r, r + 16)
        table = [(inner_ref[j, 0, at], inner_ref[j, 1, at]) for j in range(AVG - 1)]

        def one(o, carry, at=at, table=table):
            c = o * AVG
            re = vis_ref[c, 0, at].astype(jnp.float32)
            im = vis_ref[c, 1, at].astype(jnp.float32)
            for j in range(1, AVG):
                a = vis_ref[c + j, 0, at].astype(jnp.float32)
                b = vis_ref[c + j, 1, at].astype(jnp.float32)
                tc, ts = table[j - 1]
                re += a * tc - b * ts
                im += a * ts + b * tc
            tc = outer_ref[o, 0, at]
            ts = outer_ref[o, 1, at]
            out_ref[o, 0, at] = (re * tc - im * ts).astype(jnp.bfloat16)
            out_ref[o, 1, at] = (re * ts + im * tc).astype(jnp.bfloat16)
            return carry

        lax.fori_loop(0, n_out, one, 0, unroll=4)


def average(delay, vis):
    n_ch, halves, rows, bv = vis.shape
    n_out = n_ch // AVG
    return pl.pallas_call(
        average_kernel,
        out_shape=jax.ShapeDtypeStruct((n_out, halves, rows, bv), jnp.bfloat16),
        in_specs=[vmem()] * 2,
        out_specs=vmem(),
        scratch_shapes=[
            pltpu.VMEM((AVG - 1, 2, rows, bv), jnp.float32),
            pltpu.VMEM((n_out, 2, rows, bv), jnp.float32),
        ],
        compiler_params=pltpu.CompilerParams(vmem_limit_bytes=8 * MIB),
        name="average",
    )(delay, vis)


def grid_kernel(n_pieces, *refs):
    piece_vmem, rows_ref, place_ref, code_ref, k_ref, out_ref, piece_ref, x_ref, c_ref, piece_sem = refs
    piece_copy = pltpu.make_async_copy(piece_vmem, piece_ref, piece_sem.at[0])
    piece_copy.start()
    n_src, _, per, bv = rows_ref.shape
    re = rows_ref[:, 0].reshape(n_src * per, bv)
    im = rows_ref[:, 1].reshape(n_src * per, bv)
    x = jnp.concatenate([re, im], axis=1)
    order = to_bf16(iota((x_ref.shape[0], n_src * per), 0) == place_ref[...])
    x_ref[...] = jnp.dot(order, x, preferred_element_type=jnp.float32).astype(jnp.bfloat16)
    c_ref[...] = jnp.zeros_like(c_ref)
    piece_copy.wait()
    for lane, first in ((0, 0), (64, k_ref.shape[0] // 2)):
        for begin in range(0, n_pieces, STRETCH):

            @pl.when(begin < piece_ref[2, lane])
            def _(begin=begin, lane=lane, first=first):
                for i in range(lane + begin, lane + min(begin + STRETCH, n_pieces)):
                    at = pl.ds(pl.multiple_of(piece_ref[0, i] * GROUP, GROUP), PIECE)
                    product = jnp.dot(x_ref[at, :], k_ref[first + piece_ref[1, i]], preferred_element_type=jnp.float32)
                    c_ref[at, :] = product.astype(jnp.bfloat16)

    n_used = code_ref.shape[1]
    tiles = to_bf16(iota((out_ref.shape[0] * out_ref.shape[1], n_used), 0) == code_ref[...])
    grid = jnp.dot(tiles, c_ref[:n_used, :], preferred_element_type=jnp.float32)
    out_ref[...] = grid.astype(jnp.bfloat16).reshape(out_ref.shape)


def grid_rows(piece, rows, place, code, kernels, n_codes):
    n_planes, k_rows, cells = kernels.shape
    n_rows = place.shape[1]
    n_order, _ = sizes(n_rows, n_planes)
    n_chan = rows.shape[0]
    n_pieces = n_rows // PIECE + n_planes // 2
    assert n_pieces <= 64
    return pl.pallas_call(
        functools.partial(grid_kernel, n_pieces),
        out_shape=jax.ShapeDtypeStruct((n_chan, n_codes // n_chan, cells), jnp.bfloat16),
        in_specs=[vmem()] * 5,
        out_specs=vmem(),
        scratch_shapes=[
            pltpu.SMEM(piece.shape, jnp.int32),
            pltpu.VMEM((n_order, k_rows), jnp.bfloat16),
            pltpu.VMEM((n_order, cells), jnp.bfloat16),
            pltpu.SemaphoreType.DMA((1,)),
        ],
        compiler_params=pltpu.CompilerParams(vmem_limit_bytes=20 * MIB),
        name="grid_rows",
    )(piece, rows, place, code, kernels)


def strip_kernel(main_ref, out_ref):
    n_out, per, cells = main_ref.shape
    half = cells // 2
    low = main_ref[:, :, :128].reshape(n_out * per, 128).astype(jnp.float32)
    high = main_ref[:, :, half : half + 128].reshape(n_out * per, 128).astype(jnp.float32)
    lane = lax.broadcasted_iota(jnp.int32, low.shape, 1)
    strip = jnp.where(lane < STRIP, low, pltpu.roll(high, STRIP, 1)).astype(jnp.bfloat16)
    out_ref[...] = strip.reshape(out_ref.shape)


def strips_of(main):
    n_out, per, _ = main.shape
    return pl.pallas_call(
        strip_kernel,
        out_shape=jax.ShapeDtypeStruct((n_out, per, 2 * STRIP), jnp.bfloat16),
        in_specs=[vmem()],
        out_specs=vmem(),
        compiler_params=pltpu.CompilerParams(vmem_limit_bytes=8 * MIB),
        name="strips",
    )(main)


def placing(n_out, t_dev):
    n_rows = n_out * t_dev
    to = iota((n_rows, n_rows), 0)
    return (iota((n_rows, n_rows), 1) == (to % n_out) * t_dev + to // n_out).astype(jnp.float32)


def place_kernel(main_ref, out_hbm, rest_ref, done_ref, sem):
    n_out, per, cells = main_ref.shape
    t_dev = per // 2
    run = cells // 4
    place = placing(n_out, t_dev).astype(jnp.bfloat16)
    copies = []
    for slot in range(2):
        main = main_ref[:, slot * t_dev : (slot + 1) * t_dev, :].reshape(n_out * t_dev, cells)
        main = jnp.dot(place, main, preferred_element_type=jnp.float32)
        for i in range(2):
            at = slice(2 * i * run, (2 * i + 1) * run)
            done_ref[i, :, slot] = main[:, at].reshape(t_dev, n_out, run)
            rest_ref[i, :, slot] = main[:, at.stop : at.stop + run].reshape(t_dev, n_out, run)
    for i in range(2):
        copies.append(pltpu.make_async_copy(done_ref.at[i], out_hbm.at[:, :, :, pl.ds(2 * i * run, run)], sem.at[i]))
        copies[-1].start()
    for copy in copies:
        copy.wait()


def place_main(main):
    n_out, per, cells = main.shape
    part = (2, per // 2, 2, n_out, cells // 4)
    return pl.pallas_call(
        place_kernel,
        out_shape=[
            pltpu.HBM((per // 2, 2, n_out, cells), jnp.float32),
            jax.ShapeDtypeStruct(part, jnp.float32),
        ],
        in_specs=[vmem()],
        out_specs=[pl.BlockSpec(memory_space=pltpu.HBM), vmem()],
        scratch_shapes=[pltpu.VMEM(part, jnp.float32), pltpu.SemaphoreType.DMA((2,))],
        compiler_params=pltpu.CompilerParams(vmem_limit_bytes=8 * MIB),
        cost_estimate=pl.CostEstimate(flops=2 * n_out * per * n_out * per // 2 * cells, transcendentals=0, bytes_accessed=3 * MIB // 2),
        name="place",
    )(main)


def join_kernel(nb_vmem, placed_hbm, rest_ref, *refs):
    strips, (out_hbm, nb_ref, strip_ref, done_ref, sem, nb_sem) = refs[:-6], refs[-6:]
    nb_copy = pltpu.make_async_copy(nb_vmem, nb_ref, nb_sem.at[0])
    nb_copy.start()
    _, t_dev, _, n_out, run = rest_ref.shape
    n_rows = n_out * t_dev
    for i, ref in enumerate(strips):
        strip_ref[i] = ref[...].reshape(strip_ref.shape[1:])
    upper = iota((n_rows, 2 * STRIP), 1) >= STRIP
    quarter = (0.25 * placing(n_out, t_dev)).astype(jnp.bfloat16)
    n_nb = nb_ref.shape[1] // 2
    nb_copy.wait()
    copies = []
    for slot in range(2):
        blend = jnp.zeros((n_rows, 2 * STRIP), jnp.float32)
        for k in range(n_nb):
            strip = strip_ref[nb_ref[slot, k], :, nb_ref[slot, n_nb + k]].reshape(n_rows, 2 * STRIP)
            blend += jnp.dot(quarter, strip, preferred_element_type=jnp.float32)
        for i, part in enumerate((pltpu.roll(blend, STRIP, 1), blend)):
            part = jnp.where(upper, part, 0.0).reshape(t_dev, n_out, run)
            done_ref[i, :, slot] = rest_ref[i, :, slot] + part
            target = out_hbm.at[:, slot, :, pl.ds((2 * i + 1) * run, run)]
            copies.append(pltpu.make_async_copy(done_ref.at[i, :, slot], target, sem.at[slot, i]))
            copies[-1].start()
    for copy in copies:
        copy.wait()


def join(sources, placed, rest, strips):
    _, t_dev, _, n_out, run = rest.shape
    assert run == 2 * STRIP
    return pl.pallas_call(
        join_kernel,
        out_shape=pltpu.HBM(placed.shape, placed.dtype),
        in_specs=[vmem(), pl.BlockSpec(memory_space=pltpu.HBM)] + [vmem()] * (1 + len(strips)),
        out_specs=pl.BlockSpec(memory_space=pltpu.HBM),
        scratch_shapes=[
            pltpu.SMEM(sources.shape, jnp.int32),
            pltpu.VMEM((len(strips), n_out, 2, t_dev, 2 * STRIP), jnp.bfloat16),
            pltpu.VMEM(rest.shape, jnp.float32),
            pltpu.SemaphoreType.DMA((2, 2)),
            pltpu.SemaphoreType.DMA((1,)),
        ],
        input_output_aliases={1: 0},
        compiler_params=pltpu.CompilerParams(vmem_limit_bytes=16 * MIB),
        name="join",
    )(sources, placed, rest, *strips)


def exchange(x, axis):
    return lax.all_to_all(x, axis, split_axis=0, concat_axis=0, tiled=True)


def local(visibilities, kernels, delays, tile_of, plane_of, counts, neighbours):
    n_facet = lax.axis_size("facet")
    n_chan = lax.axis_size("chan")
    facet_index = lax.axis_index("facet")
    halves, facets, blocks, _, bv = visibilities.shape
    fac_dev = facets // n_facet
    n_tiles = 16 * n_chan
    t_dev = n_tiles // n_chan
    n_rows = fac_dev * blocks
    per = n_rows // n_chan

    vis = visibilities.reshape(halves, n_facet * n_chan, per, bv)
    vis, delay, place, code, piece = send_order(
        counts, plane_of, tile_of, delays.reshape(n_chan, per, bv), vis, kernels.shape[0], t_dev
    )
    vis = exchange(vis, ("facet", "chan"))

    rows = exchange(average(delay, vis), "chan")
    main = exchange(grid_rows(piece, rows, place, code, kernels, fac_dev * n_tiles), "chan")

    own = strips_of(main)
    chips = n_facet // 2
    along = lambda x, dz: lax.ppermute(x, "facet", [(f, (f + 2 * dz) % n_facet) for f in range(n_facet)])
    across = lambda x: lax.ppermute(x, "facet", [(f, f ^ 1) for f in range(n_facet)])
    arrived = {dz: along(own, dz) for dz in range(1, chips - 1)}
    placed, rest = place_main(main)
    own, rest = lax.optimization_barrier((own, rest))
    arrived[chips - 1] = along(own, chips - 1)
    strips = [own] + [arrived[dz] for dz in range(1, chips)]
    strips += [across(s) for s in strips]
    mine = lax.dynamic_slice_in_dim(neighbours, facet_index * fac_dev, fac_dev, 0)
    group = mine // fac_dev
    source = (facet_index // 2 - group // 2) % chips + chips * ((group + facet_index) % 2)
    sources = jnp.concatenate([source, mine % fac_dev], axis=1).astype(jnp.int32)
    return join(sources, placed, rest, strips)


def solution(mesh):
    return jax.shard_map(
        local,
        mesh=mesh,
        in_specs=(
            P(None, None, None, ("facet", "chan"), None),
            P(),
            P("facet", None, None),
            P("facet", None),
            P("facet", None),
            P("facet"),
            P(),
        ),
        out_specs=P("chan", "facet", None, None),
        check_vma=False,
    )
```

```python
import functools
import math

import jax
import jax.numpy as jnp
from jax import lax
from jax.experimental import pallas as pl
from jax.experimental.pallas import tpu as pltpu
from jax.sharding import PartitionSpec as P

AVG = 8
TS = 16
EDGE = 4
STRIP = EDGE * TS
GROUP = 16
PIECE = 64
STRETCH = 8
MIB = 1024 * 1024

SIN = (-1.0 / 6, 1.0 / 120, -1.0 / 5040, 1.0 / 362880, -1.0 / 39916800)
COS = (-1.0 / 2, 1.0 / 24, -1.0 / 720, 1.0 / 40320, -1.0 / 3628800, 1.0 / 479001600)


def series(turns):
    x = (2.0 * math.pi) * turns
    y = x * x
    s = jnp.full_like(x, SIN[-1])
    for k in SIN[-2::-1]:
        s = s * y + k
    c = jnp.full_like(x, COS[-1])
    for k in COS[-2::-1]:
        c = c * y + k
    return c * y + 1.0, (s * y + 1.0) * x


def turn_by(turns):
    half = jnp.round(2.0 * turns)
    c, s = series(turns - 0.5 * half)
    odd = (half - 2.0 * jnp.floor(0.5 * half)) > 0.5
    sign = jnp.where(odd, -1.0, 1.0)
    return c * sign, s * sign


def times(a, b):
    return a[0] * b[0] - a[1] * b[1], a[0] * b[1] + a[1] * b[0]


def vmem():
    return pl.BlockSpec(memory_space=pltpu.VMEM)


def to_bf16(mask):
    return mask.astype(jnp.float32).astype(jnp.bfloat16)


def iota(shape, dim):
    return lax.broadcasted_iota(jnp.int32, shape, dim)


def fill_tables(n_planes, t_dev, count_ref, plane_ref, tile_ref, place_ref, code_ref, piece_ref):
    f32 = jnp.float32
    slots, blocks = plane_ref.shape
    n_rows = slots * blocks
    planes, tiles = [], []
    for slot in range(slots):
        alive = iota((1, blocks), 1) < count_ref[slot]
        planes.append(jnp.where(alive, plane_ref[slot : slot + 1, :], -1))
        tiles.append(tile_ref[slot : slot + 1, :])
    plane = jnp.concatenate(planes, axis=1)
    tile = jnp.concatenate(tiles, axis=1)
    mine = plane == iota((n_planes, n_rows), 0)
    before = to_bf16(iota((n_rows, n_rows), 0) < iota((n_rows, n_rows), 1))
    rank = jnp.dot(to_bf16(mine), before, preferred_element_type=f32)
    count = jnp.sum(mine.astype(f32), axis=1, keepdims=True)
    groups = jnp.floor((count + (GROUP - 1)) * (1.0 / GROUP))
    pieces = jnp.floor((groups + (PIECE // GROUP - 1)) * (GROUP / PIECE))
    earlier = to_bf16(iota((n_planes, n_planes), 1) < iota((n_planes, n_planes), 0))
    both = jnp.concatenate(
        [jnp.broadcast_to(groups, (n_planes, 128)), jnp.broadcast_to(pieces, (n_planes, 128))], axis=1
    )
    both = jnp.dot(earlier, both.astype(jnp.bfloat16), preferred_element_type=f32)
    first_group = both[:, 0:1]
    first_piece = both[:, 128:129]
    place = jnp.sum(jnp.where(mine, rank + GROUP * first_group, 0.0), axis=0, keepdims=True)
    live = jnp.sum(mine.astype(f32), axis=0, keepdims=True)
    place = jnp.where(live > 0.5, place, -1.0).astype(jnp.int32)
    place_ref[...] = place
    n_used = code_ref.shape[1]
    order = to_bf16(iota((n_used, n_rows), 0) == place)

    row = iota((8, n_rows), 0)
    slot = (iota((8, n_rows), 1) >= n_rows // 2).astype(f32)
    values = jnp.where(row == 0, tile.astype(f32) + 1.0, jnp.where(row == 1, slot, 0.0))
    ordered = lax.dot_general(
        values.astype(jnp.bfloat16), order, (((1,), (1,)), ((), ())), preferred_element_type=f32
    )
    tile = ordered[0:1].astype(jnp.int32) - 1
    slot = ordered[1:2].astype(jnp.int32)
    code = (tile // t_dev) * (2 * t_dev) + slot * t_dev + tile % t_dev
    code_ref[...] = jnp.where(tile < 0, -1, code)

    lower = jnp.sum(jnp.where(iota((n_planes, 1), 0) < n_planes // 2, pieces, 0.0))
    upper = jnp.sum(pieces) - lower
    lane = iota((n_planes, 128), 1)
    at = (lane % 64).astype(f32)
    is_upper = lane >= 64
    which = jnp.minimum(at, jnp.where(is_upper, upper, lower) - 1.0) + jnp.where(is_upper, lower, 0.0)
    taken = (which >= first_piece) & (which < first_piece + pieces)
    group = first_group + (PIECE // GROUP) * (which - first_piece)
    group = jnp.sum(jnp.where(taken, group, 0.0), axis=0, keepdims=True)
    owner = jnp.sum(jnp.where(taken, iota((n_planes, 128), 0).astype(f32), 0.0), axis=0, keepdims=True)
    owner = owner - jnp.where(iota((1, 128), 1) >= 64, float(n_planes // 2), 0.0)
    row = iota((8, 128), 0)
    totals = jnp.where(iota((8, 128), 1) >= 64, upper, lower)
    value = jnp.where(row == 0, group, jnp.where(row == 1, jnp.maximum(owner, 0.0), jnp.where(row == 2, totals, 0.0)))
    piece_ref[...] = value.astype(jnp.int32)


def sizes(n_rows, n_planes):
    used = n_rows + n_planes * (GROUP - 1)
    n_order = -(-(used - GROUP + PIECE) // 32) * 32
    n_used = -(-used // 256) * 256
    assert n_used <= n_order
    return n_order, n_used


def send_kernel(n_planes, t_dev, *refs):
    (count_hbm, plane_hbm, tile_hbm, delay_hbm, vis_hbm), refs = refs[:5], refs[5:]
    (out_ref, delay_ref, *tables), (count_ref, plane_ref, tile_ref, small_sem, sem) = refs[:-5], refs[-5:]
    smalls = [
        pltpu.make_async_copy(count_hbm, count_ref, small_sem.at[0]),
        pltpu.make_async_copy(plane_hbm, plane_ref, small_sem.at[1]),
        pltpu.make_async_copy(tile_hbm, tile_ref, small_sem.at[2]),
        pltpu.make_async_copy(delay_hbm.at[lax.axis_index("chan")], delay_ref, small_sem.at[3]),
    ]
    for copy in smalls:
        copy.start()
    for copy in smalls:
        copy.wait()
    halves, dests = vis_hbm.shape[:2]
    n = sem.shape[1]
    copies = []
    for i in range(n):
        at = pl.ds(i * (dests // n), dests // n)
        for h in range(halves):
            copies.append(pltpu.make_async_copy(vis_hbm.at[h, at], out_ref.at[at, h], sem.at[h, i]))
            copies[-1].start()

    @pl.when(count_ref[0] >= 0)
    def _():
        fill_tables(n_planes, t_dev, count_ref, plane_ref, tile_ref, *tables)

    for copy in copies:
        copy.wait()


def send_order(counts, planes, tiles, delays, vis, n_planes, t_dev):
    halves, dests, rows, bv = vis.shape
    n_rows = planes.shape[0] * planes.shape[1]
    n_order, n_used = sizes(n_rows, n_planes)
    args = [pltpu.with_memory_space_constraint(x, pltpu.HBM) for x in (counts, planes, tiles, delays, vis)]
    return pl.pallas_call(
        functools.partial(send_kernel, n_planes, t_dev),
        out_shape=[
            jax.ShapeDtypeStruct((dests, halves, rows, bv), vis.dtype),
            jax.ShapeDtypeStruct(delays.shape[1:], delays.dtype),
            jax.ShapeDtypeStruct((1, n_rows), jnp.int32),
            jax.ShapeDtypeStruct((1, n_used), jnp.int32),
            jax.ShapeDtypeStruct((8, 128), jnp.int32),
        ],
        in_specs=[pl.BlockSpec(memory_space=pltpu.HBM)] * len(args),
        out_specs=[vmem()] * 5,
        scratch_shapes=[
            pltpu.SMEM(counts.shape, jnp.int32),
            pltpu.VMEM(planes.shape, jnp.int32),
            pltpu.VMEM(tiles.shape, jnp.int32),
            pltpu.SemaphoreType.DMA((4,)),
            pltpu.SemaphoreType.DMA((halves, 2)),
        ],
        compiler_params=pltpu.CompilerParams(vmem_limit_bytes=32 * MIB),
        name="send_order",
    )(*args)


def fill_turns(d, inner_ref, outer_ref):
    small = series(d * (1.0 / 256.0))
    table = [None, small]
    for j in range(2, AVG):
        table.append(times(table[j // 2], table[j - j // 2]))
    for j in range(1, AVG):
        inner_ref[j - 1, 0] = table[j][0]
        inner_ref[j - 1, 1] = table[j][1]
    c, s = turn_by(d)
    turn = (c * (1.0 / AVG), s * (1.0 / AVG))
    step = series(d * (1.0 / 32.0))
    for o in range(outer_ref.shape[0]):
        outer_ref[o, 0] = turn[0]
        outer_ref[o, 1] = turn[1]
        turn = times(turn, step)


def average_kernel(delay_ref, vis_ref, out_ref, inner_ref, outer_ref):
    fill_turns(delay_ref[...], inner_ref, outer_ref)
    n_out, _, rows, _ = out_ref.shape
    for r in range(0, rows, 16):
        at = slice(r, r + 16)
        table = [(inner_ref[j, 0, at], inner_ref[j, 1, at]) for j in range(AVG - 1)]

        def one(o, carry, at=at, table=table):
            c = o * AVG
            re = vis_ref[c, 0, at].astype(jnp.float32)
            im = vis_ref[c, 1, at].astype(jnp.float32)
            for j in range(1, AVG):
                a = vis_ref[c + j, 0, at].astype(jnp.float32)
                b = vis_ref[c + j, 1, at].astype(jnp.float32)
                tc, ts = table[j - 1]
                re += a * tc - b * ts
                im += a * ts + b * tc
            tc = outer_ref[o, 0, at]
            ts = outer_ref[o, 1, at]
            out_ref[o, 0, at] = (re * tc - im * ts).astype(jnp.bfloat16)
            out_ref[o, 1, at] = (re * ts + im * tc).astype(jnp.bfloat16)
            return carry

        lax.fori_loop(0, n_out, one, 0, unroll=4)


def average(delay, vis):
    n_ch, halves, rows, bv = vis.shape
    n_out = n_ch // AVG
    return pl.pallas_call(
        average_kernel,
        out_shape=jax.ShapeDtypeStruct((n_out, halves, rows, bv), jnp.bfloat16),
        in_specs=[vmem()] * 2,
        out_specs=vmem(),
        scratch_shapes=[
            pltpu.VMEM((AVG - 1, 2, rows, bv), jnp.float32),
            pltpu.VMEM((n_out, 2, rows, bv), jnp.float32),
        ],
        compiler_params=pltpu.CompilerParams(vmem_limit_bytes=8 * MIB),
        cost_estimate=pl.CostEstimate(flops=300 * 9 * n_ch * halves * rows * bv, transcendentals=0, bytes_accessed=300 * 5 * MIB),
        name="average",
    )(delay, vis)


def grid_kernel(n_pieces, *refs):
    piece_vmem, rows_ref, place_ref, code_ref, k_ref, out_ref, piece_ref, x_ref, c_ref, piece_sem = refs
    piece_copy = pltpu.make_async_copy(piece_vmem, piece_ref, piece_sem.at[0])
    piece_copy.start()
    n_src, _, per, bv = rows_ref.shape
    re = rows_ref[:, 0].reshape(n_src * per, bv)
    im = rows_ref[:, 1].reshape(n_src * per, bv)
    x = jnp.concatenate([re, im], axis=1)
    order = to_bf16(iota((x_ref.shape[0], n_src * per), 0) == place_ref[...])
    x_ref[...] = jnp.dot(order, x, preferred_element_type=jnp.float32).astype(jnp.bfloat16)
    c_ref[...] = jnp.zeros_like(c_ref)
    piece_copy.wait()
    for lane, first in ((0, 0), (64, k_ref.shape[0] // 2)):
        for begin in range(0, n_pieces, STRETCH):

            @pl.when(begin < piece_ref[2, lane])
            def _(begin=begin, lane=lane, first=first):
                for i in range(lane + begin, lane + min(begin + STRETCH, n_pieces)):
                    at = pl.ds(pl.multiple_of(piece_ref[0, i] * GROUP, GROUP), PIECE)
                    product = jnp.dot(x_ref[at, :], k_ref[first + piece_ref[1, i]], preferred_element_type=jnp.float32)
                    c_ref[at, :] = product.astype(jnp.bfloat16)

    n_used = code_ref.shape[1]
    tiles = to_bf16(iota((out_ref.shape[0] * out_ref.shape[1], n_used), 0) == code_ref[...])
    grid = jnp.dot(tiles, c_ref[:n_used, :], preferred_element_type=jnp.float32)
    out_ref[...] = grid.astype(jnp.bfloat16).reshape(out_ref.shape)


def grid_rows(piece, rows, place, code, kernels, n_codes):
    n_planes, k_rows, cells = kernels.shape
    n_rows = place.shape[1]
    n_order, _ = sizes(n_rows, n_planes)
    n_chan = rows.shape[0]
    n_pieces = n_rows // PIECE + n_planes // 2
    assert n_pieces <= 64
    return pl.pallas_call(
        functools.partial(grid_kernel, n_pieces),
        out_shape=jax.ShapeDtypeStruct((n_chan, n_codes // n_chan, cells), jnp.bfloat16),
        in_specs=[vmem()] * 5,
        out_specs=vmem(),
        scratch_shapes=[
            pltpu.SMEM(piece.shape, jnp.int32),
            pltpu.VMEM((n_order, k_rows), jnp.bfloat16),
            pltpu.VMEM((n_order, cells), jnp.bfloat16),
            pltpu.SemaphoreType.DMA((1,)),
        ],
        compiler_params=pltpu.CompilerParams(vmem_limit_bytes=20 * MIB),
        name="grid_rows",
    )(piece, rows, place, code, kernels)


def strip_kernel(main_ref, out_ref):
    n_out, per, cells = main_ref.shape
    half = cells // 2
    low = main_ref[:, :, :128].reshape(n_out * per, 128).astype(jnp.float32)
    high = main_ref[:, :, half : half + 128].reshape(n_out * per, 128).astype(jnp.float32)
    lane = lax.broadcasted_iota(jnp.int32, low.shape, 1)
    strip = jnp.where(lane < STRIP, low, pltpu.roll(high, STRIP, 1)).astype(jnp.bfloat16)
    out_ref[...] = strip.reshape(out_ref.shape)


def strips_of(main):
    n_out, per, _ = main.shape
    return pl.pallas_call(
        strip_kernel,
        out_shape=jax.ShapeDtypeStruct((n_out, per, 2 * STRIP), jnp.bfloat16),
        in_specs=[vmem()],
        out_specs=vmem(),
        compiler_params=pltpu.CompilerParams(vmem_limit_bytes=8 * MIB),
        name="strips",
    )(main)


def placing(n_out, t_dev):
    n_rows = n_out * t_dev
    to = iota((n_rows, n_rows), 0)
    return (iota((n_rows, n_rows), 1) == (to % n_out) * t_dev + to // n_out).astype(jnp.float32)


def place_kernel(main_ref, out_hbm, rest_ref, done_ref, sem):
    n_out, per, cells = main_ref.shape
    t_dev = per // 2
    run = cells // 4
    place = placing(n_out, t_dev).astype(jnp.bfloat16)
    copies = []
    for slot in range(2):
        main = main_ref[:, slot * t_dev : (slot + 1) * t_dev, :].reshape(n_out * t_dev, cells)
        main = jnp.dot(place, main, preferred_element_type=jnp.float32)
        for i in range(2):
            at = slice(2 * i * run, (2 * i + 1) * run)
            done_ref[i, :, slot] = main[:, at].reshape(t_dev, n_out, run)
            rest_ref[i, :, slot] = main[:, at.stop : at.stop + run].reshape(t_dev, n_out, run)
    for i in range(2):
        copies.append(pltpu.make_async_copy(done_ref.at[i], out_hbm.at[:, :, :, pl.ds(2 * i * run, run)], sem.at[i]))
        copies[-1].start()
    for copy in copies:
        copy.wait()


def place_main(main):
    n_out, per, cells = main.shape
    part = (2, per // 2, 2, n_out, cells // 4)
    return pl.pallas_call(
        place_kernel,
        out_shape=[
            pltpu.HBM((per // 2, 2, n_out, cells), jnp.float32),
            jax.ShapeDtypeStruct(part, jnp.float32),
        ],
        in_specs=[vmem()],
        out_specs=[pl.BlockSpec(memory_space=pltpu.HBM), vmem()],
        scratch_shapes=[pltpu.VMEM(part, jnp.float32), pltpu.SemaphoreType.DMA((2,))],
        compiler_params=pltpu.CompilerParams(vmem_limit_bytes=8 * MIB),
        cost_estimate=pl.CostEstimate(flops=2 * n_out * per * n_out * per // 2 * cells, transcendentals=0, bytes_accessed=3 * MIB // 2),
        name="place",
    )(main)


def join_kernel(nb_vmem, placed_hbm, rest_ref, *refs):
    strips, (out_hbm, nb_ref, strip_ref, done_ref, sem, nb_sem) = refs[:-6], refs[-6:]
    nb_copy = pltpu.make_async_copy(nb_vmem, nb_ref, nb_sem.at[0])
    nb_copy.start()
    _, t_dev, _, n_out, run = rest_ref.shape
    n_rows = n_out * t_dev
    for i, ref in enumerate(strips):
        strip_ref[i] = ref[...].reshape(strip_ref.shape[1:])
    upper = iota((n_rows, 2 * STRIP), 1) >= STRIP
    quarter = (0.25 * placing(n_out, t_dev)).astype(jnp.bfloat16)
    n_nb = nb_ref.shape[1] // 2
    nb_copy.wait()
    copies = []
    for slot in range(2):
        blend = jnp.zeros((n_rows, 2 * STRIP), jnp.float32)
        for k in range(n_nb):
            strip = strip_ref[nb_ref[slot, k], :, nb_ref[slot, n_nb + k]].reshape(n_rows, 2 * STRIP)
            blend += jnp.dot(quarter, strip, preferred_element_type=jnp.float32)
        for i, part in enumerate((pltpu.roll(blend, STRIP, 1), blend)):
            part = jnp.where(upper, part, 0.0).reshape(t_dev, n_out, run)
            done_ref[i, :, slot] = rest_ref[i, :, slot] + part
            target = out_hbm.at[:, slot, :, pl.ds((2 * i + 1) * run, run)]
            copies.append(pltpu.make_async_copy(done_ref.at[i, :, slot], target, sem.at[slot, i]))
            copies[-1].start()
    for copy in copies:
        copy.wait()


def join(sources, placed, rest, strips):
    _, t_dev, _, n_out, run = rest.shape
    assert run == 2 * STRIP
    return pl.pallas_call(
        join_kernel,
        out_shape=pltpu.HBM(placed.shape, placed.dtype),
        in_specs=[vmem(), pl.BlockSpec(memory_space=pltpu.HBM)] + [vmem()] * (1 + len(strips)),
        out_specs=pl.BlockSpec(memory_space=pltpu.HBM),
        scratch_shapes=[
            pltpu.SMEM(sources.shape, jnp.int32),
            pltpu.VMEM((len(strips), n_out, 2, t_dev, 2 * STRIP), jnp.bfloat16),
            pltpu.VMEM(rest.shape, jnp.float32),
            pltpu.SemaphoreType.DMA((2, 2)),
            pltpu.SemaphoreType.DMA((1,)),
        ],
        input_output_aliases={1: 0},
        compiler_params=pltpu.CompilerParams(vmem_limit_bytes=16 * MIB),
        name="join",
    )(sources, placed, rest, *strips)


def exchange(x, axis):
    return lax.all_to_all(x, axis, split_axis=0, concat_axis=0, tiled=True)


def local(visibilities, kernels, delays, tile_of, plane_of, counts, neighbours):
    n_facet = lax.axis_size("facet")
    n_chan = lax.axis_size("chan")
    facet_index = lax.axis_index("facet")
    halves, facets, blocks, _, bv = visibilities.shape
    fac_dev = facets // n_facet
    n_tiles = 16 * n_chan
    t_dev = n_tiles // n_chan
    n_rows = fac_dev * blocks
    per = n_rows // n_chan

    vis = visibilities.reshape(halves, n_facet * n_chan, per, bv)
    vis, delay, place, code, piece = send_order(
        counts, plane_of, tile_of, delays.reshape(n_chan, per, bv), vis, kernels.shape[0], t_dev
    )
    vis = exchange(vis, ("facet", "chan"))

    rows = exchange(average(delay, vis), "chan")
    main = exchange(grid_rows(piece, rows, place, code, kernels, fac_dev * n_tiles), "chan")

    own = strips_of(main)
    chips = n_facet // 2
    along = lambda x, dz: lax.ppermute(x, "facet", [(f, (f + 2 * dz) % n_facet) for f in range(n_facet)])
    across = lambda x: lax.ppermute(x, "facet", [(f, f ^ 1) for f in range(n_facet)])
    arrived = {dz: along(own, dz) for dz in range(1, chips - 1)}
    placed, rest = place_main(main)
    own, rest = lax.optimization_barrier((own, rest))
    arrived[chips - 1] = along(own, chips - 1)
    strips = [own] + [arrived[dz] for dz in range(1, chips)]
    strips += [across(s) for s in strips]
    mine = lax.dynamic_slice_in_dim(neighbours, facet_index * fac_dev, fac_dev, 0)
    group = mine // fac_dev
    source = (facet_index // 2 - group // 2) % chips + chips * ((group + facet_index) % 2)
    sources = jnp.concatenate([source, mine % fac_dev], axis=1).astype(jnp.int32)
    return join(sources, placed, rest, strips)


def solution(mesh):
    return jax.shard_map(
        local,
        mesh=mesh,
        in_specs=(
            P(None, None, None, ("facet", "chan"), None),
            P(),
            P("facet", None, None),
            P("facet", None),
            P("facet", None),
            P("facet"),
            P(),
        ),
        out_specs=P("chan", "facet", None, None),
        check_vma=False,
    )
```

```python
import functools
import math

import jax
import jax.numpy as jnp
from jax import lax
from jax.experimental import pallas as pl
from jax.experimental.pallas import tpu as pltpu
from jax.sharding import PartitionSpec as P

AVG = 8
TS = 16
EDGE = 4
STRIP = EDGE * TS
GROUP = 16
PIECE = 64
STRETCH = 8
MIB = 1024 * 1024

SIN = (-1.0 / 6, 1.0 / 120, -1.0 / 5040, 1.0 / 362880, -1.0 / 39916800)
COS = (-1.0 / 2, 1.0 / 24, -1.0 / 720, 1.0 / 40320, -1.0 / 3628800, 1.0 / 479001600)


def series(turns):
    x = (2.0 * math.pi) * turns
    y = x * x
    s = jnp.full_like(x, SIN[-1])
    for k in SIN[-2::-1]:
        s = s * y + k
    c = jnp.full_like(x, COS[-1])
    for k in COS[-2::-1]:
        c = c * y + k
    return c * y + 1.0, (s * y + 1.0) * x


def turn_by(turns):
    half = jnp.round(2.0 * turns)
    c, s = series(turns - 0.5 * half)
    odd = (half - 2.0 * jnp.floor(0.5 * half)) > 0.5
    sign = jnp.where(odd, -1.0, 1.0)
    return c * sign, s * sign


def times(a, b):
    return a[0] * b[0] - a[1] * b[1], a[0] * b[1] + a[1] * b[0]


def vmem():
    return pl.BlockSpec(memory_space=pltpu.VMEM)


def to_bf16(mask):
    return mask.astype(jnp.float32).astype(jnp.bfloat16)


def iota(shape, dim):
    return lax.broadcasted_iota(jnp.int32, shape, dim)


def fill_tables(n_planes, t_dev, count_ref, plane_ref, tile_ref, place_ref, code_ref, piece_ref):
    f32 = jnp.float32
    slots, blocks = plane_ref.shape
    n_rows = slots * blocks
    planes, tiles = [], []
    for slot in range(slots):
        alive = iota((1, blocks), 1) < count_ref[slot]
        planes.append(jnp.where(alive, plane_ref[slot : slot + 1, :], -1))
        tiles.append(tile_ref[slot : slot + 1, :])
    plane = jnp.concatenate(planes, axis=1)
    tile = jnp.concatenate(tiles, axis=1)
    mine = plane == iota((n_planes, n_rows), 0)
    before = to_bf16(iota((n_rows, n_rows), 0) < iota((n_rows, n_rows), 1))
    rank = jnp.dot(to_bf16(mine), before, preferred_element_type=f32)
    count = jnp.sum(mine.astype(f32), axis=1, keepdims=True)
    groups = jnp.floor((count + (GROUP - 1)) * (1.0 / GROUP))
    pieces = jnp.floor((groups + (PIECE // GROUP - 1)) * (GROUP / PIECE))
    earlier = to_bf16(iota((n_planes, n_planes), 1) < iota((n_planes, n_planes), 0))
    both = jnp.concatenate(
        [jnp.broadcast_to(groups, (n_planes, 128)), jnp.broadcast_to(pieces, (n_planes, 128))], axis=1
    )
    both = jnp.dot(earlier, both.astype(jnp.bfloat16), preferred_element_type=f32)
    first_group = both[:, 0:1]
    first_piece = both[:, 128:129]
    place = jnp.sum(jnp.where(mine, rank + GROUP * first_group, 0.0), axis=0, keepdims=True)
    live = jnp.sum(mine.astype(f32), axis=0, keepdims=True)
    place = jnp.where(live > 0.5, place, -1.0).astype(jnp.int32)
    place_ref[...] = place
    n_used = code_ref.shape[1]
    order = to_bf16(iota((n_used, n_rows), 0) == place)

    row = iota((8, n_rows), 0)
    slot = (iota((8, n_rows), 1) >= n_rows // 2).astype(f32)
    values = jnp.where(row == 0, tile.astype(f32) + 1.0, jnp.where(row == 1, slot, 0.0))
    ordered = lax.dot_general(
        values.astype(jnp.bfloat16), order, (((1,), (1,)), ((), ())), preferred_element_type=f32
    )
    tile = ordered[0:1].astype(jnp.int32) - 1
    slot = ordered[1:2].astype(jnp.int32)
    code = (tile // t_dev) * (2 * t_dev) + slot * t_dev + tile % t_dev
    code_ref[...] = jnp.where(tile < 0, -1, code)

    lower = jnp.sum(jnp.where(iota((n_planes, 1), 0) < n_planes // 2, pieces, 0.0))
    upper = jnp.sum(pieces) - lower
    lane = iota((n_planes, 128), 1)
    at = (lane % 64).astype(f32)
    is_upper = lane >= 64
    which = jnp.minimum(at, jnp.where(is_upper, upper, lower) - 1.0) + jnp.where(is_upper, lower, 0.0)
    taken = (which >= first_piece) & (which < first_piece + pieces)
    group = first_group + (PIECE // GROUP) * (which - first_piece)
    group = jnp.sum(jnp.where(taken, group, 0.0), axis=0, keepdims=True)
    owner = jnp.sum(jnp.where(taken, iota((n_planes, 128), 0).astype(f32), 0.0), axis=0, keepdims=True)
    owner = owner - jnp.where(iota((1, 128), 1) >= 64, float(n_planes // 2), 0.0)
    row = iota((8, 128), 0)
    totals = jnp.where(iota((8, 128), 1) >= 64, upper, lower)
    value = jnp.where(row == 0, group, jnp.where(row == 1, jnp.maximum(owner, 0.0), jnp.where(row == 2, totals, 0.0)))
    piece_ref[...] = value.astype(jnp.int32)


def sizes(n_rows, n_planes):
    used = n_rows + n_planes * (GROUP - 1)
    n_order = -(-(used - GROUP + PIECE) // 32) * 32
    n_used = -(-used // 256) * 256
    assert n_used <= n_order
    return n_order, n_used


def send_kernel(n_planes, t_dev, *refs):
    (count_hbm, plane_hbm, tile_hbm, delay_hbm, vis_hbm), refs = refs[:5], refs[5:]
    (out_ref, inner_ref, outer_ref, *tables), scratch = refs[:-6], refs[-6:]
    delay_ref, count_ref, plane_ref, tile_ref, small_sem, sem = scratch
    smalls = [
        pltpu.make_async_copy(count_hbm, count_ref, small_sem.at[0]),
        pltpu.make_async_copy(plane_hbm, plane_ref, small_sem.at[1]),
        pltpu.make_async_copy(tile_hbm, tile_ref, small_sem.at[2]),
        pltpu.make_async_copy(delay_hbm.at[lax.axis_index("chan")], delay_ref, small_sem.at[3]),
    ]
    for copy in smalls:
        copy.start()
    for copy in smalls:
        copy.wait()
    halves, dests = vis_hbm.shape[:2]
    n = sem.shape[1]
    copies = []
    for i in range(n):
        at = pl.ds(i * (dests // n), dests // n)
        for h in range(halves):
            copies.append(pltpu.make_async_copy(vis_hbm.at[h, at], out_ref.at[at, h], sem.at[h, i]))
            copies[-1].start()

    @pl.when(count_ref[0] >= 0)
    def _():
        fill_turns(delay_ref[...], inner_ref, outer_ref)
        fill_tables(n_planes, t_dev, count_ref, plane_ref, tile_ref, *tables)

    for copy in copies:
        copy.wait()


def send_order(counts, planes, tiles, delays, vis, n_planes, n_out, t_dev):
    halves, dests, rows, bv = vis.shape
    n_rows = planes.shape[0] * planes.shape[1]
    n_order, n_used = sizes(n_rows, n_planes)
    args = [pltpu.with_memory_space_constraint(x, pltpu.HBM) for x in (counts, planes, tiles, delays, vis)]
    return pl.pallas_call(
        functools.partial(send_kernel, n_planes, t_dev),
        out_shape=[
            jax.ShapeDtypeStruct((dests, halves, rows, bv), vis.dtype),
            jax.ShapeDtypeStruct((AVG - 1, 2, rows, bv), jnp.float32),
            jax.ShapeDtypeStruct((n_out, 2, rows, bv), jnp.float32),
            jax.ShapeDtypeStruct((1, n_rows), jnp.int32),
            jax.ShapeDtypeStruct((1, n_used), jnp.int32),
            jax.ShapeDtypeStruct((8, 128), jnp.int32),
        ],
        in_specs=[pl.BlockSpec(memory_space=pltpu.HBM)] * len(args),
        out_specs=[vmem()] * 6,
        scratch_shapes=[
            pltpu.VMEM((rows, bv), jnp.float32),
            pltpu.SMEM(counts.shape, jnp.int32),
            pltpu.VMEM(planes.shape, jnp.int32),
            pltpu.VMEM(tiles.shape, jnp.int32),
            pltpu.SemaphoreType.DMA((4,)),
            pltpu.SemaphoreType.DMA((halves, 2)),
        ],
        compiler_params=pltpu.CompilerParams(vmem_limit_bytes=32 * MIB),
        name="send_order",
    )(*args)


def fill_turns(d, inner_ref, outer_ref):
    small = series(d * (1.0 / 256.0))
    table = [None, small]
    for j in range(2, AVG):
        table.append(times(table[j // 2], table[j - j // 2]))
    for j in range(1, AVG):
        inner_ref[j - 1, 0] = table[j][0]
        inner_ref[j - 1, 1] = table[j][1]
    c, s = turn_by(d)
    turn = (c * (1.0 / AVG), s * (1.0 / AVG))
    step = series(d * (1.0 / 32.0))
    for o in range(outer_ref.shape[0]):
        outer_ref[o, 0] = turn[0]
        outer_ref[o, 1] = turn[1]
        turn = times(turn, step)


def average_kernel(inner_ref, outer_ref, vis_ref, out_ref):
    n_out, _, rows, _ = out_ref.shape
    for r in range(0, rows, 16):
        at = slice(r, r + 16)
        table = [(inner_ref[j, 0, at], inner_ref[j, 1, at]) for j in range(AVG - 1)]

        def one(o, carry, at=at, table=table):
            c = o * AVG
            re = vis_ref[c, 0, at].astype(jnp.float32)
            im = vis_ref[c, 1, at].astype(jnp.float32)
            for j in range(1, AVG):
                a = vis_ref[c + j, 0, at].astype(jnp.float32)
                b = vis_ref[c + j, 1, at].astype(jnp.float32)
                tc, ts = table[j - 1]
                re += a * tc - b * ts
                im += a * ts + b * tc
            tc = outer_ref[o, 0, at]
            ts = outer_ref[o, 1, at]
            out_ref[o, 0, at] = (re * tc - im * ts).astype(jnp.bfloat16)
            out_ref[o, 1, at] = (re * ts + im * tc).astype(jnp.bfloat16)
            return carry

        lax.fori_loop(0, n_out, one, 0, unroll=4)


def average(inner, outer, vis):
    n_ch, halves, rows, bv = vis.shape
    n_out = n_ch // AVG
    return pl.pallas_call(
        average_kernel,
        out_shape=jax.ShapeDtypeStruct((n_out, halves, rows, bv), jnp.bfloat16),
        in_specs=[vmem()] * 3,
        out_specs=vmem(),
        compiler_params=pltpu.CompilerParams(vmem_limit_bytes=8 * MIB),
        cost_estimate=pl.CostEstimate(flops=300 * 9 * n_ch * halves * rows * bv, transcendentals=0, bytes_accessed=300 * 5 * MIB),
        name="average",
    )(inner, outer, vis)


def grid_kernel(n_pieces, *refs):
    piece_vmem, rows_ref, place_ref, code_ref, k_ref, out_ref, piece_ref, x_ref, c_ref, piece_sem = refs
    piece_copy = pltpu.make_async_copy(piece_vmem, piece_ref, piece_sem.at[0])
    piece_copy.start()
    n_src, _, per, bv = rows_ref.shape
    re = rows_ref[:, 0].reshape(n_src * per, bv)
    im = rows_ref[:, 1].reshape(n_src * per, bv)
    x = jnp.concatenate([re, im], axis=1)
    order = to_bf16(iota((x_ref.shape[0], n_src * per), 0) == place_ref[...])
    x_ref[...] = jnp.dot(order, x, preferred_element_type=jnp.float32).astype(jnp.bfloat16)
    c_ref[...] = jnp.zeros_like(c_ref)
    piece_copy.wait()
    for lane, first in ((0, 0), (64, k_ref.shape[0] // 2)):
        for begin in range(0, n_pieces, STRETCH):

            @pl.when(begin < piece_ref[2, lane])
            def _(begin=begin, lane=lane, first=first):
                for i in range(lane + begin, lane + min(begin + STRETCH, n_pieces)):
                    at = pl.ds(pl.multiple_of(piece_ref[0, i] * GROUP, GROUP), PIECE)
                    product = jnp.dot(x_ref[at, :], k_ref[first + piece_ref[1, i]], preferred_element_type=jnp.float32)
                    c_ref[at, :] = product.astype(jnp.bfloat16)

    n_used = code_ref.shape[1]
    tiles = to_bf16(iota((out_ref.shape[0] * out_ref.shape[1], n_used), 0) == code_ref[...])
    grid = jnp.dot(tiles, c_ref[:n_used, :], preferred_element_type=jnp.float32)
    out_ref[...] = grid.astype(jnp.bfloat16).reshape(out_ref.shape)


def grid_rows(piece, rows, place, code, kernels, n_codes):
    n_planes, k_rows, cells = kernels.shape
    n_rows = place.shape[1]
    n_order, _ = sizes(n_rows, n_planes)
    n_chan = rows.shape[0]
    n_pieces = n_rows // PIECE + n_planes // 2
    assert n_pieces <= 64
    return pl.pallas_call(
        functools.partial(grid_kernel, n_pieces),
        out_shape=jax.ShapeDtypeStruct((n_chan, n_codes // n_chan, cells), jnp.bfloat16),
        in_specs=[vmem()] * 5,
        out_specs=vmem(),
        scratch_shapes=[
            pltpu.SMEM(piece.shape, jnp.int32),
            pltpu.VMEM((n_order, k_rows), jnp.bfloat16),
            pltpu.VMEM((n_order, cells), jnp.bfloat16),
            pltpu.SemaphoreType.DMA((1,)),
        ],
        compiler_params=pltpu.CompilerParams(vmem_limit_bytes=20 * MIB),
        name="grid_rows",
    )(piece, rows, place, code, kernels)


def strip_kernel(main_ref, out_ref):
    n_out, per, cells = main_ref.shape
    half = cells // 2
    low = main_ref[:, :, :128].reshape(n_out * per, 128).astype(jnp.float32)
    high = main_ref[:, :, half : half + 128].reshape(n_out * per, 128).astype(jnp.float32)
    lane = lax.broadcasted_iota(jnp.int32, low.shape, 1)
    strip = jnp.where(lane < STRIP, low, pltpu.roll(high, STRIP, 1)).astype(jnp.bfloat16)
    out_ref[...] = strip.reshape(out_ref.shape)


def strips_of(main):
    n_out, per, _ = main.shape
    return pl.pallas_call(
        strip_kernel,
        out_shape=jax.ShapeDtypeStruct((n_out, per, 2 * STRIP), jnp.bfloat16),
        in_specs=[vmem()],
        out_specs=vmem(),
        compiler_params=pltpu.CompilerParams(vmem_limit_bytes=8 * MIB),
        name="strips",
    )(main)


def placing(n_out, t_dev):
    n_rows = n_out * t_dev
    to = iota((n_rows, n_rows), 0)
    return (iota((n_rows, n_rows), 1) == (to % n_out) * t_dev + to // n_out).astype(jnp.float32)


def place_kernel(main_ref, out_hbm, rest_ref, done_ref, sem):
    n_out, per, cells = main_ref.shape
    t_dev = per // 2
    run = cells // 4
    place = placing(n_out, t_dev).astype(jnp.bfloat16)
    copies = []
    for slot in range(2):
        main = main_ref[:, slot * t_dev : (slot + 1) * t_dev, :].reshape(n_out * t_dev, cells)
        main = jnp.dot(place, main, preferred_element_type=jnp.float32)
        for i in range(2):
            at = slice(2 * i * run, (2 * i + 1) * run)
            done_ref[i, :, slot] = main[:, at].reshape(t_dev, n_out, run)
            rest_ref[i, :, slot] = main[:, at.stop : at.stop + run].reshape(t_dev, n_out, run)
    for i in range(2):
        copies.append(pltpu.make_async_copy(done_ref.at[i], out_hbm.at[:, :, :, pl.ds(2 * i * run, run)], sem.at[i]))
        copies[-1].start()
    for copy in copies:
        copy.wait()


def place_main(main):
    n_out, per, cells = main.shape
    part = (2, per // 2, 2, n_out, cells // 4)
    return pl.pallas_call(
        place_kernel,
        out_shape=[
            pltpu.HBM((per // 2, 2, n_out, cells), jnp.float32),
            jax.ShapeDtypeStruct(part, jnp.float32),
        ],
        in_specs=[vmem()],
        out_specs=[pl.BlockSpec(memory_space=pltpu.HBM), vmem()],
        scratch_shapes=[pltpu.VMEM(part, jnp.float32), pltpu.SemaphoreType.DMA((2,))],
        compiler_params=pltpu.CompilerParams(vmem_limit_bytes=8 * MIB),
        cost_estimate=pl.CostEstimate(flops=2 * n_out * per * n_out * per // 2 * cells, transcendentals=0, bytes_accessed=3 * MIB // 2),
        name="place",
    )(main)


def join_kernel(nb_vmem, placed_hbm, rest_ref, *refs):
    strips, (out_hbm, nb_ref, strip_ref, done_ref, sem, nb_sem) = refs[:-6], refs[-6:]
    nb_copy = pltpu.make_async_copy(nb_vmem, nb_ref, nb_sem.at[0])
    nb_copy.start()
    _, t_dev, _, n_out, run = rest_ref.shape
    n_rows = n_out * t_dev
    for i, ref in enumerate(strips):
        strip_ref[i] = ref[...].reshape(strip_ref.shape[1:])
    upper = iota((n_rows, 2 * STRIP), 1) >= STRIP
    quarter = (0.25 * placing(n_out, t_dev)).astype(jnp.bfloat16)
    n_nb = nb_ref.shape[1] // 2
    nb_copy.wait()
    copies = []
    for slot in range(2):
        blend = jnp.zeros((n_rows, 2 * STRIP), jnp.float32)
        for k in range(n_nb):
            strip = strip_ref[nb_ref[slot, k], :, nb_ref[slot, n_nb + k]].reshape(n_rows, 2 * STRIP)
            blend += jnp.dot(quarter, strip, preferred_element_type=jnp.float32)
        for i, part in enumerate((pltpu.roll(blend, STRIP, 1), blend)):
            part = jnp.where(upper, part, 0.0).reshape(t_dev, n_out, run)
            done_ref[i, :, slot] = rest_ref[i, :, slot] + part
            target = out_hbm.at[:, slot, :, pl.ds((2 * i + 1) * run, run)]
            copies.append(pltpu.make_async_copy(done_ref.at[i, :, slot], target, sem.at[slot, i]))
            copies[-1].start()
    for copy in copies:
        copy.wait()


def join(sources, placed, rest, strips):
    _, t_dev, _, n_out, run = rest.shape
    assert run == 2 * STRIP
    return pl.pallas_call(
        join_kernel,
        out_shape=pltpu.HBM(placed.shape, placed.dtype),
        in_specs=[vmem(), pl.BlockSpec(memory_space=pltpu.HBM)] + [vmem()] * (1 + len(strips)),
        out_specs=pl.BlockSpec(memory_space=pltpu.HBM),
        scratch_shapes=[
            pltpu.SMEM(sources.shape, jnp.int32),
            pltpu.VMEM((len(strips), n_out, 2, t_dev, 2 * STRIP), jnp.bfloat16),
            pltpu.VMEM(rest.shape, jnp.float32),
            pltpu.SemaphoreType.DMA((2, 2)),
            pltpu.SemaphoreType.DMA((1,)),
        ],
        input_output_aliases={1: 0},
        compiler_params=pltpu.CompilerParams(vmem_limit_bytes=16 * MIB),
        name="join",
    )(sources, placed, rest, *strips)


def exchange(x, axis):
    return lax.all_to_all(x, axis, split_axis=0, concat_axis=0, tiled=True)


def local(visibilities, kernels, delays, tile_of, plane_of, counts, neighbours):
    n_facet = lax.axis_size("facet")
    n_chan = lax.axis_size("chan")
    facet_index = lax.axis_index("facet")
    halves, facets, blocks, _, bv = visibilities.shape
    fac_dev = facets // n_facet
    n_tiles = 16 * n_chan
    t_dev = n_tiles // n_chan
    n_rows = fac_dev * blocks
    per = n_rows // n_chan

    vis = visibilities.reshape(halves, n_facet * n_chan, per, bv)
    vis, inner, outer, place, code, piece = send_order(
        counts, plane_of, tile_of, delays.reshape(n_chan, per, bv), vis, kernels.shape[0], n_chan, t_dev
    )
    vis = exchange(vis, ("facet", "chan"))

    rows = exchange(average(inner, outer, vis), "chan")
    main = exchange(grid_rows(piece, rows, place, code, kernels, fac_dev * n_tiles), "chan")

    own = strips_of(main)
    chips = n_facet // 2
    along = lambda x, dz: lax.ppermute(x, "facet", [(f, (f + 2 * dz) % n_facet) for f in range(n_facet)])
    across = lambda x: lax.ppermute(x, "facet", [(f, f ^ 1) for f in range(n_facet)])
    arrived = {dz: along(own, dz) for dz in range(1, chips - 1)}
    placed, rest = place_main(main)
    own, rest = lax.optimization_barrier((own, rest))
    arrived[chips - 1] = along(own, chips - 1)
    strips = [own] + [arrived[dz] for dz in range(1, chips)]
    strips += [across(s) for s in strips]
    mine = lax.dynamic_slice_in_dim(neighbours, facet_index * fac_dev, fac_dev, 0)
    group = mine // fac_dev
    source = (facet_index // 2 - group // 2) % chips + chips * ((group + facet_index) % 2)
    sources = jnp.concatenate([source, mine % fac_dev], axis=1).astype(jnp.int32)
    return join(sources, placed, rest, strips)


def solution(mesh):
    return jax.shard_map(
        local,
        mesh=mesh,
        in_specs=(
            P(None, None, None, ("facet", "chan"), None),
            P(),
            P("facet", None, None),
            P("facet", None),
            P("facet", None),
            P("facet"),
            P(),
        ),
        out_specs=P("chan", "facet", None, None),
        check_vma=False,
    )
```

```python
import functools
import math

import jax
import jax.numpy as jnp
from jax import lax
from jax.experimental import pallas as pl
from jax.experimental.pallas import tpu as pltpu
from jax.sharding import PartitionSpec as P

AVG = 8
TS = 16
EDGE = 4
STRIP = EDGE * TS
GROUP = 16
PIECE = 64
STRETCH = 8
MIB = 1024 * 1024

SIN = (-1.0 / 6, 1.0 / 120, -1.0 / 5040, 1.0 / 362880, -1.0 / 39916800)
COS = (-1.0 / 2, 1.0 / 24, -1.0 / 720, 1.0 / 40320, -1.0 / 3628800, 1.0 / 479001600)


def series(turns):
    x = (2.0 * math.pi) * turns
    y = x * x
    s = jnp.full_like(x, SIN[-1])
    for k in SIN[-2::-1]:
        s = s * y + k
    c = jnp.full_like(x, COS[-1])
    for k in COS[-2::-1]:
        c = c * y + k
    return c * y + 1.0, (s * y + 1.0) * x


def turn_by(turns):
    half = jnp.round(2.0 * turns)
    c, s = series(turns - 0.5 * half)
    odd = (half - 2.0 * jnp.floor(0.5 * half)) > 0.5
    sign = jnp.where(odd, -1.0, 1.0)
    return c * sign, s * sign


def times(a, b):
    return a[0] * b[0] - a[1] * b[1], a[0] * b[1] + a[1] * b[0]


def vmem():
    return pl.BlockSpec(memory_space=pltpu.VMEM)


def to_bf16(mask):
    return mask.astype(jnp.float32).astype(jnp.bfloat16)


def iota(shape, dim):
    return lax.broadcasted_iota(jnp.int32, shape, dim)


def fill_tables(n_planes, t_dev, count_ref, plane_ref, tile_ref, place_ref, code_ref, piece_ref):
    f32 = jnp.float32
    slots, blocks = plane_ref.shape
    n_rows = slots * blocks
    planes, tiles = [], []
    for slot in range(slots):
        alive = iota((1, blocks), 1) < count_ref[slot]
        planes.append(jnp.where(alive, plane_ref[slot : slot + 1, :], -1))
        tiles.append(tile_ref[slot : slot + 1, :])
    plane = jnp.concatenate(planes, axis=1)
    tile = jnp.concatenate(tiles, axis=1)
    mine = plane == iota((n_planes, n_rows), 0)
    before = to_bf16(iota((n_rows, n_rows), 0) < iota((n_rows, n_rows), 1))
    rank = jnp.dot(to_bf16(mine), before, preferred_element_type=f32)
    count = jnp.sum(mine.astype(f32), axis=1, keepdims=True)
    groups = jnp.floor((count + (GROUP - 1)) * (1.0 / GROUP))
    pieces = jnp.floor((groups + (PIECE // GROUP - 1)) * (GROUP / PIECE))
    earlier = to_bf16(iota((n_planes, n_planes), 1) < iota((n_planes, n_planes), 0))
    both = jnp.concatenate(
        [jnp.broadcast_to(groups, (n_planes, 128)), jnp.broadcast_to(pieces, (n_planes, 128))], axis=1
    )
    both = jnp.dot(earlier, both.astype(jnp.bfloat16), preferred_element_type=f32)
    first_group = both[:, 0:1]
    first_piece = both[:, 128:129]
    place = jnp.sum(jnp.where(mine, rank + GROUP * first_group, 0.0), axis=0, keepdims=True)
    live = jnp.sum(mine.astype(f32), axis=0, keepdims=True)
    place = jnp.where(live > 0.5, place, -1.0).astype(jnp.int32)
    place_ref[...] = place
    n_used = code_ref.shape[1]
    order = to_bf16(iota((n_used, n_rows), 0) == place)

    row = iota((8, n_rows), 0)
    slot = (iota((8, n_rows), 1) >= n_rows // 2).astype(f32)
    values = jnp.where(row == 0, tile.astype(f32) + 1.0, jnp.where(row == 1, slot, 0.0))
    ordered = lax.dot_general(
        values.astype(jnp.bfloat16), order, (((1,), (1,)), ((), ())), preferred_element_type=f32
    )
    tile = ordered[0:1].astype(jnp.int32) - 1
    slot = ordered[1:2].astype(jnp.int32)
    code = (tile // t_dev) * (2 * t_dev) + slot * t_dev + tile % t_dev
    code_ref[...] = jnp.where(tile < 0, -1, code)

    lower = jnp.sum(jnp.where(iota((n_planes, 1), 0) < n_planes // 2, pieces, 0.0))
    upper = jnp.sum(pieces) - lower
    lane = iota((n_planes, 128), 1)
    at = (lane % 64).astype(f32)
    is_upper = lane >= 64
    which = jnp.minimum(at, jnp.where(is_upper, upper, lower) - 1.0) + jnp.where(is_upper, lower, 0.0)
    taken = (which >= first_piece) & (which < first_piece + pieces)
    group = first_group + (PIECE // GROUP) * (which - first_piece)
    group = jnp.sum(jnp.where(taken, group, 0.0), axis=0, keepdims=True)
    owner = jnp.sum(jnp.where(taken, iota((n_planes, 128), 0).astype(f32), 0.0), axis=0, keepdims=True)
    owner = owner - jnp.where(iota((1, 128), 1) >= 64, float(n_planes // 2), 0.0)
    row = iota((8, 128), 0)
    totals = jnp.where(iota((8, 128), 1) >= 64, upper, lower)
    value = jnp.where(row == 0, group, jnp.where(row == 1, jnp.maximum(owner, 0.0), jnp.where(row == 2, totals, 0.0)))
    piece_ref[...] = value.astype(jnp.int32)


def sizes(n_rows, n_planes):
    used = n_rows + n_planes * (GROUP - 1)
    n_order = -(-(used - GROUP + PIECE) // 32) * 32
    n_used = -(-used // 256) * 256
    assert n_used <= n_order
    return n_order, n_used


def send_kernel(n_planes, t_dev, *refs):
    (count_hbm, plane_hbm, tile_hbm, delay_hbm, vis_hbm), refs = refs[:5], refs[5:]
    (out_ref, inner_ref, outer_ref, *tables), scratch = refs[:-6], refs[-6:]
    delay_ref, count_ref, plane_ref, tile_ref, small_sem, sem = scratch
    smalls = [
        pltpu.make_async_copy(count_hbm, count_ref, small_sem.at[0]),
        pltpu.make_async_copy(plane_hbm, plane_ref, small_sem.at[1]),
        pltpu.make_async_copy(tile_hbm, tile_ref, small_sem.at[2]),
        pltpu.make_async_copy(delay_hbm.at[lax.axis_index("chan")], delay_ref, small_sem.at[3]),
    ]
    for copy in smalls:
        copy.start()
    for copy in smalls:
        copy.wait()
    halves, dests = vis_hbm.shape[:2]
    n = sem.shape[1]
    copies = []
    for i in range(n):
        at = pl.ds(i * (dests // n), dests // n)
        for h in range(halves):
            copies.append(pltpu.make_async_copy(vis_hbm.at[h, at], out_ref.at[at, h], sem.at[h, i]))
            copies[-1].start()

    @pl.when(count_ref[0] >= 0)
    def _():
        fill_turns(delay_ref[...], inner_ref, outer_ref)
        fill_tables(n_planes, t_dev, count_ref, plane_ref, tile_ref, *tables)

    for copy in copies:
        copy.wait()


def send_order(counts, planes, tiles, delays, vis, n_planes, n_out, t_dev):
    halves, dests, rows, bv = vis.shape
    n_rows = planes.shape[0] * planes.shape[1]
    n_order, n_used = sizes(n_rows, n_planes)
    args = [pltpu.with_memory_space_constraint(x, pltpu.HBM) for x in (counts, planes, tiles, delays, vis)]
    return pl.pallas_call(
        functools.partial(send_kernel, n_planes, t_dev),
        out_shape=[
            jax.ShapeDtypeStruct((dests, halves, rows, bv), vis.dtype),
            jax.ShapeDtypeStruct((AVG - 1, 2, rows, bv), jnp.float32),
            jax.ShapeDtypeStruct((n_out, 2, rows, bv), jnp.float32),
            jax.ShapeDtypeStruct((1, n_rows), jnp.int32),
            jax.ShapeDtypeStruct((1, n_used), jnp.int32),
            jax.ShapeDtypeStruct((8, 128), jnp.int32),
        ],
        in_specs=[pl.BlockSpec(memory_space=pltpu.HBM)] * len(args),
        out_specs=[vmem()] * 6,
        scratch_shapes=[
            pltpu.VMEM((rows, bv), jnp.float32),
            pltpu.SMEM(counts.shape, jnp.int32),
            pltpu.VMEM(planes.shape, jnp.int32),
            pltpu.VMEM(tiles.shape, jnp.int32),
            pltpu.SemaphoreType.DMA((4,)),
            pltpu.SemaphoreType.DMA((halves, 2)),
        ],
        compiler_params=pltpu.CompilerParams(vmem_limit_bytes=32 * MIB),
        name="send_order",
    )(*args)


def fill_turns(d, inner_ref, outer_ref):
    small = series(d * (1.0 / 256.0))
    table = [None, small]
    for j in range(2, AVG):
        table.append(times(table[j // 2], table[j - j // 2]))
    for j in range(1, AVG):
        inner_ref[j - 1, 0] = table[j][0]
        inner_ref[j - 1, 1] = table[j][1]
    c, s = turn_by(d)
    turn = (c * (1.0 / AVG), s * (1.0 / AVG))
    step = series(d * (1.0 / 32.0))
    for o in range(outer_ref.shape[0]):
        outer_ref[o, 0] = turn[0]
        outer_ref[o, 1] = turn[1]
        turn = times(turn, step)


def average_kernel(inner_ref, outer_ref, vis_ref, out_ref):
    n_out, _, rows, _ = out_ref.shape
    for r in range(0, rows, 16):
        at = slice(r, r + 16)
        table = [(inner_ref[j, 0, at], inner_ref[j, 1, at]) for j in range(AVG - 1)]

        def one(o, carry, at=at, table=table):
            c = o * AVG
            re = vis_ref[c, 0, at].astype(jnp.float32)
            im = vis_ref[c, 1, at].astype(jnp.float32)
            for j in range(1, AVG):
                a = vis_ref[c + j, 0, at].astype(jnp.float32)
                b = vis_ref[c + j, 1, at].astype(jnp.float32)
                tc, ts = table[j - 1]
                re += a * tc - b * ts
                im += a * ts + b * tc
            tc = outer_ref[o, 0, at]
            ts = outer_ref[o, 1, at]
            out_ref[o, 0, at] = (re * tc - im * ts).astype(jnp.bfloat16)
            out_ref[o, 1, at] = (re * ts + im * tc).astype(jnp.bfloat16)
            return carry

        lax.fori_loop(0, n_out, one, 0, unroll=4)


def average(inner, outer, vis):
    n_ch, halves, rows, bv = vis.shape
    n_out = n_ch // AVG
    return pl.pallas_call(
        average_kernel,
        out_shape=jax.ShapeDtypeStruct((n_out, halves, rows, bv), jnp.bfloat16),
        in_specs=[vmem()] * 3,
        out_specs=vmem(),
        compiler_params=pltpu.CompilerParams(vmem_limit_bytes=8 * MIB),
        cost_estimate=pl.CostEstimate(flops=300 * 9 * n_ch * halves * rows * bv, transcendentals=0, bytes_accessed=300 * 5 * MIB),
        name="average",
    )(inner, outer, vis)


def grid_kernel(n_pieces, *refs):
    piece_vmem, rows_ref, place_ref, code_ref, k_ref, out_ref, piece_ref, x_ref, c_ref, piece_sem = refs
    piece_copy = pltpu.make_async_copy(piece_vmem, piece_ref, piece_sem.at[0])
    piece_copy.start()
    n_src, _, per, bv = rows_ref.shape
    re = rows_ref[:, 0].reshape(n_src * per, bv)
    im = rows_ref[:, 1].reshape(n_src * per, bv)
    x = jnp.concatenate([re, im], axis=1)
    order = to_bf16(iota((x_ref.shape[0], n_src * per), 0) == place_ref[...])
    x_ref[...] = jnp.dot(order, x, preferred_element_type=jnp.float32).astype(jnp.bfloat16)
    c_ref[...] = jnp.zeros_like(c_ref)
    piece_copy.wait()
    for lane, first in ((0, 0), (64, k_ref.shape[0] // 2)):
        for begin in range(0, n_pieces, STRETCH):

            @pl.when(begin < piece_ref[2, lane])
            def _(begin=begin, lane=lane, first=first):
                for i in range(lane + begin, lane + min(begin + STRETCH, n_pieces)):
                    at = pl.ds(pl.multiple_of(piece_ref[0, i] * GROUP, GROUP), PIECE)
                    product = jnp.dot(x_ref[at, :], k_ref[first + piece_ref[1, i]], preferred_element_type=jnp.float32)
                    c_ref[at, :] = product.astype(jnp.bfloat16)

    n_used = code_ref.shape[1]
    tiles = to_bf16(iota((out_ref.shape[0] * out_ref.shape[1], n_used), 0) == code_ref[...])
    grid = jnp.dot(tiles, c_ref[:n_used, :], preferred_element_type=jnp.float32)
    out_ref[...] = grid.astype(jnp.bfloat16).reshape(out_ref.shape)


def grid_rows(piece, rows, place, code, kernels, n_codes):
    n_planes, k_rows, cells = kernels.shape
    n_rows = place.shape[1]
    n_order, _ = sizes(n_rows, n_planes)
    n_chan = rows.shape[0]
    n_pieces = n_rows // PIECE + n_planes // 2
    assert n_pieces <= 64
    return pl.pallas_call(
        functools.partial(grid_kernel, n_pieces),
        out_shape=jax.ShapeDtypeStruct((n_chan, n_codes // n_chan, cells), jnp.bfloat16),
        in_specs=[vmem()] * 5,
        out_specs=vmem(),
        scratch_shapes=[
            pltpu.SMEM(piece.shape, jnp.int32),
            pltpu.VMEM((n_order, k_rows), jnp.bfloat16),
            pltpu.VMEM((n_order, cells), jnp.bfloat16),
            pltpu.SemaphoreType.DMA((1,)),
        ],
        compiler_params=pltpu.CompilerParams(vmem_limit_bytes=20 * MIB),
        name="grid_rows",
    )(piece, rows, place, code, kernels)


def strip_kernel(main_ref, out_ref):
    n_out, per, cells = main_ref.shape
    half = cells // 2
    low = main_ref[:, :, :128].reshape(n_out * per, 128).astype(jnp.float32)
    high = main_ref[:, :, half : half + 128].reshape(n_out * per, 128).astype(jnp.float32)
    lane = lax.broadcasted_iota(jnp.int32, low.shape, 1)
    strip = jnp.where(lane < STRIP, low, pltpu.roll(high, STRIP, 1)).astype(jnp.bfloat16)
    out_ref[...] = strip.reshape(out_ref.shape)


def strips_of(main):
    n_out, per, _ = main.shape
    return pl.pallas_call(
        strip_kernel,
        out_shape=jax.ShapeDtypeStruct((n_out, per, 2 * STRIP), jnp.bfloat16),
        in_specs=[vmem()],
        out_specs=vmem(),
        compiler_params=pltpu.CompilerParams(vmem_limit_bytes=8 * MIB),
        name="strips",
    )(main)


def placing(n_out, t_dev):
    n_rows = n_out * t_dev
    to = iota((n_rows, n_rows), 0)
    return (iota((n_rows, n_rows), 1) == (to % n_out) * t_dev + to // n_out).astype(jnp.float32)


def place_kernel(main_ref, out_hbm, rest_ref, done_ref, sem):
    n_out, per, cells = main_ref.shape
    t_dev = per // 2
    run = cells // 4
    place = placing(n_out, t_dev).astype(jnp.bfloat16)
    copies = []
    for slot in range(2):
        main = main_ref[:, slot * t_dev : (slot + 1) * t_dev, :].reshape(n_out * t_dev, cells)
        main = jnp.dot(place, main, preferred_element_type=jnp.float32)
        for i in range(2):
            at = slice(2 * i * run, (2 * i + 1) * run)
            done_ref[i, :, slot] = main[:, at].reshape(t_dev, n_out, run)
            rest_ref[i, :, slot] = main[:, at.stop : at.stop + run].reshape(t_dev, n_out, run)
    for i in range(2):
        copies.append(pltpu.make_async_copy(done_ref.at[i], out_hbm.at[:, :, :, pl.ds(2 * i * run, run)], sem.at[i]))
        copies[-1].start()
    for copy in copies:
        copy.wait()


def place_main(main):
    n_out, per, cells = main.shape
    part = (2, per // 2, 2, n_out, cells // 4)
    return pl.pallas_call(
        place_kernel,
        out_shape=[
            pltpu.HBM((per // 2, 2, n_out, cells), jnp.float32),
            jax.ShapeDtypeStruct(part, jnp.float32),
        ],
        in_specs=[vmem()],
        out_specs=[pl.BlockSpec(memory_space=pltpu.HBM), vmem()],
        scratch_shapes=[pltpu.VMEM(part, jnp.float32), pltpu.SemaphoreType.DMA((2,))],
        compiler_params=pltpu.CompilerParams(vmem_limit_bytes=8 * MIB),
        cost_estimate=pl.CostEstimate(flops=2 * n_out * per * n_out * per // 2 * cells, transcendentals=0, bytes_accessed=3 * MIB // 2),
        name="place",
    )(main)


def join_kernel(nb_vmem, placed_hbm, rest_ref, *refs):
    strips, (out_hbm, strip_ref, done_ref, sem) = refs[:-4], refs[-4:]
    nb = nb_vmem[...].astype(jnp.float32)
    at = iota(nb.shape, 0) * nb.shape[1] + iota(nb.shape, 1)
    number = lambda slot, k: jnp.sum(jnp.where(at == slot * nb.shape[1] + k, nb, 0.0)).astype(jnp.int32)
    _, t_dev, _, n_out, run = rest_ref.shape
    n_rows = n_out * t_dev
    for i, ref in enumerate(strips):
        strip_ref[i] = ref[...].reshape(strip_ref.shape[1:])
    upper = iota((n_rows, 2 * STRIP), 1) >= STRIP
    quarter = (0.25 * placing(n_out, t_dev)).astype(jnp.bfloat16)
    n_nb = nb.shape[1] // 2
    copies = []
    for slot in range(2):
        blend = jnp.zeros((n_rows, 2 * STRIP), jnp.float32)
        for k in range(n_nb):
            strip = strip_ref[number(slot, k), :, number(slot, n_nb + k)].reshape(n_rows, 2 * STRIP)
            blend += jnp.dot(quarter, strip, preferred_element_type=jnp.float32)
        for i, part in enumerate((pltpu.roll(blend, STRIP, 1), blend)):
            part = jnp.where(upper, part, 0.0).reshape(t_dev, n_out, run)
            done_ref[i, :, slot] = rest_ref[i, :, slot] + part
            target = out_hbm.at[:, slot, :, pl.ds((2 * i + 1) * run, run)]
            copies.append(pltpu.make_async_copy(done_ref.at[i, :, slot], target, sem.at[slot, i]))
            copies[-1].start()
    for copy in copies:
        copy.wait()


def join(sources, placed, rest, strips):
    _, t_dev, _, n_out, run = rest.shape
    assert run == 2 * STRIP
    return pl.pallas_call(
        join_kernel,
        out_shape=pltpu.HBM(placed.shape, placed.dtype),
        in_specs=[vmem(), pl.BlockSpec(memory_space=pltpu.HBM)] + [vmem()] * (1 + len(strips)),
        out_specs=pl.BlockSpec(memory_space=pltpu.HBM),
        scratch_shapes=[
            pltpu.VMEM((len(strips), n_out, 2, t_dev, 2 * STRIP), jnp.bfloat16),
            pltpu.VMEM(rest.shape, jnp.float32),
            pltpu.SemaphoreType.DMA((2, 2)),
        ],
        input_output_aliases={1: 0},
        compiler_params=pltpu.CompilerParams(vmem_limit_bytes=16 * MIB),
        name="join",
    )(sources, placed, rest, *strips)


def exchange(x, axis):
    return lax.all_to_all(x, axis, split_axis=0, concat_axis=0, tiled=True)


def local(visibilities, kernels, delays, tile_of, plane_of, counts, neighbours):
    n_facet = lax.axis_size("facet")
    n_chan = lax.axis_size("chan")
    facet_index = lax.axis_index("facet")
    halves, facets, blocks, _, bv = visibilities.shape
    fac_dev = facets // n_facet
    n_tiles = 16 * n_chan
    t_dev = n_tiles // n_chan
    n_rows = fac_dev * blocks
    per = n_rows // n_chan

    vis = visibilities.reshape(halves, n_facet * n_chan, per, bv)
    vis, inner, outer, place, code, piece = send_order(
        counts, plane_of, tile_of, delays.reshape(n_chan, per, bv), vis, kernels.shape[0], n_chan, t_dev
    )
    vis = exchange(vis, ("facet", "chan"))

    rows = exchange(average(inner, outer, vis), "chan")
    main = exchange(grid_rows(piece, rows, place, code, kernels, fac_dev * n_tiles), "chan")

    own = strips_of(main)
    chips = n_facet // 2
    along = lambda x, dz: lax.ppermute(x, "facet", [(f, (f + 2 * dz) % n_facet) for f in range(n_facet)])
    across = lambda x: lax.ppermute(x, "facet", [(f, f ^ 1) for f in range(n_facet)])
    arrived = {dz: along(own, dz) for dz in range(1, chips - 1)}
    placed, rest = place_main(main)
    own, rest = lax.optimization_barrier((own, rest))
    arrived[chips - 1] = along(own, chips - 1)
    strips = [own] + [arrived[dz] for dz in range(1, chips)]
    strips += [across(s) for s in strips]
    mine = lax.dynamic_slice_in_dim(neighbours, facet_index * fac_dev, fac_dev, 0)
    group = mine // fac_dev
    source = (facet_index // 2 - group // 2) % chips + chips * ((group + facet_index) % 2)
    sources = jnp.concatenate([source, mine % fac_dev], axis=1).astype(jnp.int32)
    return join(sources, placed, rest, strips)


def solution(mesh):
    return jax.shard_map(
        local,
        mesh=mesh,
        in_specs=(
            P(None, None, None, ("facet", "chan"), None),
            P(),
            P("facet", None, None),
            P("facet", None),
            P("facet", None),
            P("facet"),
            P(),
        ),
        out_specs=P("chan", "facet", None, None),
        check_vma=False,
    )
```

```python
import functools
import math

import jax
import jax.numpy as jnp
from jax import lax
from jax.experimental import pallas as pl
from jax.experimental.pallas import tpu as pltpu
from jax.sharding import PartitionSpec as P

AVG = 8
TS = 16
EDGE = 4
STRIP = EDGE * TS
GROUP = 16
PIECE = 64
STRETCH = 8
MIB = 1024 * 1024

SIN = (-1.0 / 6, 1.0 / 120, -1.0 / 5040, 1.0 / 362880, -1.0 / 39916800)
COS = (-1.0 / 2, 1.0 / 24, -1.0 / 720, 1.0 / 40320, -1.0 / 3628800, 1.0 / 479001600)


def series(turns):
    x = (2.0 * math.pi) * turns
    y = x * x
    s = jnp.full_like(x, SIN[-1])
    for k in SIN[-2::-1]:
        s = s * y + k
    c = jnp.full_like(x, COS[-1])
    for k in COS[-2::-1]:
        c = c * y + k
    return c * y + 1.0, (s * y + 1.0) * x


def turn_by(turns):
    half = jnp.round(2.0 * turns)
    c, s = series(turns - 0.5 * half)
    odd = (half - 2.0 * jnp.floor(0.5 * half)) > 0.5
    sign = jnp.where(odd, -1.0, 1.0)
    return c * sign, s * sign


def times(a, b):
    return a[0] * b[0] - a[1] * b[1], a[0] * b[1] + a[1] * b[0]


def vmem():
    return pl.BlockSpec(memory_space=pltpu.VMEM)


def to_bf16(mask):
    return mask.astype(jnp.float32).astype(jnp.bfloat16)


def iota(shape, dim):
    return lax.broadcasted_iota(jnp.int32, shape, dim)


def fill_tables(n_planes, t_dev, count_ref, plane_ref, tile_ref, place_ref, code_ref, piece_ref):
    f32 = jnp.float32
    slots, blocks = plane_ref.shape
    n_rows = slots * blocks
    planes, tiles = [], []
    for slot in range(slots):
        alive = iota((1, blocks), 1) < count_ref[slot]
        planes.append(jnp.where(alive, plane_ref[slot : slot + 1, :], -1))
        tiles.append(tile_ref[slot : slot + 1, :])
    plane = jnp.concatenate(planes, axis=1)
    tile = jnp.concatenate(tiles, axis=1)
    mine = plane == iota((n_planes, n_rows), 0)
    before = to_bf16(iota((n_rows, n_rows), 0) < iota((n_rows, n_rows), 1))
    rank = jnp.dot(to_bf16(mine), before, preferred_element_type=f32)
    count = jnp.sum(mine.astype(f32), axis=1, keepdims=True)
    groups = jnp.floor((count + (GROUP - 1)) * (1.0 / GROUP))
    pieces = jnp.floor((groups + (PIECE // GROUP - 1)) * (GROUP / PIECE))
    earlier = to_bf16(iota((n_planes, n_planes), 1) < iota((n_planes, n_planes), 0))
    both = jnp.concatenate(
        [jnp.broadcast_to(groups, (n_planes, 128)), jnp.broadcast_to(pieces, (n_planes, 128))], axis=1
    )
    both = jnp.dot(earlier, both.astype(jnp.bfloat16), preferred_element_type=f32)
    first_group = both[:, 0:1]
    first_piece = both[:, 128:129]
    place = jnp.sum(jnp.where(mine, rank + GROUP * first_group, 0.0), axis=0, keepdims=True)
    live = jnp.sum(mine.astype(f32), axis=0, keepdims=True)
    place = jnp.where(live > 0.5, place, -1.0).astype(jnp.int32)
    place_ref[...] = place
    n_used = code_ref.shape[1]
    order = to_bf16(iota((n_used, n_rows), 0) == place)

    row = iota((8, n_rows), 0)
    slot = (iota((8, n_rows), 1) >= n_rows // 2).astype(f32)
    values = jnp.where(row == 0, tile.astype(f32) + 1.0, jnp.where(row == 1, slot, 0.0))
    ordered = lax.dot_general(
        values.astype(jnp.bfloat16), order, (((1,), (1,)), ((), ())), preferred_element_type=f32
    )
    tile = ordered[0:1].astype(jnp.int32) - 1
    slot = ordered[1:2].astype(jnp.int32)
    code = (tile // t_dev) * (2 * t_dev) + slot * t_dev + tile % t_dev
    code_ref[...] = jnp.where(tile < 0, -1, code)

    lower = jnp.sum(jnp.where(iota((n_planes, 1), 0) < n_planes // 2, pieces, 0.0))
    upper = jnp.sum(pieces) - lower
    lane = iota((n_planes, 128), 1)
    at = (lane % 64).astype(f32)
    is_upper = lane >= 64
    which = jnp.minimum(at, jnp.where(is_upper, upper, lower) - 1.0) + jnp.where(is_upper, lower, 0.0)
    taken = (which >= first_piece) & (which < first_piece + pieces)
    group = first_group + (PIECE // GROUP) * (which - first_piece)
    group = jnp.sum(jnp.where(taken, group, 0.0), axis=0, keepdims=True)
    owner = jnp.sum(jnp.where(taken, iota((n_planes, 128), 0).astype(f32), 0.0), axis=0, keepdims=True)
    owner = owner - jnp.where(iota((1, 128), 1) >= 64, float(n_planes // 2), 0.0)
    row = iota((8, 128), 0)
    totals = jnp.where(iota((8, 128), 1) >= 64, upper, lower)
    value = jnp.where(row == 0, group, jnp.where(row == 1, jnp.maximum(owner, 0.0), jnp.where(row == 2, totals, 0.0)))
    piece_ref[...] = value.astype(jnp.int32)


def sizes(n_rows, n_planes):
    used = n_rows + n_planes * (GROUP - 1)
    n_order = -(-(used - GROUP + PIECE) // 32) * 32
    n_used = -(-used // 256) * 256
    assert n_used <= n_order
    return n_order, n_used


def send_kernel(n_planes, t_dev, *refs):
    (count_hbm, plane_hbm, tile_hbm, delay_hbm, vis_hbm), refs = refs[:5], refs[5:]
    (out_ref, inner_ref, outer_ref, *tables), scratch = refs[:-6], refs[-6:]
    delay_ref, count_ref, plane_ref, tile_ref, small_sem, sem = scratch
    smalls = [
        pltpu.make_async_copy(count_hbm, count_ref, small_sem.at[0]),
        pltpu.make_async_copy(plane_hbm, plane_ref, small_sem.at[1]),
        pltpu.make_async_copy(tile_hbm, tile_ref, small_sem.at[2]),
        pltpu.make_async_copy(delay_hbm.at[lax.axis_index("chan")], delay_ref, small_sem.at[3]),
    ]
    for copy in smalls:
        copy.start()
    for copy in smalls:
        copy.wait()
    halves, dests = vis_hbm.shape[:2]
    n = sem.shape[1]
    copies = []
    for i in range(n):
        at = pl.ds(i * (dests // n), dests // n)
        for h in range(halves):
            copies.append(pltpu.make_async_copy(vis_hbm.at[h, at], out_ref.at[at, h], sem.at[h, i]))
            copies[-1].start()

    @pl.when(count_ref[0] >= 0)
    def _():
        fill_turns(delay_ref[...], inner_ref, outer_ref)
        fill_tables(n_planes, t_dev, count_ref, plane_ref, tile_ref, *tables)

    for copy in copies:
        copy.wait()


def send_order(counts, planes, tiles, delays, vis, n_planes, n_out, t_dev):
    halves, dests, rows, bv = vis.shape
    n_rows = planes.shape[0] * planes.shape[1]
    n_order, n_used = sizes(n_rows, n_planes)
    args = [pltpu.with_memory_space_constraint(x, pltpu.HBM) for x in (counts, planes, tiles, delays, vis)]
    return pl.pallas_call(
        functools.partial(send_kernel, n_planes, t_dev),
        out_shape=[
            jax.ShapeDtypeStruct((dests, halves, rows, bv), vis.dtype),
            jax.ShapeDtypeStruct((AVG - 1, 2, rows, bv), jnp.float32),
            jax.ShapeDtypeStruct((n_out, 2, rows, bv), jnp.float32),
            jax.ShapeDtypeStruct((1, n_rows), jnp.int32),
            jax.ShapeDtypeStruct((1, n_used), jnp.int32),
            jax.ShapeDtypeStruct((8, 128), jnp.int32),
        ],
        in_specs=[pl.BlockSpec(memory_space=pltpu.HBM)] * len(args),
        out_specs=[vmem()] * 6,
        scratch_shapes=[
            pltpu.VMEM((rows, bv), jnp.float32),
            pltpu.SMEM(counts.shape, jnp.int32),
            pltpu.VMEM(planes.shape, jnp.int32),
            pltpu.VMEM(tiles.shape, jnp.int32),
            pltpu.SemaphoreType.DMA((4,)),
            pltpu.SemaphoreType.DMA((halves, 2)),
        ],
        compiler_params=pltpu.CompilerParams(vmem_limit_bytes=32 * MIB),
        name="send_order",
    )(*args)


def fill_turns(d, inner_ref, outer_ref):
    small = series(d * (1.0 / 256.0))
    table = [None, small]
    for j in range(2, AVG):
        table.append(times(table[j // 2], table[j - j // 2]))
    for j in range(1, AVG):
        inner_ref[j - 1, 0] = table[j][0]
        inner_ref[j - 1, 1] = table[j][1]
    c, s = turn_by(d)
    turn = (c * (1.0 / AVG), s * (1.0 / AVG))
    step = series(d * (1.0 / 32.0))
    for o in range(outer_ref.shape[0]):
        outer_ref[o, 0] = turn[0]
        outer_ref[o, 1] = turn[1]
        turn = times(turn, step)


def average_kernel(inner_ref, outer_ref, vis_ref, out_ref):
    n_out, _, rows, _ = out_ref.shape
    for r in range(0, rows, 16):
        at = slice(r, r + 16)
        table = [(inner_ref[j, 0, at], inner_ref[j, 1, at]) for j in range(AVG - 1)]

        def one(o, carry, at=at, table=table):
            c = o * AVG
            re = vis_ref[c, 0, at].astype(jnp.float32)
            im = vis_ref[c, 1, at].astype(jnp.float32)
            for j in range(1, AVG):
                a = vis_ref[c + j, 0, at].astype(jnp.float32)
                b = vis_ref[c + j, 1, at].astype(jnp.float32)
                tc, ts = table[j - 1]
                re += a * tc - b * ts
                im += a * ts + b * tc
            tc = outer_ref[o, 0, at]
            ts = outer_ref[o, 1, at]
            out_ref[o, 0, at] = (re * tc - im * ts).astype(jnp.bfloat16)
            out_ref[o, 1, at] = (re * ts + im * tc).astype(jnp.bfloat16)
            return carry

        lax.fori_loop(0, n_out, one, 0, unroll=4)


def average(inner, outer, vis):
    n_ch, halves, rows, bv = vis.shape
    n_out = n_ch // AVG
    return pl.pallas_call(
        average_kernel,
        out_shape=jax.ShapeDtypeStruct((n_out, halves, rows, bv), jnp.bfloat16),
        in_specs=[vmem()] * 3,
        out_specs=vmem(),
        compiler_params=pltpu.CompilerParams(vmem_limit_bytes=8 * MIB),
        cost_estimate=pl.CostEstimate(flops=300 * 9 * n_ch * halves * rows * bv, transcendentals=0, bytes_accessed=300 * 5 * MIB),
        name="average",
    )(inner, outer, vis)


def grid_kernel(n_pieces, *refs):
    piece_vmem, rows_ref, place_ref, code_ref, k_ref, out_ref, piece_ref, x_ref, c_ref, piece_sem = refs
    piece_copy = pltpu.make_async_copy(piece_vmem, piece_ref, piece_sem.at[0])
    piece_copy.start()
    n_src, _, per, bv = rows_ref.shape
    re = rows_ref[:, 0].reshape(n_src * per, bv)
    im = rows_ref[:, 1].reshape(n_src * per, bv)
    x = jnp.concatenate([re, im], axis=1)
    order = to_bf16(iota((x_ref.shape[0], n_src * per), 0) == place_ref[...])
    x_ref[...] = jnp.dot(order, x, preferred_element_type=jnp.float32).astype(jnp.bfloat16)
    c_ref[...] = jnp.zeros_like(c_ref)
    piece_copy.wait()
    for lane, first in ((0, 0), (64, k_ref.shape[0] // 2)):
        for begin in range(0, n_pieces, STRETCH):

            @pl.when(begin < piece_ref[2, lane])
            def _(begin=begin, lane=lane, first=first):
                for i in range(lane + begin, lane + min(begin + STRETCH, n_pieces)):
                    at = pl.ds(pl.multiple_of(piece_ref[0, i] * GROUP, GROUP), PIECE)
                    product = jnp.dot(x_ref[at, :], k_ref[first + piece_ref[1, i]], preferred_element_type=jnp.float32)
                    c_ref[at, :] = product.astype(jnp.bfloat16)

    n_used = code_ref.shape[1]
    tiles = to_bf16(iota((out_ref.shape[0] * out_ref.shape[1], n_used), 0) == code_ref[...])
    grid = jnp.dot(tiles, c_ref[:n_used, :], preferred_element_type=jnp.float32)
    out_ref[...] = grid.astype(jnp.bfloat16).reshape(out_ref.shape)


def grid_rows(piece, rows, place, code, kernels, n_codes):
    n_planes, k_rows, cells = kernels.shape
    n_rows = place.shape[1]
    n_order, _ = sizes(n_rows, n_planes)
    n_chan = rows.shape[0]
    n_pieces = n_rows // PIECE + n_planes // 2
    assert n_pieces <= 64
    return pl.pallas_call(
        functools.partial(grid_kernel, n_pieces),
        out_shape=jax.ShapeDtypeStruct((n_chan, n_codes // n_chan, cells), jnp.bfloat16),
        in_specs=[vmem()] * 5,
        out_specs=vmem(),
        scratch_shapes=[
            pltpu.SMEM(piece.shape, jnp.int32),
            pltpu.VMEM((n_order, k_rows), jnp.bfloat16),
            pltpu.VMEM((n_order, cells), jnp.bfloat16),
            pltpu.SemaphoreType.DMA((1,)),
        ],
        compiler_params=pltpu.CompilerParams(vmem_limit_bytes=20 * MIB),
        name="grid_rows",
    )(piece, rows, place, code, kernels)


def strip_kernel(main_ref, out_ref):
    n_out, per, cells = main_ref.shape
    half = cells // 2
    low = main_ref[:, :, :128].reshape(n_out * per, 128).astype(jnp.float32)
    high = main_ref[:, :, half : half + 128].reshape(n_out * per, 128).astype(jnp.float32)
    lane = lax.broadcasted_iota(jnp.int32, low.shape, 1)
    strip = jnp.where(lane < STRIP, low, pltpu.roll(high, STRIP, 1)).astype(jnp.bfloat16)
    out_ref[...] = strip.reshape(out_ref.shape)


def strips_of(main):
    n_out, per, _ = main.shape
    return pl.pallas_call(
        strip_kernel,
        out_shape=jax.ShapeDtypeStruct((n_out, per, 2 * STRIP), jnp.bfloat16),
        in_specs=[vmem()],
        out_specs=vmem(),
        compiler_params=pltpu.CompilerParams(vmem_limit_bytes=8 * MIB),
        name="strips",
    )(main)


def placing(n_out, t_dev):
    n_rows = n_out * t_dev
    to = iota((n_rows, n_rows), 0)
    return (iota((n_rows, n_rows), 1) == (to % n_out) * t_dev + to // n_out).astype(jnp.float32)


def place_kernel(main_ref, out_hbm, rest_ref, done_ref, sem):
    n_out, per, cells = main_ref.shape
    t_dev = per // 2
    run = cells // 4
    place = placing(n_out, t_dev).astype(jnp.bfloat16)
    copies = []
    for slot in range(2):
        main = main_ref[:, slot * t_dev : (slot + 1) * t_dev, :].reshape(n_out * t_dev, cells)
        main = jnp.dot(place, main, preferred_element_type=jnp.float32)
        for i in range(2):
            at = slice(2 * i * run, (2 * i + 1) * run)
            done_ref[i, :, slot] = main[:, at].reshape(t_dev, n_out, run)
            rest_ref[i, :, slot] = main[:, at.stop : at.stop + run].reshape(t_dev, n_out, run)
    for i in range(2):
        copies.append(pltpu.make_async_copy(done_ref.at[i], out_hbm.at[:, :, :, pl.ds(2 * i * run, run)], sem.at[i]))
        copies[-1].start()
    for copy in copies:
        copy.wait()


def place_main(main):
    n_out, per, cells = main.shape
    part = (2, per // 2, 2, n_out, cells // 4)
    return pl.pallas_call(
        place_kernel,
        out_shape=[
            pltpu.HBM((per // 2, 2, n_out, cells), jnp.float32),
            jax.ShapeDtypeStruct(part, jnp.float32),
        ],
        in_specs=[vmem()],
        out_specs=[pl.BlockSpec(memory_space=pltpu.HBM), vmem()],
        scratch_shapes=[pltpu.VMEM(part, jnp.float32), pltpu.SemaphoreType.DMA((2,))],
        compiler_params=pltpu.CompilerParams(vmem_limit_bytes=8 * MIB),
        cost_estimate=pl.CostEstimate(flops=2 * n_out * per * n_out * per // 2 * cells, transcendentals=0, bytes_accessed=3 * MIB // 2),
        name="place",
    )(main)


def join_kernel(nb_vmem, placed_hbm, rest_ref, *refs):
    strips, (out_hbm, strip_ref, done_ref, sem) = refs[:-4], refs[-4:]
    nb = nb_vmem[...].astype(jnp.float32)
    at = iota(nb.shape, 0) * nb.shape[1] + iota(nb.shape, 1)
    number = lambda slot, k: jnp.sum(jnp.where(at == slot * nb.shape[1] + k, nb, 0.0)).astype(jnp.int32)
    _, t_dev, _, n_out, run = rest_ref.shape
    n_rows = n_out * t_dev
    for i, ref in enumerate(strips):
        strip_ref[i] = ref[...].reshape(strip_ref.shape[1:])
    upper = iota((n_rows, 2 * STRIP), 1) >= STRIP
    quarter = (0.25 * placing(n_out, t_dev)).astype(jnp.bfloat16)
    n_nb = nb.shape[1] // 2
    copies = []
    for slot in range(2):
        blend = jnp.zeros((n_rows, 2 * STRIP), jnp.float32)
        for k in range(n_nb):
            strip = strip_ref[number(slot, k), :, number(slot, n_nb + k)].reshape(n_rows, 2 * STRIP)
            blend += jnp.dot(quarter, strip, preferred_element_type=jnp.float32)
        for i, part in enumerate((pltpu.roll(blend, STRIP, 1), blend)):
            part = jnp.where(upper, part, 0.0).reshape(t_dev, n_out, run)
            done_ref[i, :, slot] = rest_ref[i, :, slot] + part
            target = out_hbm.at[:, slot, :, pl.ds((2 * i + 1) * run, run)]
            copies.append(pltpu.make_async_copy(done_ref.at[i, :, slot], target, sem.at[slot, i]))
            copies[-1].start()
    for copy in copies:
        copy.wait()


def join(sources, placed, rest, strips):
    _, t_dev, _, n_out, run = rest.shape
    assert run == 2 * STRIP
    return pl.pallas_call(
        join_kernel,
        out_shape=pltpu.HBM(placed.shape, placed.dtype),
        in_specs=[vmem(), pl.BlockSpec(memory_space=pltpu.HBM)] + [vmem()] * (1 + len(strips)),
        out_specs=pl.BlockSpec(memory_space=pltpu.HBM),
        scratch_shapes=[
            pltpu.VMEM((len(strips), n_out, 2, t_dev, 2 * STRIP), jnp.bfloat16),
            pltpu.VMEM(rest.shape, jnp.float32),
            pltpu.SemaphoreType.DMA((2, 2)),
        ],
        input_output_aliases={1: 0},
        compiler_params=pltpu.CompilerParams(vmem_limit_bytes=16 * MIB),
        name="join",
    )(sources, placed, rest, *strips)


def exchange(x, axis):
    return lax.all_to_all(x, axis, split_axis=0, concat_axis=0, tiled=True)


def local(visibilities, kernels, delays, tile_of, plane_of, counts, neighbours):
    n_facet = lax.axis_size("facet")
    n_chan = lax.axis_size("chan")
    facet_index = lax.axis_index("facet")
    halves, facets, blocks, _, bv = visibilities.shape
    fac_dev = facets // n_facet
    n_tiles = 16 * n_chan
    t_dev = n_tiles // n_chan
    n_rows = fac_dev * blocks
    per = n_rows // n_chan

    vis = visibilities.reshape(halves, n_facet * n_chan, per, bv)
    vis, inner, outer, place, code, piece = send_order(
        counts, plane_of, tile_of, delays.reshape(n_chan, per, bv), vis, kernels.shape[0], n_chan, t_dev
    )
    vis = exchange(vis, ("facet", "chan"))

    rows = exchange(average(inner, outer, vis), "chan")
    main = exchange(grid_rows(piece, rows, place, code, kernels, fac_dev * n_tiles), "chan")

    own = strips_of(main)
    chips = n_facet // 2
    along = lambda x, dz: lax.ppermute(x, "facet", [(f, (f + 2 * dz) % n_facet) for f in range(n_facet)])
    across = lambda x: lax.ppermute(x, "facet", [(f, f ^ 1) for f in range(n_facet)])
    arrived = {dz: along(own, dz) for dz in range(2, chips)}
    placed, rest = place_main(main)
    own, rest = lax.optimization_barrier((own, rest))
    arrived[1] = along(own, 1)
    strips = [own] + [arrived[dz] for dz in range(1, chips)]
    strips += [across(s) for s in strips]
    mine = lax.dynamic_slice_in_dim(neighbours, facet_index * fac_dev, fac_dev, 0)
    group = mine // fac_dev
    source = (facet_index // 2 - group // 2) % chips + chips * ((group + facet_index) % 2)
    sources = jnp.concatenate([source, mine % fac_dev], axis=1).astype(jnp.int32)
    return join(sources, placed, rest, strips)


def solution(mesh):
    return jax.shard_map(
        local,
        mesh=mesh,
        in_specs=(
            P(None, None, None, ("facet", "chan"), None),
            P(),
            P("facet", None, None),
            P("facet", None),
            P("facet", None),
            P("facet"),
            P(),
        ),
        out_specs=P("chan", "facet", None, None),
        check_vma=False,
    )
```
